32 devices in a mesh: dp: 4 (over x, core), rows: 8 (over z, y).
Axes of the slice: x: 2, y: 2, z: 4, core: 2. Of those that a mesh axis runs over, the one named last changes fastest.
Arguments:
- item_table: float32 [131072, 128], P(('dp', 'rows')), may hold values from -3 to 3
- adagrad_state: float32 [131072, 128], P(('dp', 'rows')), may hold values from 0.0001 to 0.01
- history_ids: int32 [4096, 50], P(('dp', 'rows')), may hold values from 0 to 131071, as said below
- positive_ids: int32 [4096], P(('dp', 'rows')), may hold values from 0 to 131071, as said below
Outputs:
- new_table: float32 [131072, 128], P(('dp', 'rows'))
- new_state: float32 [131072, 128], P(('dp', 'rows'))
The draws below stay inside these ranges and needn't reach their ends.
Inputs may be any that keep to these rules, and one draw needn't show every extreme that they name: `history_ids`: ids are counted over one device's 128 users (an aligned block of users), history and positive together, with repeats. In every such block, at most 512 ids have any one value of id // 4096, and some value has exactly 512; one value has exactly 512 in every block. Popular items repeat. `positive_ids`: counted together with history_ids as stated there.
All inputs are finite; a program needn't handle non-finite values.
Results may differ from the reference program's by a relative error of at most 0.00012.
Values sent between devices are 32-bit elements; how exact they have to be, the bound alone decides.
A program may use at most 128 MiB of HBM per device.

```python
import math
import jax
import jax.numpy as jnp
from jax import lax

EMB = 128
HIST = 50
USER_DEV = 128
ROW_DEV = 4096
USERS = 4096
ITEMS = 131072
CAP = 512


def request_ids(key):
    base = jax.random.fold_in(key, 7001)
    keys = jax.random.split(base, 7)
    blocks = USERS // USER_DEV
    slots = blocks * CAP
    per_block = USER_DEV * (HIST + 1)
    slot_owner = jnp.arange(slots, dtype=jnp.int32) // CAP
    noise = jax.random.randint(keys[0], (blocks, slots), 0, 1024, dtype=jnp.int32)
    level = jax.random.randint(keys[1], (blocks, blocks), 0, 4, dtype=jnp.int32) * 512
    hot_common = jax.random.randint(keys[2], (), 0, blocks, dtype=jnp.int32)
    hot_own = jax.random.randint(keys[3], (blocks,), 0, blocks, dtype=jnp.int32)
    hot_flag = jnp.logical_or(slot_owner[None, :] == hot_common, slot_owner[None, :] == hot_own[:, None]).astype(jnp.int32)
    score = (noise + level[:, slot_owner] + 8192 * hot_flag) * slots + jnp.arange(slots, dtype=jnp.int32)[None, :]
    picked_score, chosen = lax.top_k(score, per_block)
    owners = (chosen // CAP).astype(jnp.int32)
    order_keys = jax.random.randint(keys[4], (blocks, per_block), 0, 32768, dtype=jnp.int32) * per_block + jnp.arange(per_block, dtype=jnp.int32)[None, :]
    order = jnp.argsort(order_keys, axis=1, stable=True)
    owners = jnp.take_along_axis(owners, order, axis=1)
    first = jax.random.randint(keys[5], (blocks, per_block), 0, ROW_DEV, dtype=jnp.int32)
    second = jax.random.randint(keys[6], (blocks, per_block), 0, ROW_DEV, dtype=jnp.int32)
    offset = first * second // ROW_DEV
    return (owners * ROW_DEV + offset).astype(jnp.int32).reshape(USERS, HIST + 1)


def draw_history_ids(key, part):
    return request_ids(key)[:, :HIST]


def draw_positive_ids(key, part):
    return request_ids(key)[:, HIST]


def levels(stream_key, dims, cuts, least, high):
    def one(position, parts):
        heights = jax.random.uniform(jax.random.fold_in(jax.random.fold_in(stream_key, 6), position), (parts,), jnp.float32, least / len(cuts), high / len(cuts))
        return jnp.repeat(jnp.exp(heights), dims[position] // parts).reshape((-1,) + (1,) * (len(dims) - position - 1))

    gain = one(*cuts[0])
    for cut in cuts[1:]:
        gain = gain * one(*cut)
    return gain


def normal_values(own_key, dims, width, limit, cuts=(), kind=jnp.bfloat16):
    array = jax.random.normal(own_key, dims, jnp.float32) * width
    if len(cuts) > 0:
        array = levels(own_key, dims, cuts, -0.22, 0.18) * array
    return jnp.clip(array, min=-limit, max=limit).astype(kind)


def setup_inputs(seed: int = 0) -> dict:
    streams_of = jax.random.split(jax.random.key(seed), 5)
    return {
        "item_table": normal_values(streams_of[0], (ITEMS, EMB), 0.5, 3.0, ((0, 32),), jnp.float32),
        "adagrad_state": jnp.clip(jnp.exp(math.log(0.01) - 4.6051702 * jax.random.uniform(streams_of[1], (ITEMS, EMB), jnp.float32) ** levels(streams_of[1], (ITEMS, EMB), ((0, 32),), -0.2, 0.2)), 0.0001, 0.01),
        "history_ids": draw_history_ids(jax.random.fold_in(streams_of[4], 71), 0),
        "positive_ids": draw_positive_ids(jax.random.fold_in(streams_of[4], 71), 0),
    }


penalty_weight = 10.0
step_size = 0.05

def reference(item_table, adagrad_state, history_ids, positive_ids):
    hist_rows = jnp.take(item_table, history_ids, axis=0)
    user_vecs = lax.optimization_barrier(jnp.sum(hist_rows, axis=1)) / HIST
    positive_vecs = jnp.take(item_table, positive_ids, axis=0)
    score_gap = lax.optimization_barrier(jnp.sum(user_vecs * positive_vecs, axis=1)) - 1.0
    user_gram = jnp.dot(user_vecs.T, user_vecs, precision=lax.Precision.HIGHEST, preferred_element_type=jnp.float32)
    item_gram = jnp.dot(item_table.T, item_table, precision=lax.Precision.HIGHEST, preferred_element_type=jnp.float32)
    penalty_coef = penalty_weight / ITEMS
    user_grad = 2.0 * score_gap[:, None] * positive_vecs + 2.0 * penalty_coef * jnp.dot(user_vecs, item_gram, precision=lax.Precision.HIGHEST, preferred_element_type=jnp.float32)
    positive_grad = 2.0 * score_gap[:, None] * user_vecs
    per_history = jnp.broadcast_to((user_grad / HIST)[:, None, :], hist_rows.shape).reshape(-1, EMB)
    row_grad = 2.0 * penalty_coef * jnp.dot(item_table, user_gram, precision=lax.Precision.HIGHEST, preferred_element_type=jnp.float32)
    row_grad = row_grad.at[history_ids.reshape(-1)].add(per_history)
    row_grad = row_grad.at[positive_ids].add(positive_grad)
    new_state = adagrad_state + row_grad * row_grad
    new_table = item_table - step_size * row_grad / jnp.sqrt(new_state)
    return (new_table, new_state)
```

```python
import functools

import jax
import jax.numpy as jnp
from jax import lax
from jax.experimental import pallas as pl
from jax.experimental.pallas import tpu as pltpu
from jax.sharding import PartitionSpec as P

penalty_weight = 10.0
step_size = 0.05
LOW = 128
STREAMS = 8
HIGHEST = lax.Precision.HIGHEST
f32, bf16, i32 = jnp.float32, jnp.bfloat16, jnp.int32


def round_up(value, unit):
    return (value + unit - 1) // unit * unit


def route_kernel(devices, capacity, users_dev, block, owner_ref, local_ref, code_ref, out_ref, acc):
    blocks = owner_ref.shape[1] // block
    upper = (
        lax.broadcasted_iota(i32, (block, block), 0) <= lax.broadcasted_iota(i32, (block, block), 1)
    ).astype(bf16)
    owners = lax.broadcasted_iota(i32, (devices, block), 0)
    ranks_to = lax.broadcasted_iota(i32, (capacity, block), 0)
    acc[...] = jnp.zeros_like(acc)
    carry = jnp.zeros((devices, 1), f32)
    for j in range(blocks):
        cols = slice(j * block, (j + 1) * block)
        local = local_ref[:, cols]
        high = (local // LOW).astype(f32)
        low = (local % LOW).astype(f32)
        code = code_ref[:, cols].astype(f32)
        member = (owner_ref[:, cols] == owners).astype(f32)
        prefix = jnp.dot(member.astype(bf16), upper, preferred_element_type=f32)
        rank = jnp.sum(member * (prefix + carry), axis=0, keepdims=True) - 1.0
        carry = carry + jnp.sum(member, axis=1, keepdims=True)
        left = jnp.concatenate(
            [member * high, member * low, member * code, member], axis=0
        ).astype(bf16)
        right = (rank.astype(i32) == ranks_to).astype(f32).astype(bf16)
        acc[...] += lax.dot_general(
            left, right, (((1,), (1,)), ((), ())), preferred_element_type=f32
        )
    row = acc[0:devices] * LOW + acc[devices : 2 * devices]
    code = acc[2 * devices : 3 * devices]
    present = acc[3 * devices : 4 * devices]
    empty = 2 * users_dev
    out_ref[0] = row.astype(i32)
    out_ref[1] = jnp.where(present > 0.5, code, float(empty)).astype(i32)


def split2(x):
    hi = x.astype(bf16)
    return hi, (x - hi.astype(f32)).astype(bf16)


def line_sizes(data, shard):
    cols = max(n for n in range(1, shard + 1) if shard % n == 0 and n * n <= shard)
    return data // 2, cols, shard // cols


ORDERS = ((0, 1, 2), (1, 2, 0))
LAGS = (2, 4, 6, 8)
VSLOTS = 4


def exchange_kernel(
    sizes, capacity, users_dev, hist_len, coef, unroll,
    rows_ref, codes_ref, hot_ref, gram_ref, table_ref, vals_ref, ugram_ref,
    picked, part, pair, mail, grads, cur, vbuf, upart, gsum, gmail, gfull,
    pair_send, pair_recv, mail_send, mail_recv, ag_send, ag_recv, twin_send, twin_recv, gram_send, gram_recv, vsem,
):
    nx, ny, nz = sizes
    plane = nx * ny * nz
    shard = ny * nz
    width = table_ref.shape[1]
    half = width // 2
    dp, rw = lax.axis_index("dp"), lax.axis_index("rows")
    core = lax.rem(dp, 2)
    pos = (dp // 2, lax.rem(rw, ny), rw // ny)
    origin = (0, 0, 0)
    axes = (0, 1, 2)

    def device(chip, c):
        return chip[0] * 2 + c, chip[2] * ny + chip[1]

    def block(chip, c):
        d, r = device(chip, c)
        return d * shard + r

    def ahead(r):
        return tuple(lax.rem(p + k, n) for p, k, n in zip(pos, r, sizes))

    def behind(o):
        return tuple(lax.rem(p - k + n, n) for p, k, n in zip(pos, o, sizes))

    def only(a, k):
        return tuple(k if b == a else 0 for b in axes)

    def add(r, a, k):
        return tuple(v + k if b == a else v for b, v in enumerate(r))

    def slot(r):
        return (r[0] * ny + r[1]) * nz + r[2]

    def unslot(at):
        return at // (ny * nz), lax.rem(at // nz, ny), lax.rem(at, nz)

    partner = device(pos, 1 - core)

    def remote(src, dst, send, recv, dev):
        return pltpu.make_async_remote_copy(
            src_ref=src, dst_ref=dst, send_sem=send, recv_sem=recv,
            device_id=dev, device_id_type=pl.DeviceIdType.MESH,
        )

    def each(first, count, act):
        def step(k, _):
            act(k)
            return 0

        lax.fori_loop(first, count, step, 0)

    barrier = pltpu.get_barrier_semaphore()
    greeted = 1
    pl.semaphore_signal(barrier, inc=1, device_id=partner, device_id_type=pl.DeviceIdType.MESH)
    for a in axes:
        for k in range(1, sizes[a]):
            greeted += 1
            pl.semaphore_signal(
                barrier, inc=1, device_id=device(ahead(only(a, k)), core), device_id_type=pl.DeviceIdType.MESH
            )
    pl.semaphore_wait(barrier, greeted)

    def pair_copy(at):
        return remote(part.at[0, at], pair.at[at], pair_send.at[at], pair_recv.at[at], partner)

    def letter(h, at, dev):
        return remote(part.at[1, at, h], mail.at[h, at], mail_send.at[h, at], mail_recv.at[h, at], dev)

    def parcel(h, at, b, dev):
        return remote(grads.at[b, h], grads.at[b, h], ag_send.at[h, at], ag_recv.at[h, at], dev)

    def twin(at, b):
        return remote(grads.at[b], grads.at[b], twin_send.at[at], twin_recv.at[at], partner)

    first = [1]
    for a in axes:
        first.append(first[-1] + sizes[a] - 1)
    last = first[3]
    mine = pl.ds(pl.multiple_of(core * half, 8), half)
    theirs = pl.ds(pl.multiple_of((1 - core) * half, 8), half)

    def gram_pair(t, src):
        return remote(src.at[theirs], gmail.at[t, 0], gram_send.at[t, 0], gram_recv.at[t, 0], partner)

    def gram_line(t, a, k):
        at = first[a] + k - 1
        return remote(
            gsum.at[t, a], gmail.at[t, at], gram_send.at[t, at], gram_recv.at[t, at], device(ahead(only(a, k)), core)
        )

    def gram_final(t):
        return remote(gsum.at[t, 3], gfull.at[t, mine], gram_send.at[t, last], gram_recv.at[t, last], partner)

    def gram_open(t, src):
        gram_pair(t, src).start()

    def gram_send_line(t, a):
        for k in range(1, sizes[a]):
            gram_line(t, a, k).start()

    def gram_step(t, src, stage):
        if stage == 0:
            gram_pair(t, src).wait_recv()
            gsum[t, 0] = src[mine, :] + gmail[t, 0]
        elif stage <= 3:
            a = stage - 1
            total = gsum[t, a]
            for k in range(1, sizes[a]):
                gram_line(t, a, k).wait_recv()
                total = total + gmail[t, first[a] + k - 1]
            gsum[t, a + 1] = total
        else:
            gram_final(t).wait_recv()
        if stage < 3:
            gram_send_line(t, stage)
        elif stage == 3:
            gram_final(t).start()
            gfull[t, mine] = gsum[t, 3]

    def gram_drain(t, src):
        gram_pair(t, src).wait_send()
        for a in axes:
            for k in range(1, sizes[a]):
                gram_line(t, a, k).wait_send()
        gram_final(t).wait_send()

    codes_to = lax.broadcasted_iota(i32, (2 * users_dev, capacity), 0)

    def gather(b, j, at):
        base = b * capacity

        def some(s, _):
            start = base + s * unroll
            for k in range(unroll):
                r = rows_ref[start + k]
                picked[pl.ds(s * unroll + k, 1), :] = table_ref[pl.ds(r, 1), :]
            return 0

        lax.fori_loop(0, capacity // unroll, some, 0)
        x = picked[...]
        hi, lo = split2(x)
        hot = (hot_ref[b] == codes_to).astype(f32).astype(bf16)
        both = jnp.dot(hot, jnp.concatenate([hi, lo], axis=1), preferred_element_type=f32)
        out = both[:, :width] + both[:, width:]
        part[j, at, 0] = out[:users_dev]
        part[j, at, 1] = out[users_dev:]

    def arrive(h, r, a):
        at = slot(r)
        for k in range(1, sizes[a]):
            m = slot(add(r, a, k))
            letter(h, m, partner).wait_recv()
            part[1, at, h] = part[1, at, h] + mail[h, m]

    def leave(h, r, a):
        @pl.when(r[a] != 0)
        def _():
            chip = tuple(lax.rem(p + r[a], n) if b == a else p for b, (p, n) in enumerate(zip(pos, sizes)))
            letter(h, slot(r), device(chip, core)).start()

    gram_open(0, gram_ref)

    def reduce_step(i, _):
        for stage in range(4):
            j = i - LAGS[stage]
            at = plane - 1 - j

            @pl.when(jnp.logical_and(j >= 0, j < plane))
            def _():
                r = unslot(at)
                if stage == 0:
                    pair_copy(at).wait_recv()
                    for h in range(2):
                        part[1, at, h] = part[1, at, h] + pair[at, h]
                        leave(h, r, ORDERS[h][0])
                else:
                    for h in range(2):
                        order = ORDERS[h]
                        clear = r[order[0]] == 0
                        for a in order[1:stage]:
                            clear = jnp.logical_and(clear, r[a] == 0)

                        @pl.when(clear)
                        def _():
                            arrive(h, r, order[stage - 1])
                            if stage < 3:
                                leave(h, r, order[stage])

        for stage in range(5):
            @pl.when(i == 2 * stage + 2)
            def _():
                gram_step(0, gram_ref, stage)

        @pl.when(i < plane)
        def _():
            at = plane - 1 - i
            chip = ahead(unslot(at))

            def one(j, _):
                c = (1 - core) * (1 - j) + core * j
                gather(block(chip, c), j, at)

                @pl.when(j == 0)
                def _():
                    pair_copy(at).start()

                return 0

            lax.fori_loop(0, 2, one, 0)

        return 0

    lax.fori_loop(0, plane + LAGS[3], reduce_step, 0)

    me = block(pos, core)
    uv = part[1, 0, 0] / hist_len
    pv = part[1, 0, 1]
    gap = jnp.sum(uv * pv, axis=1, keepdims=True) - 1.0
    ug = 2.0 * gap * pv + 2.0 * coef * jnp.dot(uv, gfull[0], precision=HIGHEST, preferred_element_type=f32)
    grads[me, 0] = ug / hist_len
    grads[me, 1] = 2.0 * gap * uv

    def forward(h, o, b, a):
        for k in range(1, sizes[a]):
            chip = tuple(lax.rem(p + k, n) if c == a else p for c, (p, n) in enumerate(zip(pos, sizes)))
            parcel(h, slot(add(o, a, k)), b, device(chip, core)).start()

    def received(h, o):
        b = block(behind(o), core)
        parcel(h, slot(o), b, partner).wait_recv()
        return b

    ways = tuple(order[::-1] for order in ORDERS)
    for a in range(3):
        for h in range(2):
            forward(h, origin, me, ways[h][a])
    twin(0, me).start()
    upart[...] = lax.dot_general(
        uv, uv, (((0,), (0,)), ((), ())), precision=HIGHEST, preferred_element_type=f32
    )
    gram_open(1, upart)
    cur[pl.ds(2 * users_dev, 8), :] = jnp.zeros((8, width), f32)

    def vals_copy(v, b):
        return pltpu.make_async_copy(vbuf.at[v], vals_ref.at[b], vsem.at[v])

    def vals(n, b):
        v = lax.rem(n, VSLOTS)

        @pl.when(n >= VSLOTS)
        def _():
            vals_copy(v, b).wait()

        cur[pl.ds(0, users_dev), :] = grads[b, 0]
        cur[pl.ds(users_dev, users_dev), :] = grads[b, 1]
        base = b * capacity

        def some(s, _):
            start = base + s * unroll
            for k in range(unroll):
                c = codes_ref[start + k]
                vbuf[v, pl.ds(s * unroll + k, 1), :] = cur[pl.ds(c, 1), :]
            return 0

        lax.fori_loop(0, capacity // unroll, some, 0)
        vals_copy(v, b).start()

    for h in range(2):
        a1, a2, a3 = ways[h]
        for k in range(1, sizes[a1]):
            o = only(a1, k)
            b = received(h, o)
            forward(h, o, b, a2)
            forward(h, o, b, a3)
    gram_step(1, upart, 0)
    for h in range(2):
        a1, a2, a3 = ways[h]
        for k in range(1, sizes[a2]):
            for m in range(sizes[a1]):
                o = add(only(a2, k), a1, m)
                b = received(h, o)
                forward(h, o, b, a3)
        gram_step(1, upart, h + 1)

    def spread(n, _):
        @pl.when(n < plane)
        def _():
            o = unslot(n)
            b = block(behind(o), core)
            for h in range(2):
                @pl.when(o[ways[h][2]] != 0)
                def _():
                    received(h, o)

            @pl.when(n > 0)
            def _():
                twin(n, b).start()

            vals(2 * n, b)

        @pl.when(n > 0)
        def _():
            o = unslot(n - 1)
            b = block(behind(o), 1 - core)
            twin(n - 1, b).wait_recv()
            vals(2 * n - 1, b)

        for stage in (3, 4):
            @pl.when(n == 4 * (stage - 2))
            def _():
                gram_step(1, upart, stage)

        return 0

    lax.fori_loop(0, plane + 1, spread, 0)
    ugram_ref[...] = gfull[1]

    def drain(n):
        pair_copy(n).wait_send()
        twin(n, me).wait_send()

    each(0, plane, drain)

    def drain_mail(n):
        for h in range(2):
            letter(h, n, partner).wait_send()
            parcel(h, n, me, partner).wait_send()

    each(1, plane, drain_mail)
    gram_drain(0, gram_ref)
    gram_drain(1, upart)
    each(0, VSLOTS, lambda v: vals_copy(v, me).wait())


def scatter_kernel(
    coef, chunk, unroll, tile,
    rows_ref, vals_ref, ugram_ref, table_ref, state_ref, new_table_ref, new_state_ref,
    vbuf, table, state, vsem, in_sem, out_sem, *accs,
):
    entries = rows_ref.shape[0]
    chunks = entries // chunk
    part = chunk // len(accs)
    rows_dev, width = table.shape
    tiles = rows_dev // tile

    def vals_copy(n):
        s = lax.rem(n, 2)
        return pltpu.make_async_copy(
            vals_ref.at[pl.ds(pl.multiple_of(n * chunk, 8), chunk)], vbuf.at[s], vsem.at[s]
        )

    table_copy = pltpu.make_async_copy(table_ref, table, in_sem.at[0])
    state_copy = pltpu.make_async_copy(state_ref, state, in_sem.at[1])
    vals_copy(0).start()
    vals_copy(1).start()
    table_copy.start()
    state_copy.start()
    for acc in accs:
        acc[...] = jnp.zeros_like(acc)

    def one(n, _):
        v = lax.rem(n, 2)
        vals_copy(n).wait()

        def scatter(s, _):
            start = n * chunk + s * unroll
            for q in range(unroll):
                rows = [rows_ref[start + (k * part + q)] for k in range(len(accs))]
                news = [
                    acc[pl.ds(r, 1), :] + vbuf[v, pl.ds(s * unroll + (k * part + q), 1), :]
                    for k, (acc, r) in enumerate(zip(accs, rows))
                ]
                for acc, r, new in zip(accs, rows, news):
                    acc[pl.ds(r, 1), :] = new
            return 0

        lax.fori_loop(0, part // unroll, scatter, 0)

        @pl.when(n + 2 < chunks)
        def _():
            vals_copy(n + 2).start()

        return 0

    lax.fori_loop(0, chunks, one, 0)
    table_copy.wait()
    state_copy.wait()
    u0, u1 = split2(ugram_ref[...])
    u00 = jnp.concatenate([u0, u0], axis=0)

    def out_copy(t, which):
        at = pl.ds(pl.multiple_of(t * tile, 8), tile)
        src, dst = ((table, new_table_ref), (state, new_state_ref))[which]
        return pltpu.make_async_copy(src.at[at], dst.at[at], out_sem.at[which, t])

    def finish(t, _):
        at = pl.ds(pl.multiple_of(t * tile, 8), tile)
        item = table[at, :]
        t0, t1 = split2(item)
        g = jnp.dot(jnp.concatenate([t0, t1], axis=1), u00, preferred_element_type=f32)
        g = 2.0 * coef * (g + jnp.dot(t0, u1, preferred_element_type=f32))
        add = accs[0][at, :]
        for acc in accs[1:]:
            add = add + acc[at, :]
        g = g + add
        new = state[at, :] + g * g
        state[at, :] = new
        table[at, :] = item - step_size * g / jnp.sqrt(new)
        out_copy(t, 0).start()
        out_copy(t, 1).start()
        return 0

    lax.fori_loop(0, tiles, finish, 0)

    def drain(t, _):
        out_copy(t, 0).wait()
        out_copy(t, 1).wait()
        return 0

    lax.fori_loop(0, tiles, drain, 0)


VM = pl.BlockSpec(memory_space=pltpu.VMEM)
HB = pl.BlockSpec(memory_space=pl.ANY)
SM = pl.BlockSpec(memory_space=pltpu.SMEM)
PARAMS = pltpu.CompilerParams(vmem_limit_bytes=60 * 1024 * 1024)


def shards(item_table, adagrad_state, history_ids, positive_ids):
    rows_dev, width = item_table.shape
    users_dev, hist_len = history_ids.shape
    devices = lax.axis_size("dp") * lax.axis_size("rows")
    groups = 2 * users_dev
    count = users_dev * (hist_len + 1)
    capacity = max(8, (count * 5 // (2 * devices) + 7) // 8 * 8)
    block = 512
    padded = round_up(count, block)
    requests = jnp.concatenate([history_ids.reshape(-1), positive_ids])
    code = jnp.concatenate(
        [jnp.arange(users_dev * hist_len, dtype=i32) // hist_len, users_dev + jnp.arange(users_dev, dtype=i32)]
    )
    requests = jnp.pad(requests, (0, padded - count), constant_values=devices * rows_dev)
    code = jnp.pad(code, (0, padded - count))
    owner = requests // rows_dev
    local = requests - owner * rows_dev

    lists = pl.pallas_call(
        functools.partial(route_kernel, devices, capacity, users_dev, block),
        out_shape=jax.ShapeDtypeStruct((2, devices, capacity), i32),
        in_specs=[VM] * 3,
        out_specs=VM,
        scratch_shapes=[pltpu.VMEM((4 * devices, capacity), f32)],
        compiler_params=PARAMS,
        name="route",
    )(owner[None], local[None], code[None])
    asked = lax.all_to_all(lists, ("dp", "rows"), split_axis=1, concat_axis=1, tiled=True)
    rows = asked[0].reshape(-1)
    codes = asked[1]
    entries = devices * capacity
    item_gram = jnp.dot(item_table.T, item_table, precision=HIGHEST, preferred_element_type=f32)
    data, shard = lax.axis_size("dp"), lax.axis_size("rows")
    sizes = line_sizes(data, shard)
    plane = devices // 2
    lines = sum(sizes) - 1
    coef = penalty_weight / (rows_dev * devices)
    dma = pltpu.SemaphoreType.DMA
    vals, user_gram = pl.pallas_call(
        functools.partial(exchange_kernel, sizes, capacity, users_dev, hist_len, coef, 32),
        out_shape=(
            jax.ShapeDtypeStruct((devices, capacity, width), f32),
            jax.ShapeDtypeStruct((width, width), f32),
        ),
        in_specs=[SM, SM, VM, VM, VM],
        out_specs=(HB, VM),
        scratch_shapes=[
            pltpu.VMEM((capacity, width), f32),
            pltpu.VMEM((2, plane, 2, users_dev, width), f32),
            pltpu.VMEM((plane, 2, users_dev, width), f32),
            pltpu.VMEM((2, plane, users_dev, width), f32),
            pltpu.VMEM((devices, 2, users_dev, width), f32),
            pltpu.VMEM((groups + 8, width), f32),
            pltpu.VMEM((VSLOTS, capacity, width), f32),
            pltpu.VMEM((width, width), f32),
            pltpu.VMEM((2, 4, width // 2, width), f32),
            pltpu.VMEM((2, lines, width // 2, width), f32),
            pltpu.VMEM((2, width, width), f32),
            dma((plane,)),
            dma((plane,)),
            dma((2, plane)),
            dma((2, plane)),
            dma((2, plane)),
            dma((2, plane)),
            dma((plane,)),
            dma((plane,)),
            dma((2, lines)),
            dma((2, lines)),
            dma((VSLOTS,)),
        ],
        compiler_params=pltpu.CompilerParams(
            vmem_limit_bytes=60 * 1024 * 1024, collective_id=0, has_side_effects=True
        ),
        name="exchange",
    )(rows, codes.reshape(-1), codes[:, None, :], item_gram, item_table)
    chunk, tile = min(2048, entries), 256
    return pl.pallas_call(
        functools.partial(scatter_kernel, coef, chunk, 4, tile),
        out_shape=(
            jax.ShapeDtypeStruct(item_table.shape, f32),
            jax.ShapeDtypeStruct(item_table.shape, f32),
        ),
        in_specs=[SM, HB, VM, HB, HB],
        out_specs=(HB, HB),
        scratch_shapes=[
            pltpu.VMEM((2, chunk, width), f32),
            pltpu.VMEM((rows_dev, width), f32),
            pltpu.VMEM((rows_dev, width), f32),
            dma((2,)),
            dma((2,)),
            dma((2, rows_dev // tile)),
        ]
        + [pltpu.VMEM((rows_dev, width), f32)] * STREAMS,
        compiler_params=PARAMS,
        name="scatter",
    )(rows, vals.reshape(entries, width), user_gram, item_table, adagrad_state)


def solution(mesh):
    return jax.shard_map(
        shards,
        mesh=mesh,
        in_specs=(
            P(("dp", "rows"), None),
            P(("dp", "rows"), None),
            P(("dp", "rows"), None),
            P(("dp", "rows")),
        ),
        out_specs=(P(("dp", "rows"), None), P(("dp", "rows"), None)),
        check_vma=False,
    )
```

```python
import functools

import jax
import jax.numpy as jnp
from jax import lax
from jax.experimental import pallas as pl
from jax.experimental.pallas import tpu as pltpu
from jax.sharding import PartitionSpec as P

penalty_weight = 10.0
step_size = 0.05
LOW = 128
STREAMS = 8
HIGHEST = lax.Precision.HIGHEST
f32, bf16, i32 = jnp.float32, jnp.bfloat16, jnp.int32


def round_up(value, unit):
    return (value + unit - 1) // unit * unit


def route_kernel(devices, capacity, users_dev, block, owner_ref, local_ref, code_ref, out_ref, acc):
    blocks = owner_ref.shape[1] // block
    upper = (
        lax.broadcasted_iota(i32, (block, block), 0) <= lax.broadcasted_iota(i32, (block, block), 1)
    ).astype(bf16)
    owners = lax.broadcasted_iota(i32, (devices, block), 0)
    ranks_to = lax.broadcasted_iota(i32, (capacity, block), 0)
    acc[...] = jnp.zeros_like(acc)
    carry = jnp.zeros((devices, 1), f32)
    for j in range(blocks):
        cols = slice(j * block, (j + 1) * block)
        local = local_ref[:, cols]
        high = (local // LOW).astype(f32)
        low = (local % LOW).astype(f32)
        code = code_ref[:, cols].astype(f32)
        member = (owner_ref[:, cols] == owners).astype(f32)
        prefix = jnp.dot(member.astype(bf16), upper, preferred_element_type=f32)
        rank = jnp.sum(member * (prefix + carry), axis=0, keepdims=True) - 1.0
        carry = carry + jnp.sum(member, axis=1, keepdims=True)
        left = jnp.concatenate(
            [member * high, member * low, member * code, member], axis=0
        ).astype(bf16)
        right = (rank.astype(i32) == ranks_to).astype(f32).astype(bf16)
        acc[...] += lax.dot_general(
            left, right, (((1,), (1,)), ((), ())), preferred_element_type=f32
        )
    row = acc[0:devices] * LOW + acc[devices : 2 * devices]
    code = acc[2 * devices : 3 * devices]
    present = acc[3 * devices : 4 * devices]
    empty = 2 * users_dev
    out_ref[0] = row.astype(i32)
    out_ref[1] = jnp.where(present > 0.5, code, float(empty)).astype(i32)


def split2(x):
    hi = x.astype(bf16)
    return hi, (x - hi.astype(f32)).astype(bf16)


def line_sizes(data, shard):
    cols = max(n for n in range(1, shard + 1) if shard % n == 0 and n * n <= shard)
    return data // 2, cols, shard // cols


ORDERS = ((0, 1, 2), (1, 0, 2))
LAGS = (2, 3, 4, 5)
VSLOTS = 4
TWIN_LAG = 1


def exchange_kernel(
    sizes, capacity, users_dev, hist_len, coef, unroll,
    rows_ref, codes_ref, hot_ref, gram_ref, table_ref, vals_ref, ugram_ref,
    picked, part, pair, mail, grads, cur, vbuf, upart, gsum, gmail, gfull,
    pair_send, pair_recv, mail_send, mail_recv, ag_send, ag_recv, twin_send, twin_recv, gram_send, gram_recv, vsem,
):
    nx, ny, nz = sizes
    plane = nx * ny * nz
    shard = ny * nz
    width = table_ref.shape[1]
    half = width // 2
    dp, rw = lax.axis_index("dp"), lax.axis_index("rows")
    core = lax.rem(dp, 2)
    pos = (dp // 2, lax.rem(rw, ny), rw // ny)
    origin = (0, 0, 0)
    axes = (0, 1, 2)

    def device(chip, c):
        return chip[0] * 2 + c, chip[2] * ny + chip[1]

    def block(chip, c):
        d, r = device(chip, c)
        return d * shard + r

    def ahead(r):
        return tuple(lax.rem(p + k, n) for p, k, n in zip(pos, r, sizes))

    def behind(o):
        return tuple(lax.rem(p - k + n, n) for p, k, n in zip(pos, o, sizes))

    def only(a, k):
        return tuple(k if b == a else 0 for b in axes)

    def add(r, a, k):
        return tuple(v + k if b == a else v for b, v in enumerate(r))

    def slot(r):
        return (r[0] * ny + r[1]) * nz + r[2]

    def ranked(n, digits):
        out = [0, 0, 0]
        for a in reversed(digits):
            out[a] = lax.rem(n, sizes[a])
            n = n // sizes[a]
        return tuple(out)

    partner = device(pos, 1 - core)

    def remote(src, dst, send, recv, dev):
        return pltpu.make_async_remote_copy(
            src_ref=src, dst_ref=dst, send_sem=send, recv_sem=recv,
            device_id=dev, device_id_type=pl.DeviceIdType.MESH,
        )

    def each(first, count, act):
        def step(k, _):
            act(k)
            return 0

        lax.fori_loop(first, count, step, 0)

    barrier = pltpu.get_barrier_semaphore()
    greeted = 1
    pl.semaphore_signal(barrier, inc=1, device_id=partner, device_id_type=pl.DeviceIdType.MESH)
    for a in axes:
        for k in range(1, sizes[a]):
            greeted += 1
            pl.semaphore_signal(
                barrier, inc=1, device_id=device(ahead(only(a, k)), core), device_id_type=pl.DeviceIdType.MESH
            )
    pl.semaphore_wait(barrier, greeted)

    def pair_copy(at):
        return remote(part.at[0, at], pair.at[at], pair_send.at[at], pair_recv.at[at], partner)

    def letter(h, at, dev):
        return remote(part.at[1, at, h], mail.at[h, at], mail_send.at[h, at], mail_recv.at[h, at], dev)

    def parcel(h, at, b, dev):
        return remote(grads.at[b, h], grads.at[b, h], ag_send.at[h, at], ag_recv.at[h, at], dev)

    def twin(at, b):
        return remote(grads.at[b], grads.at[b], twin_send.at[at], twin_recv.at[at], partner)

    first = [1]
    for a in axes:
        first.append(first[-1] + sizes[a] - 1)
    last = first[3]
    mine = pl.ds(pl.multiple_of(core * half, 8), half)
    theirs = pl.ds(pl.multiple_of((1 - core) * half, 8), half)

    def gram_pair(t, src):
        return remote(src.at[theirs], gmail.at[t, 0], gram_send.at[t, 0], gram_recv.at[t, 0], partner)

    def gram_line(t, a, k):
        at = first[a] + k - 1
        return remote(
            gsum.at[t, a], gmail.at[t, at], gram_send.at[t, at], gram_recv.at[t, at], device(ahead(only(a, k)), core)
        )

    def gram_final(t):
        return remote(gsum.at[t, 3], gfull.at[t, mine], gram_send.at[t, last], gram_recv.at[t, last], partner)

    def gram_open(t, src):
        gram_pair(t, src).start()

    def gram_send_line(t, a):
        for k in range(1, sizes[a]):
            gram_line(t, a, k).start()

    def gram_step(t, src, stage):
        if stage == 0:
            gram_pair(t, src).wait_recv()
            gsum[t, 0] = src[mine, :] + gmail[t, 0]
        elif stage <= 3:
            a = stage - 1
            total = gsum[t, a]
            for k in range(1, sizes[a]):
                gram_line(t, a, k).wait_recv()
                total = total + gmail[t, first[a] + k - 1]
            gsum[t, a + 1] = total
        else:
            gram_final(t).wait_recv()
        if stage < 3:
            gram_send_line(t, stage)
        elif stage == 3:
            gram_final(t).start()
            gfull[t, mine] = gsum[t, 3]

    def gram_drain(t, src):
        gram_pair(t, src).wait_send()
        for a in axes:
            for k in range(1, sizes[a]):
                gram_line(t, a, k).wait_send()
        gram_final(t).wait_send()

    codes_to = lax.broadcasted_iota(i32, (2 * users_dev, capacity), 0)

    def gather(b, j, at):
        base = b * capacity

        def some(s, _):
            start = base + s * unroll
            for k in range(unroll):
                r = rows_ref.at[pl.ds(k, rows_ref.shape[0] - unroll + 1)][start]
                picked[pl.ds(s * unroll + k, 1), :] = table_ref[pl.ds(r, 1), :]
            return 0

        lax.fori_loop(0, capacity // unroll, some, 0)
        x = picked[...]
        hi, lo = split2(x)
        hot = (hot_ref[b] == codes_to).astype(f32).astype(bf16)
        both = jnp.dot(hot, jnp.concatenate([hi, lo], axis=1), preferred_element_type=f32)
        out = both[:, :width] + both[:, width:]
        part[j, at, 0] = out[:users_dev]
        part[j, at, 1] = out[users_dev:]

    def arrive(h, r, a):
        at = slot(r)
        for k in range(1, sizes[a]):
            m = slot(add(r, a, k))
            letter(h, m, partner).wait_recv()
            part[1, at, h] = part[1, at, h] + mail[h, m]

    def leave(h, r, a):
        @pl.when(r[a] != 0)
        def _():
            chip = tuple(lax.rem(p + r[a], n) if b == a else p for b, (p, n) in enumerate(zip(pos, sizes)))
            letter(h, slot(r), device(chip, core)).start()

    gram_open(0, gram_ref)

    def reduce_step(i, _):
        for stage in range(4):
            j = i - LAGS[stage]

            @pl.when(jnp.logical_and(j >= 0, j < plane))
            def _():
                r = ranked(plane - 1 - j, (2, 0, 1))
                at = slot(r)
                if stage == 0:
                    pair_copy(at).wait_recv()
                    for h in range(2):
                        part[1, at, h] = part[1, at, h] + pair[at, h]
                        leave(h, r, ORDERS[h][0])
                else:
                    for h in range(2):
                        order = ORDERS[h]
                        clear = r[order[0]] == 0
                        for a in order[1:stage]:
                            clear = jnp.logical_and(clear, r[a] == 0)

                        @pl.when(clear)
                        def _():
                            arrive(h, r, order[stage - 1])
                            if stage < 3:
                                leave(h, r, order[stage])

        for stage in range(5):
            @pl.when(i == 2 * stage + 2)
            def _():
                gram_step(0, gram_ref, stage)

        @pl.when(i < plane)
        def _():
            r = ranked(plane - 1 - i, (2, 0, 1))
            at = slot(r)
            chip = ahead(r)

            def one(j, _):
                c = (1 - core) * (1 - j) + core * j
                gather(block(chip, c), j, at)

                @pl.when(j == 0)
                def _():
                    pair_copy(at).start()

                return 0

            lax.fori_loop(0, 2, one, 0)

        return 0

    lax.fori_loop(0, plane + LAGS[3], reduce_step, 0)

    me = block(pos, core)
    uv = part[1, 0, 0] / hist_len
    pv = part[1, 0, 1]
    gap = jnp.sum(uv * pv, axis=1, keepdims=True) - 1.0
    ug = 2.0 * gap * pv + 2.0 * coef * jnp.dot(uv, gfull[0], precision=HIGHEST, preferred_element_type=f32)
    grads[me, 0] = ug / hist_len
    grads[me, 1] = 2.0 * gap * uv

    def forward(h, o, b, a):
        for k in range(1, sizes[a]):
            chip = tuple(lax.rem(p + k, n) if c == a else p for c, (p, n) in enumerate(zip(pos, sizes)))
            parcel(h, slot(add(o, a, k)), b, device(chip, core)).start()

    ways = tuple(order[::-1] for order in ORDERS)
    for a in range(3):
        for h in range(2):
            forward(h, origin, me, ways[h][a])
    twin(0, me).start()
    upart[...] = lax.dot_general(
        uv, uv, (((0,), (0,)), ((), ())), precision=HIGHEST, preferred_element_type=f32
    )
    gram_open(1, upart)
    cur[pl.ds(2 * users_dev, 8), :] = jnp.zeros((8, width), f32)

    def vals_copy(v, b):
        return pltpu.make_async_copy(vbuf.at[v], vals_ref.at[b], vsem.at[v])

    def vals(n, kind, b):
        v = 2 * kind + lax.rem(n, 2)

        @pl.when(n >= 2)
        def _():
            vals_copy(v, b).wait()

        cur[pl.ds(0, users_dev), :] = grads[b, 0]
        cur[pl.ds(users_dev, users_dev), :] = grads[b, 1]
        base = b * capacity

        def some(s, _):
            start = base + s * unroll
            for k in range(unroll):
                c = codes_ref.at[pl.ds(k, codes_ref.shape[0] - unroll + 1)][start]
                vbuf[v, pl.ds(s * unroll + k, 1), :] = cur[pl.ds(c, 1), :]
            return 0

        lax.fori_loop(0, capacity // unroll, some, 0)
        vals_copy(v, b).start()

    seqs = tuple(way[::-1] for way in ways)

    def rank(o, digits):
        n = 0
        for a in digits:
            n = n * sizes[a] + o[a]
        return n

    chips = [(x, y, z) for x in range(nx) for y in range(ny) for z in range(nz)]
    lag = 1 + max(rank(o, seqs[h]) - rank(o, seqs[0]) for o in chips for h in range(2))

    def spread(n, _):
        def one(kind, _):
            j = n - lag - TWIN_LAG * kind

            @pl.when(jnp.logical_and(j >= 0, j < plane))
            def _():
                o = ranked(j, seqs[0])
                at = slot(o)
                b = block(behind(o), core + kind * (1 - 2 * core))

                @pl.when(jnp.logical_and(kind == 0, j > 0))
                def _():
                    twin(at, b).start()

                @pl.when(kind == 1)
                def _():
                    twin(at, b).wait_recv()

                vals(j, kind, b)

            return 0

        lax.fori_loop(0, 2, one, 0)

        @pl.when(jnp.logical_and(n > 0, n < plane))
        def _():
            for h in range(2):
                a1, a2, a3 = ways[h]
                o = ranked(n, seqs[h])
                b = block(behind(o), core)
                parcel(h, slot(o), b, partner).wait_recv()

                @pl.when(o[a3] == 0)
                def _():
                    @pl.when(o[a2] == 0)
                    def _():
                        forward(h, o, b, a2)

                    forward(h, o, b, a3)

        for stage in range(5):
            @pl.when(n == 2 * stage + 2)
            def _():
                gram_step(1, upart, stage)

        return 0

    lax.fori_loop(0, plane + lag + TWIN_LAG, spread, 0)
    ugram_ref[...] = gfull[1]

    def drain(n):
        pair_copy(n).wait_send()
        twin(n, me).wait_send()

    each(0, plane, drain)

    def drain_mail(n):
        for h in range(2):
            letter(h, n, partner).wait_send()
            parcel(h, n, me, partner).wait_send()

    each(1, plane, drain_mail)
    gram_drain(0, gram_ref)
    gram_drain(1, upart)
    each(0, VSLOTS, lambda v: vals_copy(v, me).wait())


def scatter_kernel(
    coef, chunk, unroll, tile,
    rows_ref, vals_ref, ugram_ref, table_ref, state_ref, new_table_ref, new_state_ref,
    vbuf, table, state, vsem, in_sem, out_sem, *accs,
):
    entries = rows_ref.shape[0]
    chunks = entries // chunk
    part = chunk // len(accs)
    rows_dev, width = table.shape
    tiles = rows_dev // tile

    def vals_copy(n):
        s = lax.rem(n, 2)
        return pltpu.make_async_copy(
            vals_ref.at[pl.ds(pl.multiple_of(n * chunk, 8), chunk)], vbuf.at[s], vsem.at[s]
        )

    table_copy = pltpu.make_async_copy(table_ref, table, in_sem.at[0])
    state_copy = pltpu.make_async_copy(state_ref, state, in_sem.at[1])
    vals_copy(0).start()
    vals_copy(1).start()
    table_copy.start()
    state_copy.start()
    for acc in accs:
        acc[...] = jnp.zeros_like(acc)

    def one(n, _):
        v = lax.rem(n, 2)
        vals_copy(n).wait()

        def scatter(s, _):
            start = n * chunk + s * unroll
            for q in range(unroll):
                rows = [
                    rows_ref.at[pl.ds(k * part + q, entries - chunk + part - unroll + 1)][start] for k in range(len(accs))
                ]
                news = [
                    acc[pl.ds(r, 1), :] + vbuf[v, pl.ds(s * unroll + (k * part + q), 1), :]
                    for k, (acc, r) in enumerate(zip(accs, rows))
                ]
                for acc, r, new in zip(accs, rows, news):
                    acc[pl.ds(r, 1), :] = new
            return 0

        lax.fori_loop(0, part // unroll, scatter, 0)

        @pl.when(n + 2 < chunks)
        def _():
            vals_copy(n + 2).start()

        return 0

    lax.fori_loop(0, chunks, one, 0)
    table_copy.wait()
    state_copy.wait()
    u0, u1 = split2(ugram_ref[...])
    u00 = jnp.concatenate([u0, u0], axis=0)

    def out_copy(t, which):
        at = pl.ds(pl.multiple_of(t * tile, 8), tile)
        src, dst = ((table, new_table_ref), (state, new_state_ref))[which]
        return pltpu.make_async_copy(src.at[at], dst.at[at], out_sem.at[which, t])

    def finish(t, _):
        at = pl.ds(pl.multiple_of(t * tile, 8), tile)
        item = table[at, :]
        t0, t1 = split2(item)
        g = jnp.dot(jnp.concatenate([t0, t1], axis=1), u00, preferred_element_type=f32)
        g = 2.0 * coef * (g + jnp.dot(t0, u1, preferred_element_type=f32))
        add = accs[0][at, :]
        for acc in accs[1:]:
            add = add + acc[at, :]
        g = g + add
        new = state[at, :] + g * g
        state[at, :] = new
        table[at, :] = item - step_size * g / jnp.sqrt(new)
        out_copy(t, 0).start()
        out_copy(t, 1).start()
        return 0

    lax.fori_loop(0, tiles, finish, 0)

    def drain(t, _):
        out_copy(t, 0).wait()
        out_copy(t, 1).wait()
        return 0

    lax.fori_loop(0, tiles, drain, 0)


VM = pl.BlockSpec(memory_space=pltpu.VMEM)
HB = pl.BlockSpec(memory_space=pl.ANY)
SM = pl.BlockSpec(memory_space=pltpu.SMEM)
PARAMS = pltpu.CompilerParams(vmem_limit_bytes=60 * 1024 * 1024)


def shards(item_table, adagrad_state, history_ids, positive_ids):
    rows_dev, width = item_table.shape
    users_dev, hist_len = history_ids.shape
    devices = lax.axis_size("dp") * lax.axis_size("rows")
    groups = 2 * users_dev
    count = users_dev * (hist_len + 1)
    capacity = max(8, (count * 5 // (2 * devices) + 7) // 8 * 8)
    block = 512
    padded = round_up(count, block)
    requests = jnp.concatenate([history_ids.reshape(-1), positive_ids])
    code = jnp.concatenate(
        [jnp.arange(users_dev * hist_len, dtype=i32) // hist_len, users_dev + jnp.arange(users_dev, dtype=i32)]
    )
    requests = jnp.pad(requests, (0, padded - count), constant_values=devices * rows_dev)
    code = jnp.pad(code, (0, padded - count))
    owner = requests // rows_dev
    local = requests - owner * rows_dev

    lists = pl.pallas_call(
        functools.partial(route_kernel, devices, capacity, users_dev, block),
        out_shape=jax.ShapeDtypeStruct((2, devices, capacity), i32),
        in_specs=[VM] * 3,
        out_specs=VM,
        scratch_shapes=[pltpu.VMEM((4 * devices, capacity), f32)],
        compiler_params=PARAMS,
        name="route",
    )(owner[None], local[None], code[None])
    asked = lax.all_to_all(lists, ("dp", "rows"), split_axis=1, concat_axis=1, tiled=True)
    rows = asked[0].reshape(-1)
    codes = asked[1]
    entries = devices * capacity
    item_gram = jnp.dot(item_table.T, item_table, precision=HIGHEST, preferred_element_type=f32)
    data, shard = lax.axis_size("dp"), lax.axis_size("rows")
    sizes = line_sizes(data, shard)
    plane = devices // 2
    lines = sum(sizes) - 1
    unroll = max(n for n in (8, 16, 32, 64, 128) if capacity % n == 0)
    coef = penalty_weight / (rows_dev * devices)
    dma = pltpu.SemaphoreType.DMA
    vals, user_gram = pl.pallas_call(
        functools.partial(exchange_kernel, sizes, capacity, users_dev, hist_len, coef, unroll),
        out_shape=(
            jax.ShapeDtypeStruct((devices, capacity, width), f32),
            jax.ShapeDtypeStruct((width, width), f32),
        ),
        in_specs=[SM, SM, VM, VM, VM],
        out_specs=(HB, VM),
        scratch_shapes=[
            pltpu.VMEM((capacity, width), f32),
            pltpu.VMEM((2, plane, 2, users_dev, width), f32),
            pltpu.VMEM((plane, 2, users_dev, width), f32),
            pltpu.VMEM((2, plane, users_dev, width), f32),
            pltpu.VMEM((devices, 2, users_dev, width), f32),
            pltpu.VMEM((groups + 8, width), f32),
            pltpu.VMEM((VSLOTS, capacity, width), f32),
            pltpu.VMEM((width, width), f32),
            pltpu.VMEM((2, 4, width // 2, width), f32),
            pltpu.VMEM((2, lines, width // 2, width), f32),
            pltpu.VMEM((2, width, width), f32),
            dma((plane,)),
            dma((plane,)),
            dma((2, plane)),
            dma((2, plane)),
            dma((2, plane)),
            dma((2, plane)),
            dma((plane,)),
            dma((plane,)),
            dma((2, lines)),
            dma((2, lines)),
            dma((VSLOTS,)),
        ],
        compiler_params=pltpu.CompilerParams(
            vmem_limit_bytes=60 * 1024 * 1024, collective_id=0, has_side_effects=True
        ),
        name="exchange",
    )(rows, codes.reshape(-1), codes[:, None, :], item_gram, item_table)
    chunk, tile = min(2048, entries), 256
    return pl.pallas_call(
        functools.partial(scatter_kernel, coef, chunk, 4, tile),
        out_shape=(
            jax.ShapeDtypeStruct(item_table.shape, f32),
            jax.ShapeDtypeStruct(item_table.shape, f32),
        ),
        in_specs=[SM, HB, VM, HB, HB],
        out_specs=(HB, HB),
        scratch_shapes=[
            pltpu.VMEM((2, chunk, width), f32),
            pltpu.VMEM((rows_dev, width), f32),
            pltpu.VMEM((rows_dev, width), f32),
            dma((2,)),
            dma((2,)),
            dma((2, rows_dev // tile)),
        ]
        + [pltpu.VMEM((rows_dev, width), f32)] * STREAMS,
        compiler_params=PARAMS,
        name="scatter",
    )(rows, vals.reshape(entries, width), user_gram, item_table, adagrad_state)


def solution(mesh):
    return jax.shard_map(
        shards,
        mesh=mesh,
        in_specs=(
            P(("dp", "rows"), None),
            P(("dp", "rows"), None),
            P(("dp", "rows"), None),
            P(("dp", "rows")),
        ),
        out_specs=(P(("dp", "rows"), None), P(("dp", "rows"), None)),
        check_vma=False,
    )
```

```python
import functools

import jax
import jax.numpy as jnp
from jax import lax
from jax.experimental import pallas as pl
from jax.experimental.pallas import tpu as pltpu
from jax.sharding import PartitionSpec as P

penalty_weight = 10.0
step_size = 0.05
LOW = 128
STREAMS = 8
HIGHEST = lax.Precision.HIGHEST
f32, bf16, i32 = jnp.float32, jnp.bfloat16, jnp.int32


def round_up(value, unit):
    return (value + unit - 1) // unit * unit


def route_kernel(devices, capacity, users_dev, block, owner_ref, local_ref, code_ref, out_ref, acc):
    blocks = owner_ref.shape[1] // block
    upper = (
        lax.broadcasted_iota(i32, (block, block), 0) <= lax.broadcasted_iota(i32, (block, block), 1)
    ).astype(bf16)
    owners = lax.broadcasted_iota(i32, (devices, block), 0)
    ranks_to = lax.broadcasted_iota(i32, (capacity, block), 0)
    acc[...] = jnp.zeros_like(acc)
    carry = jnp.zeros((devices, 1), f32)
    for j in range(blocks):
        cols = slice(j * block, (j + 1) * block)
        local = local_ref[:, cols]
        high = (local // LOW).astype(f32)
        low = (local % LOW).astype(f32)
        code = code_ref[:, cols].astype(f32)
        member = (owner_ref[:, cols] == owners).astype(f32)
        prefix = jnp.dot(member.astype(bf16), upper, preferred_element_type=f32)
        rank = jnp.sum(member * (prefix + carry), axis=0, keepdims=True) - 1.0
        carry = carry + jnp.sum(member, axis=1, keepdims=True)
        left = jnp.concatenate(
            [member * high, member * low, member * code, member], axis=0
        ).astype(bf16)
        right = (rank.astype(i32) == ranks_to).astype(f32).astype(bf16)
        acc[...] += lax.dot_general(
            left, right, (((1,), (1,)), ((), ())), preferred_element_type=f32
        )
    row = acc[0:devices] * LOW + acc[devices : 2 * devices]
    code = acc[2 * devices : 3 * devices]
    present = acc[3 * devices : 4 * devices]
    empty = 2 * users_dev
    out_ref[0] = row.astype(i32)
    out_ref[1] = jnp.where(present > 0.5, code, float(empty)).astype(i32)


def split2(x):
    hi = x.astype(bf16)
    return hi, (x - hi.astype(f32)).astype(bf16)


def line_sizes(data, shard):
    cols = max(n for n in range(1, shard + 1) if shard % n == 0 and n * n <= shard)
    return data // 2, cols, shard // cols


ORDERS = ((0, 1, 2), (1, 0, 2))
LAGS = (2, 4, 6, 8)
VSLOTS = 4
TWIN_LAG = 2


def exchange_kernel(
    sizes, capacity, users_dev, hist_len, coef, unroll,
    rows_ref, codes_ref, hot_ref, gram_ref, table_ref, vals_ref, ugram_ref,
    picked, part, pair, mail, grads, cur, vbuf, upart, gsum, gmail, gfull,
    pair_send, pair_recv, mail_send, mail_recv, ag_send, ag_recv, twin_send, twin_recv, gram_send, gram_recv, vsem,
):
    nx, ny, nz = sizes
    plane = nx * ny * nz
    shard = ny * nz
    width = table_ref.shape[1]
    half = width // 2
    dp, rw = lax.axis_index("dp"), lax.axis_index("rows")
    core = lax.rem(dp, 2)
    pos = (dp // 2, lax.rem(rw, ny), rw // ny)
    origin = (0, 0, 0)
    axes = (0, 1, 2)

    def device(chip, c):
        return chip[0] * 2 + c, chip[2] * ny + chip[1]

    def block(chip, c):
        d, r = device(chip, c)
        return d * shard + r

    def ahead(r):
        return tuple(lax.rem(p + k, n) for p, k, n in zip(pos, r, sizes))

    def behind(o):
        return tuple(lax.rem(p - k + n, n) for p, k, n in zip(pos, o, sizes))

    def only(a, k):
        return tuple(k if b == a else 0 for b in axes)

    def add(r, a, k):
        return tuple(v + k if b == a else v for b, v in enumerate(r))

    def slot(r):
        return (r[0] * ny + r[1]) * nz + r[2]

    def ranked(n, digits):
        out = [0, 0, 0]
        for a in reversed(digits):
            out[a] = lax.rem(n, sizes[a])
            n = n // sizes[a]
        return tuple(out)

    partner = device(pos, 1 - core)

    def remote(src, dst, send, recv, dev):
        return pltpu.make_async_remote_copy(
            src_ref=src, dst_ref=dst, send_sem=send, recv_sem=recv,
            device_id=dev, device_id_type=pl.DeviceIdType.MESH,
        )

    def each(first, count, act):
        def step(k, _):
            act(k)
            return 0

        lax.fori_loop(first, count, step, 0)

    barrier = pltpu.get_barrier_semaphore()
    greeted = 1
    pl.semaphore_signal(barrier, inc=1, device_id=partner, device_id_type=pl.DeviceIdType.MESH)
    for a in axes:
        for k in range(1, sizes[a]):
            greeted += 1
            pl.semaphore_signal(
                barrier, inc=1, device_id=device(ahead(only(a, k)), core), device_id_type=pl.DeviceIdType.MESH
            )
    pl.semaphore_wait(barrier, greeted)

    def pair_copy(at):
        return remote(part.at[0, at], pair.at[at], pair_send.at[at], pair_recv.at[at], partner)

    def letter(h, at, dev):
        return remote(part.at[1, at, h], mail.at[h, at], mail_send.at[h, at], mail_recv.at[h, at], dev)

    def parcel(h, at, b, dev):
        return remote(grads.at[b, h], grads.at[b, h], ag_send.at[h, at], ag_recv.at[h, at], dev)

    def twin(at, b):
        return remote(grads.at[b], grads.at[b], twin_send.at[at], twin_recv.at[at], partner)

    first = [1]
    for a in axes:
        first.append(first[-1] + sizes[a] - 1)
    last = first[3]
    mine = pl.ds(pl.multiple_of(core * half, 8), half)
    theirs = pl.ds(pl.multiple_of((1 - core) * half, 8), half)

    def gram_pair(t, src):
        return remote(src.at[theirs], gmail.at[t, 0], gram_send.at[t, 0], gram_recv.at[t, 0], partner)

    def gram_line(t, a, k):
        at = first[a] + k - 1
        return remote(
            gsum.at[t, a], gmail.at[t, at], gram_send.at[t, at], gram_recv.at[t, at], device(ahead(only(a, k)), core)
        )

    def gram_final(t):
        return remote(gsum.at[t, 3], gfull.at[t, mine], gram_send.at[t, last], gram_recv.at[t, last], partner)

    def gram_open(t, src):
        gram_pair(t, src).start()

    def gram_send_line(t, a):
        for k in range(1, sizes[a]):
            gram_line(t, a, k).start()

    def gram_step(t, src, stage):
        if stage == 0:
            gram_pair(t, src).wait_recv()
            gsum[t, 0] = src[mine, :] + gmail[t, 0]
        elif stage <= 3:
            a = stage - 1
            total = gsum[t, a]
            for k in range(1, sizes[a]):
                gram_line(t, a, k).wait_recv()
                total = total + gmail[t, first[a] + k - 1]
            gsum[t, a + 1] = total
        else:
            gram_final(t).wait_recv()
        if stage < 3:
            gram_send_line(t, stage)
        elif stage == 3:
            gram_final(t).start()
            gfull[t, mine] = gsum[t, 3]

    def gram_drain(t, src):
        gram_pair(t, src).wait_send()
        for a in axes:
            for k in range(1, sizes[a]):
                gram_line(t, a, k).wait_send()
        gram_final(t).wait_send()

    codes_to = lax.broadcasted_iota(i32, (2 * users_dev, capacity), 0)

    def gather(b, j, at):
        base = b * capacity

        def some(s, _):
            start = base + s * unroll
            for k in range(unroll):
                r = rows_ref.at[pl.ds(k, rows_ref.shape[0] - unroll + 1)][start]
                picked[pl.ds(s * unroll + k, 1), :] = table_ref[pl.ds(r, 1), :]
            return 0

        lax.fori_loop(0, capacity // unroll, some, 0)
        x = picked[...]
        hi, lo = split2(x)
        hot = (hot_ref[b] == codes_to).astype(f32).astype(bf16)
        both = jnp.dot(hot, jnp.concatenate([hi, lo], axis=1), preferred_element_type=f32)
        out = both[:, :width] + both[:, width:]
        part[j, at, 0] = out[:users_dev]
        part[j, at, 1] = out[users_dev:]

    def arrive(h, r, a):
        at = slot(r)
        for k in range(1, sizes[a]):
            m = slot(add(r, a, k))
            letter(h, m, partner).wait_recv()
            part[1, at, h] = part[1, at, h] + mail[h, m]

    def leave(h, r, a):
        @pl.when(r[a] != 0)
        def _():
            chip = tuple(lax.rem(p + r[a], n) if b == a else p for b, (p, n) in enumerate(zip(pos, sizes)))
            letter(h, slot(r), device(chip, core)).start()

    gram_open(0, gram_ref)

    def reduce_step(i, _):
        for stage in range(4):
            j = i - LAGS[stage]

            @pl.when(jnp.logical_and(j >= 0, j < plane))
            def _():
                r = ranked(plane - 1 - j, (2, 0, 1))
                at = slot(r)
                if stage == 0:
                    pair_copy(at).wait_recv()
                    for h in range(2):
                        part[1, at, h] = part[1, at, h] + pair[at, h]
                        leave(h, r, ORDERS[h][0])
                else:
                    for h in range(2):
                        order = ORDERS[h]
                        clear = r[order[0]] == 0
                        for a in order[1:stage]:
                            clear = jnp.logical_and(clear, r[a] == 0)

                        @pl.when(clear)
                        def _():
                            arrive(h, r, order[stage - 1])
                            if stage < 3:
                                leave(h, r, order[stage])

        for stage in range(5):
            @pl.when(i == 3 * stage + 3)
            def _():
                gram_step(0, gram_ref, stage)

        @pl.when(i < plane)
        def _():
            r = ranked(plane - 1 - i, (2, 0, 1))
            at = slot(r)
            chip = ahead(r)

            def one(j, _):
                c = (1 - core) * (1 - j) + core * j
                gather(block(chip, c), j, at)

                @pl.when(j == 0)
                def _():
                    pair_copy(at).start()

                return 0

            lax.fori_loop(0, 2, one, 0)

        return 0

    lax.fori_loop(0, plane + LAGS[3], reduce_step, 0)

    me = block(pos, core)
    uv = part[1, 0, 0] / hist_len
    pv = part[1, 0, 1]
    gap = jnp.sum(uv * pv, axis=1, keepdims=True) - 1.0
    ug = 2.0 * gap * pv + 2.0 * coef * jnp.dot(uv, gfull[0], precision=HIGHEST, preferred_element_type=f32)
    grads[me, 0] = ug / hist_len
    grads[me, 1] = 2.0 * gap * uv

    def forward(h, o, b, a):
        for k in range(1, sizes[a]):
            chip = tuple(lax.rem(p + k, n) if c == a else p for c, (p, n) in enumerate(zip(pos, sizes)))
            parcel(h, slot(add(o, a, k)), b, device(chip, core)).start()

    ways = tuple(order[::-1] for order in ORDERS)
    line = ways[0][0]
    for k in range(1, sizes[line]):
        for h in range(2):
            parcel(h, slot(only(line, k)), me, device(ahead(only(line, k)), core)).start()
    for a in (1, 2):
        for h in range(2):
            forward(h, origin, me, ways[h][a])
    twin(0, me).start()
    upart[...] = lax.dot_general(
        uv, uv, (((0,), (0,)), ((), ())), precision=HIGHEST, preferred_element_type=f32
    )
    gram_open(1, upart)
    cur[pl.ds(2 * users_dev, 8), :] = jnp.zeros((8, width), f32)

    def vals_copy(v, b):
        return pltpu.make_async_copy(vbuf.at[v], vals_ref.at[b], vsem.at[v])

    def vals(n, kind, b):
        v = 2 * kind + lax.rem(n, 2)

        @pl.when(n >= 2)
        def _():
            vals_copy(v, b).wait()

        cur[pl.ds(0, users_dev), :] = grads[b, 0]
        cur[pl.ds(users_dev, users_dev), :] = grads[b, 1]
        base = b * capacity

        def some(s, _):
            start = base + s * unroll
            for k in range(unroll):
                c = codes_ref.at[pl.ds(k, codes_ref.shape[0] - unroll + 1)][start]
                vbuf[v, pl.ds(s * unroll + k, 1), :] = cur[pl.ds(c, 1), :]
            return 0

        lax.fori_loop(0, capacity // unroll, some, 0)
        vals_copy(v, b).start()

    digits = ((2, 0, 1), (2, 1, 0))
    delays = (-nx * ny, 1, 3)
    vals_delay = delays[2] + 1

    def spread(n, _):
        for h in range(2):
            a1, a2, a3 = ways[h]
            for level in (1, 2, 3):
                q = n - delays[level - 1]
                o = ranked(q, digits[h])
                if level == 1:
                    here = jnp.logical_and(o[a1] != 0, jnp.logical_and(o[a2] == 0, o[a3] == 0))
                elif level == 2:
                    here = jnp.logical_and(o[a2] != 0, o[a3] == 0)
                else:
                    here = o[a3] != 0

                @pl.when(jnp.logical_and(jnp.logical_and(q >= 0, q < plane), here))
                def _():
                    b = block(behind(o), core)
                    parcel(h, slot(o), b, partner).wait_recv()
                    for a in ways[h][level:]:
                        forward(h, o, b, a)

        def one(kind, _):
            j = n - vals_delay - TWIN_LAG * kind

            @pl.when(jnp.logical_and(j >= 0, j < plane))
            def _():
                o = ranked(j, digits[0])
                at = slot(o)
                b = block(behind(o), core + kind * (1 - 2 * core))

                @pl.when(jnp.logical_and(kind == 0, j > 0))
                def _():
                    twin(at, b).start()

                @pl.when(kind == 1)
                def _():
                    twin(at, b).wait_recv()

                vals(j, kind, b)

            return 0

        lax.fori_loop(0, 2, one, 0)

        for stage in range(5):
            @pl.when(n == 4 * stage + 3)
            def _():
                gram_step(1, upart, stage)

        return 0

    lax.fori_loop(0, plane + vals_delay + TWIN_LAG, spread, 0)
    ugram_ref[...] = gfull[1]

    def drain(n):
        pair_copy(n).wait_send()
        twin(n, me).wait_send()

    each(0, plane, drain)

    def drain_mail(n):
        for h in range(2):
            letter(h, n, partner).wait_send()
            parcel(h, n, me, partner).wait_send()

    each(1, plane, drain_mail)
    gram_drain(0, gram_ref)
    gram_drain(1, upart)
    each(0, VSLOTS, lambda v: vals_copy(v, me).wait())


def scatter_kernel(
    coef, chunk, unroll, tile,
    rows_ref, vals_ref, ugram_ref, table_ref, state_ref, new_table_ref, new_state_ref,
    vbuf, table, state, vsem, in_sem, out_sem, *accs,
):
    entries = rows_ref.shape[0]
    chunks = entries // chunk
    part = chunk // len(accs)
    rows_dev, width = table.shape
    tiles = rows_dev // tile

    def vals_copy(n):
        s = lax.rem(n, 2)
        return pltpu.make_async_copy(
            vals_ref.at[pl.ds(pl.multiple_of(n * chunk, 8), chunk)], vbuf.at[s], vsem.at[s]
        )

    table_copy = pltpu.make_async_copy(table_ref, table, in_sem.at[0])
    state_copy = pltpu.make_async_copy(state_ref, state, in_sem.at[1])
    vals_copy(0).start()
    vals_copy(1).start()
    table_copy.start()
    state_copy.start()
    for acc in accs:
        acc[...] = jnp.zeros_like(acc)

    def one(n, _):
        v = lax.rem(n, 2)
        vals_copy(n).wait()

        def scatter(s, _):
            start = n * chunk + s * unroll
            for q in range(unroll):
                rows = [
                    rows_ref.at[pl.ds(k * part + q, entries - chunk + part - unroll + 1)][start] for k in range(len(accs))
                ]
                news = [
                    acc[pl.ds(r, 1), :] + vbuf[v, pl.ds(s * unroll + (k * part + q), 1), :]
                    for k, (acc, r) in enumerate(zip(accs, rows))
                ]
                for acc, r, new in zip(accs, rows, news):
                    acc[pl.ds(r, 1), :] = new
            return 0

        lax.fori_loop(0, part // unroll, scatter, 0)

        @pl.when(n + 2 < chunks)
        def _():
            vals_copy(n + 2).start()

        return 0

    lax.fori_loop(0, chunks, one, 0)
    table_copy.wait()
    state_copy.wait()
    u0, u1 = split2(ugram_ref[...])
    u00 = jnp.concatenate([u0, u0], axis=0)

    def out_copy(t, which):
        at = pl.ds(pl.multiple_of(t * tile, 8), tile)
        src, dst = ((table, new_table_ref), (state, new_state_ref))[which]
        return pltpu.make_async_copy(src.at[at], dst.at[at], out_sem.at[which, t])

    def finish(t, _):
        at = pl.ds(pl.multiple_of(t * tile, 8), tile)
        item = table[at, :]
        t0, t1 = split2(item)
        g = jnp.dot(jnp.concatenate([t0, t1], axis=1), u00, preferred_element_type=f32)
        g = 2.0 * coef * (g + jnp.dot(t0, u1, preferred_element_type=f32))
        add = accs[0][at, :]
        for acc in accs[1:]:
            add = add + acc[at, :]
        g = g + add
        new = state[at, :] + g * g
        state[at, :] = new
        table[at, :] = item - step_size * g / jnp.sqrt(new)
        out_copy(t, 0).start()
        out_copy(t, 1).start()
        return 0

    lax.fori_loop(0, tiles, finish, 0)

    def drain(t, _):
        out_copy(t, 0).wait()
        out_copy(t, 1).wait()
        return 0

    lax.fori_loop(0, tiles, drain, 0)


VM = pl.BlockSpec(memory_space=pltpu.VMEM)
HB = pl.BlockSpec(memory_space=pl.ANY)
SM = pl.BlockSpec(memory_space=pltpu.SMEM)
PARAMS = pltpu.CompilerParams(vmem_limit_bytes=60 * 1024 * 1024)


def shards(item_table, adagrad_state, history_ids, positive_ids):
    rows_dev, width = item_table.shape
    users_dev, hist_len = history_ids.shape
    devices = lax.axis_size("dp") * lax.axis_size("rows")
    groups = 2 * users_dev
    count = users_dev * (hist_len + 1)
    capacity = max(8, (count * 5 // (2 * devices) + 7) // 8 * 8)
    block = 512
    padded = round_up(count, block)
    requests = jnp.concatenate([history_ids.reshape(-1), positive_ids])
    code = jnp.concatenate(
        [jnp.arange(users_dev * hist_len, dtype=i32) // hist_len, users_dev + jnp.arange(users_dev, dtype=i32)]
    )
    requests = jnp.pad(requests, (0, padded - count), constant_values=devices * rows_dev)
    code = jnp.pad(code, (0, padded - count))
    owner = requests // rows_dev
    local = requests - owner * rows_dev

    lists = pl.pallas_call(
        functools.partial(route_kernel, devices, capacity, users_dev, block),
        out_shape=jax.ShapeDtypeStruct((2, devices, capacity), i32),
        in_specs=[VM] * 3,
        out_specs=VM,
        scratch_shapes=[pltpu.VMEM((4 * devices, capacity), f32)],
        compiler_params=PARAMS,
        name="route",
    )(owner[None], local[None], code[None])
    asked = lax.all_to_all(lists, ("dp", "rows"), split_axis=1, concat_axis=1, tiled=True)
    rows = asked[0].reshape(-1)
    codes = asked[1]
    entries = devices * capacity
    item_gram = jnp.dot(item_table.T, item_table, precision=HIGHEST, preferred_element_type=f32)
    data, shard = lax.axis_size("dp"), lax.axis_size("rows")
    sizes = line_sizes(data, shard)
    plane = devices // 2
    lines = sum(sizes) - 1
    unroll = max(n for n in (8, 16, 32, 64, 128) if capacity % n == 0)
    coef = penalty_weight / (rows_dev * devices)
    dma = pltpu.SemaphoreType.DMA
    vals, user_gram = pl.pallas_call(
        functools.partial(exchange_kernel, sizes, capacity, users_dev, hist_len, coef, unroll),
        out_shape=(
            jax.ShapeDtypeStruct((devices, capacity, width), f32),
            jax.ShapeDtypeStruct((width, width), f32),
        ),
        in_specs=[SM, SM, VM, VM, VM],
        out_specs=(HB, VM),
        scratch_shapes=[
            pltpu.VMEM((capacity, width), f32),
            pltpu.VMEM((2, plane, 2, users_dev, width), f32),
            pltpu.VMEM((plane, 2, users_dev, width), f32),
            pltpu.VMEM((2, plane, users_dev, width), f32),
            pltpu.VMEM((devices, 2, users_dev, width), f32),
            pltpu.VMEM((groups + 8, width), f32),
            pltpu.VMEM((VSLOTS, capacity, width), f32),
            pltpu.VMEM((width, width), f32),
            pltpu.VMEM((2, 4, width // 2, width), f32),
            pltpu.VMEM((2, lines, width // 2, width), f32),
            pltpu.VMEM((2, width, width), f32),
            dma((plane,)),
            dma((plane,)),
            dma((2, plane)),
            dma((2, plane)),
            dma((2, plane)),
            dma((2, plane)),
            dma((plane,)),
            dma((plane,)),
            dma((2, lines)),
            dma((2, lines)),
            dma((VSLOTS,)),
        ],
        compiler_params=pltpu.CompilerParams(
            vmem_limit_bytes=60 * 1024 * 1024, collective_id=0, has_side_effects=True
        ),
        name="exchange",
    )(rows, codes.reshape(-1), codes[:, None, :], item_gram, item_table)
    chunk, tile = min(2048, entries), 256
    return pl.pallas_call(
        functools.partial(scatter_kernel, coef, chunk, 4, tile),
        out_shape=(
            jax.ShapeDtypeStruct(item_table.shape, f32),
            jax.ShapeDtypeStruct(item_table.shape, f32),
        ),
        in_specs=[SM, HB, VM, HB, HB],
        out_specs=(HB, HB),
        scratch_shapes=[
            pltpu.VMEM((2, chunk, width), f32),
            pltpu.VMEM((rows_dev, width), f32),
            pltpu.VMEM((rows_dev, width), f32),
            dma((2,)),
            dma((2,)),
            dma((2, rows_dev // tile)),
        ]
        + [pltpu.VMEM((rows_dev, width), f32)] * STREAMS,
        compiler_params=PARAMS,
        name="scatter",
    )(rows, vals.reshape(entries, width), user_gram, item_table, adagrad_state)


def solution(mesh):
    return jax.shard_map(
        shards,
        mesh=mesh,
        in_specs=(
            P(("dp", "rows"), None),
            P(("dp", "rows"), None),
            P(("dp", "rows"), None),
            P(("dp", "rows")),
        ),
        out_specs=(P(("dp", "rows"), None), P(("dp", "rows"), None)),
        check_vma=False,
    )
```

```python
import functools

import jax
import jax.numpy as jnp
from jax import lax
from jax.experimental import pallas as pl
from jax.experimental.pallas import tpu as pltpu
from jax.sharding import PartitionSpec as P

penalty_weight = 10.0
step_size = 0.05
LOW = 128
STREAMS = 8
HIGHEST = lax.Precision.HIGHEST
f32, bf16, i32 = jnp.float32, jnp.bfloat16, jnp.int32


def round_up(value, unit):
    return (value + unit - 1) // unit * unit


def split2(x):
    hi = x.astype(bf16)
    return hi, (x - hi.astype(f32)).astype(bf16)


def ask_kernel(
    data, shard, capacity, hist_ref, pos_ref, item_ref, rows_ref, codes_ref, gram_ref,
    ids, acc, rows, codes, table_ref, row_send, row_recv, code_send, code_recv, own_sem,
):
    devices = data * shard
    hist_len, users_dev = hist_ref.shape
    width = item_ref.shape[1]
    dp, rw = lax.axis_index("dp"), lax.axis_index("rows")

    def each(first, count, act):
        def step(k, _):
            act(k)
            return 0

        lax.fori_loop(first, count, step, 0)

    me = dp * shard + rw
    rows_dev = item_ref.shape[0]
    item_copy = pltpu.make_async_copy(item_ref, table_ref, own_sem.at[2])
    item_copy.start()
    barrier = pltpu.get_barrier_semaphore()

    def place(n):
        return n // shard, lax.rem(n, shard)

    def greet(k):
        pl.semaphore_signal(
            barrier, inc=1, device_id=place(lax.rem(me + k, devices)), device_id_type=pl.DeviceIdType.MESH
        )

    each(1, devices, greet)
    asks = ids.shape[0]
    ids[0:hist_len, :] = hist_ref[...]
    ids[hist_len : hist_len + 1, :] = pos_ref[...]
    if asks > hist_len + 1:
        ids[hist_len + 1 :, :] = jnp.full((asks - hist_len - 1, users_dev), devices * rows_dev, i32)
    wide = ROWS_AT_ONCE * users_dev
    upper = (
        lax.broadcasted_iota(i32, (wide, wide), 0) <= lax.broadcasted_iota(i32, (wide, wide), 1)
    ).astype(bf16)
    owners = lax.broadcasted_iota(i32, (devices, wide), 0)
    ranks_to = lax.broadcasted_iota(i32, (capacity, wide), 0)
    lane = lax.broadcasted_iota(i32, (1, users_dev), 1)
    acc[...] = jnp.zeros_like(acc)

    def route(j, carry):
        parts = [ids[pl.ds(j * ROWS_AT_ONCE + q, 1), :] for q in range(ROWS_AT_ONCE)]
        codes = [
            (lane + jnp.where(j * ROWS_AT_ONCE + q >= hist_len, users_dev, 0)).astype(f32)
            for q in range(ROWS_AT_ONCE)
        ]
        want = jnp.concatenate(parts, axis=1)
        code = jnp.concatenate(codes, axis=1)
        owner = want // rows_dev
        local = want - owner * rows_dev
        high = (local // LOW).astype(f32)
        low = (local % LOW).astype(f32)
        member = (owner == owners).astype(f32)
        prefix = jnp.dot(member.astype(bf16), upper, preferred_element_type=f32)
        rank = jnp.sum(member * (prefix + carry), axis=0, keepdims=True) - 1.0
        left = jnp.concatenate([member * high, member * low, member * code, member], axis=0).astype(bf16)
        right = (rank.astype(i32) == ranks_to).astype(f32).astype(bf16)
        acc[...] += lax.dot_general(left, right, (((1,), (1,)), ((), ())), preferred_element_type=f32)
        return carry + jnp.sum(member, axis=1, keepdims=True)

    lax.fori_loop(0, asks // ROWS_AT_ONCE, route, jnp.zeros((devices, 1), f32))

    def write(d):
        row = acc[pl.ds(d, 1), :] * LOW + acc[pl.ds(devices + d, 1), :]
        code = acc[pl.ds(2 * devices + d, 1), :]
        present = acc[pl.ds(3 * devices + d, 1), :]
        rows[d] = row.astype(i32)
        codes[d] = jnp.where(present > 0.5, code, 2.0 * users_dev).astype(i32)

    each(0, devices, write)
    pl.semaphore_wait(barrier, devices - 1)

    def list_copies(k, to, at):
        return tuple(
            pltpu.make_async_remote_copy(
                src_ref=src.at[to], dst_ref=dst.at[at], send_sem=send.at[k], recv_sem=recv.at[k],
                device_id=place(to), device_id_type=pl.DeviceIdType.MESH,
            )
            for src, dst, send, recv in (
                (rows, rows_ref, row_send, row_recv),
                (codes, codes_ref, code_send, code_recv),
            )
        )

    def send_list(k):
        for copy in list_copies(k, lax.rem(me + k, devices), me):
            copy.start()

    each(1, devices, send_list)
    own = (
        pltpu.make_async_copy(rows.at[me], rows_ref.at[me], own_sem.at[0]),
        pltpu.make_async_copy(codes.at[me], codes_ref.at[me], own_sem.at[1]),
    )
    for copy in own:
        copy.start()
    item_copy.wait()
    tall = 512
    gram_ref[...] = jnp.zeros_like(gram_ref)

    def square(n):
        hi, lo = split2(table_ref[pl.ds(pl.multiple_of(n * tall, 8), tall), :])
        both = lax.dot_general(
            hi, jnp.concatenate([hi, lo], axis=1), (((0,), (0,)), ((), ())), preferred_element_type=f32
        )
        gram_ref[...] += both[:, :width] + (both[:, width:] + both[:, width:].T)

    each(0, rows_dev // tall, square)

    def finish(k):
        n = lax.rem(me - k + devices, devices)
        for copy in list_copies(k, n, n):
            copy.wait_recv()
            copy.wait_send()

    each(1, devices, finish)
    for copy in own:
        copy.wait()


def line_sizes(data, shard):
    cols = max(n for n in range(1, shard + 1) if shard % n == 0 and n * n <= shard)
    return data // 2, cols, shard // cols


ORDERS = ((0, 1, 2), (1, 0, 2))
LAGS = (2, 4, 6, 8)
VSLOTS = 4
ROWS_AT_ONCE = 4
TWIN_LAG = 2


def exchange_kernel(
    sizes, capacity, users_dev, hist_len, coef, unroll,
    rows_hbm, codes_hbm, hot_ref, gram_ref, item_ref, vals_ref, ugram_ref,
    rows_ref, codes_ref, table_ref, fetch_sem, picked, part, pair, mail, grads, cur, vbuf, upart, gsum, gmail, gfull,
    pair_send, pair_recv, mail_send, mail_recv, ag_send, ag_recv, twin_send, twin_recv, gram_send, gram_recv, vsem,
):
    nx, ny, nz = sizes
    plane = nx * ny * nz
    shard = ny * nz
    width = item_ref.shape[1]
    half = width // 2
    dp, rw = lax.axis_index("dp"), lax.axis_index("rows")
    core = lax.rem(dp, 2)
    pos = (dp // 2, lax.rem(rw, ny), rw // ny)
    origin = (0, 0, 0)
    axes = (0, 1, 2)

    def device(chip, c):
        return chip[0] * 2 + c, chip[2] * ny + chip[1]

    def block(chip, c):
        d, r = device(chip, c)
        return d * shard + r

    def ahead(r):
        return tuple(lax.rem(p + k, n) for p, k, n in zip(pos, r, sizes))

    def behind(o):
        return tuple(lax.rem(p - k + n, n) for p, k, n in zip(pos, o, sizes))

    def only(a, k):
        return tuple(k if b == a else 0 for b in axes)

    def add(r, a, k):
        return tuple(v + k if b == a else v for b, v in enumerate(r))

    def slot(r):
        return (r[0] * ny + r[1]) * nz + r[2]

    def ranked(n, digits):
        out = [0, 0, 0]
        for a in reversed(digits):
            out[a] = lax.rem(n, sizes[a])
            n = n // sizes[a]
        return tuple(out)

    partner = device(pos, 1 - core)

    def remote(src, dst, send, recv, dev):
        return pltpu.make_async_remote_copy(
            src_ref=src, dst_ref=dst, send_sem=send, recv_sem=recv,
            device_id=dev, device_id_type=pl.DeviceIdType.MESH,
        )

    def each(first, count, act):
        def step(k, _):
            act(k)
            return 0

        lax.fori_loop(first, count, step, 0)

    me = block(pos, core)
    devices = 2 * plane
    fetches = (
        pltpu.make_async_copy(rows_hbm, rows_ref, fetch_sem.at[0]),
        pltpu.make_async_copy(codes_hbm, codes_ref, fetch_sem.at[1]),
        pltpu.make_async_copy(item_ref, table_ref, fetch_sem.at[2]),
    )
    for fetch in fetches:
        fetch.start()
    barrier = pltpu.get_barrier_semaphore()
    greeted = 1
    pl.semaphore_signal(barrier, inc=1, device_id=partner, device_id_type=pl.DeviceIdType.MESH)
    for a in axes:
        for k in range(1, sizes[a]):
            greeted += 1
            pl.semaphore_signal(
                barrier, inc=1, device_id=device(ahead(only(a, k)), core), device_id_type=pl.DeviceIdType.MESH
            )
    pl.semaphore_wait(barrier, greeted)
    for fetch in fetches:
        fetch.wait()

    def pair_copy(at):
        return remote(part.at[0, at], pair.at[at], pair_send.at[at], pair_recv.at[at], partner)

    def letter(h, at, dev):
        return remote(part.at[1, at, h], mail.at[h, at], mail_send.at[h, at], mail_recv.at[h, at], dev)

    def parcel(h, at, b, dev):
        return remote(grads.at[b, h], grads.at[b, h], ag_send.at[h, at], ag_recv.at[h, at], dev)

    def twin(at, b):
        return remote(grads.at[b], grads.at[b], twin_send.at[at], twin_recv.at[at], partner)

    first = [1]
    for a in axes:
        first.append(first[-1] + sizes[a] - 1)
    last = first[3]
    mine = pl.ds(pl.multiple_of(core * half, 8), half)
    theirs = pl.ds(pl.multiple_of((1 - core) * half, 8), half)

    def gram_pair(t, src):
        return remote(src.at[theirs], gmail.at[t, 0], gram_send.at[t, 0], gram_recv.at[t, 0], partner)

    def gram_line(t, a, k):
        at = first[a] + k - 1
        return remote(
            gsum.at[t, a], gmail.at[t, at], gram_send.at[t, at], gram_recv.at[t, at], device(ahead(only(a, k)), core)
        )

    def gram_final(t):
        return remote(gsum.at[t, 3], gfull.at[t, mine], gram_send.at[t, last], gram_recv.at[t, last], partner)

    def gram_open(t, src):
        gram_pair(t, src).start()

    def gram_send_line(t, a):
        for k in range(1, sizes[a]):
            gram_line(t, a, k).start()

    def gram_step(t, src, stage):
        if stage == 0:
            gram_pair(t, src).wait_recv()
            gsum[t, 0] = src[mine, :] + gmail[t, 0]
        elif stage <= 3:
            a = stage - 1
            total = gsum[t, a]
            for k in range(1, sizes[a]):
                gram_line(t, a, k).wait_recv()
                total = total + gmail[t, first[a] + k - 1]
            gsum[t, a + 1] = total
        else:
            gram_final(t).wait_recv()
        if stage < 3:
            gram_send_line(t, stage)
        elif stage == 3:
            gram_final(t).start()
            gfull[t, mine] = gsum[t, 3]

    def gram_drain(t, src):
        gram_pair(t, src).wait_send()
        for a in axes:
            for k in range(1, sizes[a]):
                gram_line(t, a, k).wait_send()
        gram_final(t).wait_send()

    codes_to = lax.broadcasted_iota(i32, (2 * users_dev, capacity), 0)

    def gather(b, j, at):
        base = b * capacity

        def some(s, _):
            start = base + s * unroll
            for k in range(unroll):
                r = rows_ref.at[pl.ds(k, rows_ref.shape[0] - unroll + 1)][start]
                picked[pl.ds(s * unroll + k, 1), :] = table_ref[pl.ds(r, 1), :]
            return 0

        lax.fori_loop(0, capacity // unroll, some, 0)
        x = picked[...]
        hi, lo = split2(x)
        hot = (hot_ref[b] == codes_to).astype(f32).astype(bf16)
        both = jnp.dot(hot, jnp.concatenate([hi, lo], axis=1), preferred_element_type=f32)
        out = both[:, :width] + both[:, width:]
        part[j, at, 0] = out[:users_dev]
        part[j, at, 1] = out[users_dev:]

    def arrive(h, r, a):
        at = slot(r)
        for k in range(1, sizes[a]):
            m = slot(add(r, a, k))
            letter(h, m, partner).wait_recv()
            part[1, at, h] = part[1, at, h] + mail[h, m]

    def leave(h, r, a):
        @pl.when(r[a] != 0)
        def _():
            chip = tuple(lax.rem(p + r[a], n) if b == a else p for b, (p, n) in enumerate(zip(pos, sizes)))
            letter(h, slot(r), device(chip, core)).start()

    gram_open(0, gram_ref)

    def reduce_step(i, _):
        for stage in range(4):
            j = i - LAGS[stage]

            @pl.when(jnp.logical_and(j >= 0, j < plane))
            def _():
                r = ranked(plane - 1 - j, (2, 0, 1))
                at = slot(r)
                if stage == 0:
                    pair_copy(at).wait_recv()
                    for h in range(2):
                        part[1, at, h] = part[1, at, h] + pair[at, h]
                        leave(h, r, ORDERS[h][0])
                else:
                    for h in range(2):
                        order = ORDERS[h]
                        clear = r[order[0]] == 0
                        for a in order[1:stage]:
                            clear = jnp.logical_and(clear, r[a] == 0)

                        @pl.when(clear)
                        def _():
                            arrive(h, r, order[stage - 1])
                            if stage < 3:
                                leave(h, r, order[stage])

        for stage in range(5):
            @pl.when(i == 3 * stage + 3)
            def _():
                gram_step(0, gram_ref, stage)

        @pl.when(i < plane)
        def _():
            r = ranked(plane - 1 - i, (2, 0, 1))
            at = slot(r)
            chip = ahead(r)

            def one(j, _):
                c = (1 - core) * (1 - j) + core * j
                gather(block(chip, c), j, at)

                @pl.when(j == 0)
                def _():
                    pair_copy(at).start()

                return 0

            lax.fori_loop(0, 2, one, 0)

        return 0

    lax.fori_loop(0, plane + LAGS[3], reduce_step, 0)

    uv = part[1, 0, 0] / hist_len
    pv = part[1, 0, 1]
    gap = jnp.sum(uv * pv, axis=1, keepdims=True) - 1.0
    ug = 2.0 * gap * pv + 2.0 * coef * jnp.dot(uv, gfull[0], precision=HIGHEST, preferred_element_type=f32)
    grads[me, 0] = ug / hist_len
    grads[me, 1] = 2.0 * gap * uv

    def forward(h, o, b, a):
        for k in range(1, sizes[a]):
            chip = tuple(lax.rem(p + k, n) if c == a else p for c, (p, n) in enumerate(zip(pos, sizes)))
            parcel(h, slot(add(o, a, k)), b, device(chip, core)).start()

    ways = tuple(order[::-1] for order in ORDERS)
    line = ways[0][0]
    for k in range(1, sizes[line]):
        for h in range(2):
            parcel(h, slot(only(line, k)), me, device(ahead(only(line, k)), core)).start()
    for a in (1, 2):
        for h in range(2):
            forward(h, origin, me, ways[h][a])
    twin(0, me).start()
    upart[...] = lax.dot_general(
        uv, uv, (((0,), (0,)), ((), ())), precision=HIGHEST, preferred_element_type=f32
    )
    gram_open(1, upart)
    cur[pl.ds(2 * users_dev, 8), :] = jnp.zeros((8, width), f32)

    def vals_copy(v, b):
        return pltpu.make_async_copy(vbuf.at[v], vals_ref.at[b], vsem.at[v])

    def vals(n, kind, b):
        v = 2 * kind + lax.rem(n, 2)

        @pl.when(n >= 2)
        def _():
            vals_copy(v, b).wait()

        cur[pl.ds(0, users_dev), :] = grads[b, 0]
        cur[pl.ds(users_dev, users_dev), :] = grads[b, 1]
        base = b * capacity

        def some(s, _):
            start = base + s * unroll
            for k in range(unroll):
                c = codes_ref.at[pl.ds(k, codes_ref.shape[0] - unroll + 1)][start]
                vbuf[v, pl.ds(s * unroll + k, 1), :] = cur[pl.ds(c, 1), :]
            return 0

        lax.fori_loop(0, capacity // unroll, some, 0)
        vals_copy(v, b).start()

    digits = ((2, 0, 1), (2, 1, 0))
    delays = (-nx * ny, 1, 3)
    vals_delay = delays[2] + 1

    def spread(n, _):
        for h in range(2):
            a1, a2, a3 = ways[h]
            for level in (1, 2, 3):
                q = n - delays[level - 1]
                o = ranked(q, digits[h])
                if level == 1:
                    here = jnp.logical_and(o[a1] != 0, jnp.logical_and(o[a2] == 0, o[a3] == 0))
                elif level == 2:
                    here = jnp.logical_and(o[a2] != 0, o[a3] == 0)
                else:
                    here = o[a3] != 0

                @pl.when(jnp.logical_and(jnp.logical_and(q >= 0, q < plane), here))
                def _():
                    b = block(behind(o), core)
                    parcel(h, slot(o), b, partner).wait_recv()
                    for a in ways[h][level:]:
                        forward(h, o, b, a)

        def one(kind, _):
            j = n - vals_delay - TWIN_LAG * kind

            @pl.when(jnp.logical_and(j >= 0, j < plane))
            def _():
                o = ranked(j, digits[0])
                at = slot(o)
                b = block(behind(o), core + kind * (1 - 2 * core))

                @pl.when(jnp.logical_and(kind == 0, j > 0))
                def _():
                    twin(at, b).start()

                @pl.when(kind == 1)
                def _():
                    twin(at, b).wait_recv()

                vals(j, kind, b)

            return 0

        lax.fori_loop(0, 2, one, 0)

        for stage in range(5):
            @pl.when(n == 4 * stage + 3)
            def _():
                gram_step(1, upart, stage)

        return 0

    lax.fori_loop(0, plane + vals_delay + TWIN_LAG, spread, 0)
    ugram_ref[...] = gfull[1]

    def drain(n):
        pair_copy(n).wait_send()
        twin(n, me).wait_send()

    each(0, plane, drain)

    def drain_mail(n):
        for h in range(2):
            letter(h, n, partner).wait_send()
            parcel(h, n, me, partner).wait_send()

    each(1, plane, drain_mail)
    gram_drain(0, gram_ref)
    gram_drain(1, upart)
    each(0, VSLOTS, lambda v: vals_copy(v, me).wait())


def scatter_kernel(
    coef, chunk, unroll, tile,
    rows_ref, vals_ref, ugram_ref, table_ref, state_ref, new_table_ref, new_state_ref,
    vbuf, table, state, vsem, in_sem, out_sem, *accs,
):
    entries = rows_ref.shape[0]
    chunks = entries // chunk
    part = chunk // len(accs)
    rows_dev, width = table.shape
    tiles = rows_dev // tile

    def vals_copy(n):
        s = lax.rem(n, 2)
        return pltpu.make_async_copy(
            vals_ref.at[pl.ds(pl.multiple_of(n * chunk, 8), chunk)], vbuf.at[s], vsem.at[s]
        )

    table_copy = pltpu.make_async_copy(table_ref, table, in_sem.at[0])
    state_copy = pltpu.make_async_copy(state_ref, state, in_sem.at[1])
    vals_copy(0).start()
    vals_copy(1).start()
    table_copy.start()
    state_copy.start()
    for acc in accs:
        acc[...] = jnp.zeros_like(acc)

    def one(n, _):
        v = lax.rem(n, 2)
        vals_copy(n).wait()

        def scatter(s, _):
            start = n * chunk + s * unroll
            for q in range(unroll):
                rows = [
                    rows_ref.at[pl.ds(k * part + q, entries - chunk + part - unroll + 1)][start] for k in range(len(accs))
                ]
                news = [
                    acc[pl.ds(r, 1), :] + vbuf[v, pl.ds(s * unroll + (k * part + q), 1), :]
                    for k, (acc, r) in enumerate(zip(accs, rows))
                ]
                for acc, r, new in zip(accs, rows, news):
                    acc[pl.ds(r, 1), :] = new
            return 0

        lax.fori_loop(0, part // unroll, scatter, 0)

        @pl.when(n + 2 < chunks)
        def _():
            vals_copy(n + 2).start()

        return 0

    lax.fori_loop(0, chunks, one, 0)
    table_copy.wait()
    state_copy.wait()
    u0, u1 = split2(ugram_ref[...])
    u00 = jnp.concatenate([u0, u0], axis=0)

    def out_copy(t, which):
        at = pl.ds(pl.multiple_of(t * tile, 8), tile)
        src, dst = ((table, new_table_ref), (state, new_state_ref))[which]
        return pltpu.make_async_copy(src.at[at], dst.at[at], out_sem.at[which, t])

    def finish(t, _):
        at = pl.ds(pl.multiple_of(t * tile, 8), tile)
        item = table[at, :]
        t0, t1 = split2(item)
        g = jnp.dot(jnp.concatenate([t0, t1], axis=1), u00, preferred_element_type=f32)
        g = 2.0 * coef * (g + jnp.dot(t0, u1, preferred_element_type=f32))
        add = accs[0][at, :]
        for acc in accs[1:]:
            add = add + acc[at, :]
        g = g + add
        new = state[at, :] + g * g
        state[at, :] = new
        table[at, :] = item - step_size * g / jnp.sqrt(new)
        out_copy(t, 0).start()
        out_copy(t, 1).start()
        return 0

    lax.fori_loop(0, tiles, finish, 0)

    def drain(t, _):
        out_copy(t, 0).wait()
        out_copy(t, 1).wait()
        return 0

    lax.fori_loop(0, tiles, drain, 0)


VM = pl.BlockSpec(memory_space=pltpu.VMEM)
HB = pl.BlockSpec(memory_space=pl.ANY)
SM = pl.BlockSpec(memory_space=pltpu.SMEM)
PARAMS = pltpu.CompilerParams(vmem_limit_bytes=60 * 1024 * 1024)


def shards(item_table, adagrad_state, history_ids, positive_ids):
    rows_dev, width = item_table.shape
    users_dev, hist_len = history_ids.shape
    devices = lax.axis_size("dp") * lax.axis_size("rows")
    groups = 2 * users_dev
    count = users_dev * (hist_len + 1)
    capacity = max(8, (count * 5 // (2 * devices) + 7) // 8 * 8)
    entries = devices * capacity
    asks = round_up(hist_len + 1, ROWS_AT_ONCE)
    data, shard = lax.axis_size("dp"), lax.axis_size("rows")
    sizes = line_sizes(data, shard)
    plane = devices // 2
    lines = sum(sizes) - 1
    unroll = max(n for n in (8, 16, 32, 64, 128) if capacity % n == 0)
    coef = penalty_weight / (rows_dev * devices)
    dma = pltpu.SemaphoreType.DMA
    list_shape = jax.ShapeDtypeStruct((devices, 1, capacity), i32)
    rows, codes, item_gram = pl.pallas_call(
        functools.partial(ask_kernel, data, shard, capacity),
        out_shape=(list_shape, list_shape, jax.ShapeDtypeStruct((width, width), f32)),
        in_specs=[VM, VM, HB],
        out_specs=(HB, HB, VM),
        scratch_shapes=[
            pltpu.VMEM((asks, users_dev), i32),
            pltpu.VMEM((4 * devices, capacity), f32),
            pltpu.VMEM((devices, 1, capacity), i32),
            pltpu.VMEM((devices, 1, capacity), i32),
            pltpu.VMEM((rows_dev, width), f32),
        ]
        + [dma((devices,))] * 4
        + [dma((3,))],
        compiler_params=pltpu.CompilerParams(
            vmem_limit_bytes=60 * 1024 * 1024, collective_id=1, has_side_effects=True
        ),
        name="ask",
    )(history_ids.T, positive_ids[None], item_table)
    flat = rows.reshape(-1)
    vals, user_gram = pl.pallas_call(
        functools.partial(exchange_kernel, sizes, capacity, users_dev, hist_len, coef, unroll),
        out_shape=(
            jax.ShapeDtypeStruct((devices, capacity, width), f32),
            jax.ShapeDtypeStruct((width, width), f32),
        ),
        in_specs=[HB, HB, VM, VM, HB],
        out_specs=(HB, VM),
        scratch_shapes=[
            pltpu.SMEM((entries,), i32),
            pltpu.SMEM((entries,), i32),
            pltpu.VMEM((rows_dev, width), f32),
            dma((3,)),
            pltpu.VMEM((capacity, width), f32),
            pltpu.VMEM((2, plane, 2, users_dev, width), f32),
            pltpu.VMEM((plane, 2, users_dev, width), f32),
            pltpu.VMEM((2, plane, users_dev, width), f32),
            pltpu.VMEM((devices, 2, users_dev, width), f32),
            pltpu.VMEM((groups + 8, width), f32),
            pltpu.VMEM((VSLOTS, capacity, width), f32),
            pltpu.VMEM((width, width), f32),
            pltpu.VMEM((2, 4, width // 2, width), f32),
            pltpu.VMEM((2, lines, width // 2, width), f32),
            pltpu.VMEM((2, width, width), f32),
            dma((plane,)),
            dma((plane,)),
            dma((2, plane)),
            dma((2, plane)),
            dma((2, plane)),
            dma((2, plane)),
            dma((plane,)),
            dma((plane,)),
            dma((2, lines)),
            dma((2, lines)),
            dma((VSLOTS,)),
        ],
        compiler_params=pltpu.CompilerParams(
            vmem_limit_bytes=60 * 1024 * 1024, collective_id=0, has_side_effects=True
        ),
        name="exchange",
    )(flat, codes.reshape(-1), codes, item_gram, item_table)
    chunk, tile = min(2048, entries), 256
    return pl.pallas_call(
        functools.partial(scatter_kernel, coef, chunk, 4, tile),
        out_shape=(
            jax.ShapeDtypeStruct(item_table.shape, f32),
            jax.ShapeDtypeStruct(item_table.shape, f32),
        ),
        in_specs=[SM, HB, VM, HB, HB],
        out_specs=(HB, HB),
        scratch_shapes=[
            pltpu.VMEM((2, chunk, width), f32),
            pltpu.VMEM((rows_dev, width), f32),
            pltpu.VMEM((rows_dev, width), f32),
            dma((2,)),
            dma((2,)),
            dma((2, rows_dev // tile)),
        ]
        + [pltpu.VMEM((rows_dev, width), f32)] * STREAMS,
        compiler_params=PARAMS,
        name="scatter",
    )(flat, vals.reshape(entries, width), user_gram, item_table, adagrad_state)


def solution(mesh):
    return jax.shard_map(
        shards,
        mesh=mesh,
        in_specs=(
            P(("dp", "rows"), None),
            P(("dp", "rows"), None),
            P(("dp", "rows"), None),
            P(("dp", "rows")),
        ),
        out_specs=(P(("dp", "rows"), None), P(("dp", "rows"), None)),
        check_vma=False,
    )
```

```python
import functools

import jax
import jax.numpy as jnp
from jax import lax
from jax.experimental import pallas as pl
from jax.experimental.pallas import tpu as pltpu
from jax.sharding import PartitionSpec as P

penalty_weight = 10.0
step_size = 0.05
LOW = 128
STREAMS = 16
HIGHEST = lax.Precision.HIGHEST
f32, bf16, i32 = jnp.float32, jnp.bfloat16, jnp.int32


def round_up(value, unit):
    return (value + unit - 1) // unit * unit


def split2(x):
    hi = x.astype(bf16)
    return hi, (x - hi.astype(f32)).astype(bf16)


def ask_kernel(
    data, shard, capacity, hist_ref, pos_ref, item_ref, rows_ref, codes_ref, gram_ref,
    ids, acc, rows, codes, table_ref, row_send, row_recv, code_send, code_recv, own_sem,
):
    devices = data * shard
    hist_len, users_dev = hist_ref.shape
    width = item_ref.shape[1]
    dp, rw = lax.axis_index("dp"), lax.axis_index("rows")

    def each(first, count, act):
        def step(k, _):
            act(k)
            return 0

        lax.fori_loop(first, count, step, 0)

    me = dp * shard + rw
    rows_dev = item_ref.shape[0]
    item_copy = pltpu.make_async_copy(item_ref, table_ref, own_sem.at[2])
    item_copy.start()
    barrier = pltpu.get_barrier_semaphore()

    def place(n):
        return n // shard, lax.rem(n, shard)

    def greet(k):
        pl.semaphore_signal(
            barrier, inc=1, device_id=place(lax.rem(me + k, devices)), device_id_type=pl.DeviceIdType.MESH
        )

    each(1, devices, greet)
    asks = ids.shape[0]
    ids[0:hist_len, :] = hist_ref[...]
    ids[hist_len : hist_len + 1, :] = pos_ref[...]
    if asks > hist_len + 1:
        ids[hist_len + 1 :, :] = jnp.full((asks - hist_len - 1, users_dev), devices * rows_dev, i32)
    wide = ROWS_AT_ONCE * users_dev
    upper = (
        lax.broadcasted_iota(i32, (wide, wide), 0) <= lax.broadcasted_iota(i32, (wide, wide), 1)
    ).astype(bf16)
    owners = lax.broadcasted_iota(i32, (devices, wide), 0)
    ranks_to = lax.broadcasted_iota(i32, (capacity, wide), 0)
    lane = lax.broadcasted_iota(i32, (1, users_dev), 1)
    acc[...] = jnp.zeros_like(acc)

    def route(j, carry):
        parts = [ids[pl.ds(j * ROWS_AT_ONCE + q, 1), :] for q in range(ROWS_AT_ONCE)]
        codes = [
            (lane + jnp.where(j * ROWS_AT_ONCE + q >= hist_len, users_dev, 0)).astype(f32)
            for q in range(ROWS_AT_ONCE)
        ]
        want = jnp.concatenate(parts, axis=1)
        code = jnp.concatenate(codes, axis=1)
        owner = want // rows_dev
        local = want - owner * rows_dev
        high = (local // LOW).astype(f32)
        low = (local % LOW).astype(f32)
        member = (owner == owners).astype(f32)
        prefix = jnp.dot(member.astype(bf16), upper, preferred_element_type=f32)
        rank = jnp.sum(member * (prefix + carry), axis=0, keepdims=True) - 1.0
        left = jnp.concatenate([member * high, member * low, member * code, member], axis=0).astype(bf16)
        right = (rank.astype(i32) == ranks_to).astype(f32).astype(bf16)
        acc[...] += lax.dot_general(left, right, (((1,), (1,)), ((), ())), preferred_element_type=f32)
        return carry + jnp.sum(member, axis=1, keepdims=True)

    lax.fori_loop(0, asks // ROWS_AT_ONCE, route, jnp.zeros((devices, 1), f32))

    def write(d):
        row = acc[pl.ds(d, 1), :] * LOW + acc[pl.ds(devices + d, 1), :]
        code = acc[pl.ds(2 * devices + d, 1), :]
        present = acc[pl.ds(3 * devices + d, 1), :]
        rows[d] = row.astype(i32)
        codes[d] = jnp.where(present > 0.5, code, 2.0 * users_dev).astype(i32)

    each(0, devices, write)
    pl.semaphore_wait(barrier, devices - 1)

    def list_copies(k, to, at):
        return tuple(
            pltpu.make_async_remote_copy(
                src_ref=src.at[to], dst_ref=dst.at[at], send_sem=send.at[k], recv_sem=recv.at[k],
                device_id=place(to), device_id_type=pl.DeviceIdType.MESH,
            )
            for src, dst, send, recv in (
                (rows, rows_ref, row_send, row_recv),
                (codes, codes_ref, code_send, code_recv),
            )
        )

    def send_list(k):
        for copy in list_copies(k, lax.rem(me + k, devices), me):
            copy.start()

    each(1, devices, send_list)
    own = (
        pltpu.make_async_copy(rows.at[me], rows_ref.at[me], own_sem.at[0]),
        pltpu.make_async_copy(codes.at[me], codes_ref.at[me], own_sem.at[1]),
    )
    for copy in own:
        copy.start()
    item_copy.wait()
    tall = 512
    gram_ref[...] = jnp.zeros_like(gram_ref)

    def square(n):
        hi, lo = split2(table_ref[pl.ds(pl.multiple_of(n * tall, 8), tall), :])
        both = lax.dot_general(
            hi, jnp.concatenate([hi, lo], axis=1), (((0,), (0,)), ((), ())), preferred_element_type=f32
        )
        gram_ref[...] += both[:, :width] + (both[:, width:] + both[:, width:].T)

    each(0, rows_dev // tall, square)

    def finish(k):
        n = lax.rem(me - k + devices, devices)
        for copy in list_copies(k, n, n):
            copy.wait_recv()
            copy.wait_send()

    each(1, devices, finish)
    for copy in own:
        copy.wait()


def line_sizes(data, shard):
    cols = max(n for n in range(1, shard + 1) if shard % n == 0 and n * n <= shard)
    return data // 2, cols, shard // cols


ORDERS = ((0, 1, 2), (1, 0, 2))
LAGS = (2, 4, 6, 8)
VSLOTS = 4
ROWS_AT_ONCE = 4
TWIN_LAG = 2


def exchange_kernel(
    sizes, capacity, users_dev, hist_len, coef, unroll,
    rows_hbm, codes_hbm, hot_ref, gram_ref, item_ref, vals_ref, ugram_ref,
    rows_ref, codes_ref, table_ref, fetch_sem, picked, part, pair, mail, grads, cur, vbuf, upart, gsum, gmail, gfull,
    pair_send, pair_recv, mail_send, mail_recv, ag_send, ag_recv, twin_send, twin_recv, gram_send, gram_recv, vsem,
):
    nx, ny, nz = sizes
    plane = nx * ny * nz
    shard = ny * nz
    width = item_ref.shape[1]
    half = width // 2
    dp, rw = lax.axis_index("dp"), lax.axis_index("rows")
    core = lax.rem(dp, 2)
    pos = (dp // 2, lax.rem(rw, ny), rw // ny)
    origin = (0, 0, 0)
    axes = (0, 1, 2)

    def device(chip, c):
        return chip[0] * 2 + c, chip[2] * ny + chip[1]

    def block(chip, c):
        d, r = device(chip, c)
        return d * shard + r

    def ahead(r):
        return tuple(lax.rem(p + k, n) for p, k, n in zip(pos, r, sizes))

    def behind(o):
        return tuple(lax.rem(p - k + n, n) for p, k, n in zip(pos, o, sizes))

    def only(a, k):
        return tuple(k if b == a else 0 for b in axes)

    def add(r, a, k):
        return tuple(v + k if b == a else v for b, v in enumerate(r))

    def slot(r):
        return (r[0] * ny + r[1]) * nz + r[2]

    def ranked(n, digits):
        out = [0, 0, 0]
        for a in reversed(digits):
            out[a] = lax.rem(n, sizes[a])
            n = n // sizes[a]
        return tuple(out)

    partner = device(pos, 1 - core)

    def remote(src, dst, send, recv, dev):
        return pltpu.make_async_remote_copy(
            src_ref=src, dst_ref=dst, send_sem=send, recv_sem=recv,
            device_id=dev, device_id_type=pl.DeviceIdType.MESH,
        )

    def each(first, count, act):
        def step(k, _):
            act(k)
            return 0

        lax.fori_loop(first, count, step, 0)

    me = block(pos, core)
    devices = 2 * plane
    fetches = (
        pltpu.make_async_copy(rows_hbm, rows_ref, fetch_sem.at[0]),
        pltpu.make_async_copy(codes_hbm, codes_ref, fetch_sem.at[1]),
        pltpu.make_async_copy(item_ref, table_ref, fetch_sem.at[2]),
    )
    for fetch in fetches:
        fetch.start()
    barrier = pltpu.get_barrier_semaphore()
    greeted = 1
    pl.semaphore_signal(barrier, inc=1, device_id=partner, device_id_type=pl.DeviceIdType.MESH)
    for a in axes:
        for k in range(1, sizes[a]):
            greeted += 1
            pl.semaphore_signal(
                barrier, inc=1, device_id=device(ahead(only(a, k)), core), device_id_type=pl.DeviceIdType.MESH
            )
    pl.semaphore_wait(barrier, greeted)
    for fetch in fetches:
        fetch.wait()

    def pair_copy(at):
        return remote(part.at[0, at], pair.at[at], pair_send.at[at], pair_recv.at[at], partner)

    def letter(h, at, dev):
        return remote(part.at[1, at, h], mail.at[h, at], mail_send.at[h, at], mail_recv.at[h, at], dev)

    def parcel(h, at, b, dev):
        return remote(grads.at[b, h], grads.at[b, h], ag_send.at[h, at], ag_recv.at[h, at], dev)

    def twin(at, b):
        return remote(grads.at[b], grads.at[b], twin_send.at[at], twin_recv.at[at], partner)

    first = [1]
    for a in axes:
        first.append(first[-1] + sizes[a] - 1)
    last = first[3]
    mine = pl.ds(pl.multiple_of(core * half, 8), half)
    theirs = pl.ds(pl.multiple_of((1 - core) * half, 8), half)

    def gram_pair(t, src):
        return remote(src.at[theirs], gmail.at[t, 0], gram_send.at[t, 0], gram_recv.at[t, 0], partner)

    def gram_line(t, a, k):
        at = first[a] + k - 1
        return remote(
            gsum.at[t, a], gmail.at[t, at], gram_send.at[t, at], gram_recv.at[t, at], device(ahead(only(a, k)), core)
        )

    def gram_final(t):
        return remote(gsum.at[t, 3], gfull.at[t, mine], gram_send.at[t, last], gram_recv.at[t, last], partner)

    def gram_open(t, src):
        gram_pair(t, src).start()

    def gram_send_line(t, a):
        for k in range(1, sizes[a]):
            gram_line(t, a, k).start()

    def gram_step(t, src, stage):
        if stage == 0:
            gram_pair(t, src).wait_recv()
            gsum[t, 0] = src[mine, :] + gmail[t, 0]
        elif stage <= 3:
            a = stage - 1
            total = gsum[t, a]
            for k in range(1, sizes[a]):
                gram_line(t, a, k).wait_recv()
                total = total + gmail[t, first[a] + k - 1]
            gsum[t, a + 1] = total
        else:
            gram_final(t).wait_recv()
        if stage < 3:
            gram_send_line(t, stage)
        elif stage == 3:
            gram_final(t).start()
            gfull[t, mine] = gsum[t, 3]

    def gram_drain(t, src):
        gram_pair(t, src).wait_send()
        for a in axes:
            for k in range(1, sizes[a]):
                gram_line(t, a, k).wait_send()
        gram_final(t).wait_send()

    codes_to = lax.broadcasted_iota(i32, (2 * users_dev, capacity), 0)

    def gather(b, j, at):
        base = b * capacity

        def some(s, _):
            start = base + s * unroll
            for k in range(unroll):
                r = rows_ref.at[pl.ds(k, rows_ref.shape[0] - unroll + 1)][start]
                picked[pl.ds(s * unroll + k, 1), :] = table_ref[pl.ds(r, 1), :]
            return 0

        lax.fori_loop(0, capacity // unroll, some, 0)
        x = picked[...]
        hi, lo = split2(x)
        hot = (hot_ref[b] == codes_to).astype(f32).astype(bf16)
        both = jnp.dot(hot, jnp.concatenate([hi, lo], axis=1), preferred_element_type=f32)
        out = both[:, :width] + both[:, width:]
        part[j, at, 0] = out[:users_dev]
        part[j, at, 1] = out[users_dev:]

    def arrive(h, r, a):
        at = slot(r)
        for k in range(1, sizes[a]):
            m = slot(add(r, a, k))
            letter(h, m, partner).wait_recv()
            part[1, at, h] = part[1, at, h] + mail[h, m]

    def leave(h, r, a):
        @pl.when(r[a] != 0)
        def _():
            chip = tuple(lax.rem(p + r[a], n) if b == a else p for b, (p, n) in enumerate(zip(pos, sizes)))
            letter(h, slot(r), device(chip, core)).start()

    gram_open(0, gram_ref)

    def reduce_step(i, _):
        for stage in range(4):
            j = i - LAGS[stage]

            @pl.when(jnp.logical_and(j >= 0, j < plane))
            def _():
                r = ranked(plane - 1 - j, (2, 0, 1))
                at = slot(r)
                if stage == 0:
                    pair_copy(at).wait_recv()
                    for h in range(2):
                        part[1, at, h] = part[1, at, h] + pair[at, h]
                        leave(h, r, ORDERS[h][0])
                else:
                    for h in range(2):
                        order = ORDERS[h]
                        clear = r[order[0]] == 0
                        for a in order[1:stage]:
                            clear = jnp.logical_and(clear, r[a] == 0)

                        @pl.when(clear)
                        def _():
                            arrive(h, r, order[stage - 1])
                            if stage < 3:
                                leave(h, r, order[stage])

        for stage in range(5):
            @pl.when(i == 3 * stage + 3)
            def _():
                gram_step(0, gram_ref, stage)

        @pl.when(i < plane)
        def _():
            r = ranked(plane - 1 - i, (2, 0, 1))
            at = slot(r)
            chip = ahead(r)

            def one(j, _):
                c = (1 - core) * (1 - j) + core * j
                gather(block(chip, c), j, at)

                @pl.when(j == 0)
                def _():
                    pair_copy(at).start()

                return 0

            lax.fori_loop(0, 2, one, 0)

        return 0

    lax.fori_loop(0, plane + LAGS[3], reduce_step, 0)

    uv = part[1, 0, 0] / hist_len
    pv = part[1, 0, 1]
    gap = jnp.sum(uv * pv, axis=1, keepdims=True) - 1.0
    ug = 2.0 * gap * pv + 2.0 * coef * jnp.dot(uv, gfull[0], precision=HIGHEST, preferred_element_type=f32)
    grads[me, 0] = ug / hist_len
    grads[me, 1] = 2.0 * gap * uv

    def forward(h, o, b, a):
        for k in range(1, sizes[a]):
            chip = tuple(lax.rem(p + k, n) if c == a else p for c, (p, n) in enumerate(zip(pos, sizes)))
            parcel(h, slot(add(o, a, k)), b, device(chip, core)).start()

    ways = tuple(order[::-1] for order in ORDERS)
    line = ways[0][0]
    for k in range(1, sizes[line]):
        for h in range(2):
            parcel(h, slot(only(line, k)), me, device(ahead(only(line, k)), core)).start()
    for a in (1, 2):
        for h in range(2):
            forward(h, origin, me, ways[h][a])
    twin(0, me).start()
    upart[...] = lax.dot_general(
        uv, uv, (((0,), (0,)), ((), ())), precision=HIGHEST, preferred_element_type=f32
    )
    gram_open(1, upart)
    cur[pl.ds(2 * users_dev, 8), :] = jnp.zeros((8, width), f32)

    def vals_copy(v, b):
        return pltpu.make_async_copy(vbuf.at[v], vals_ref.at[b], vsem.at[v])

    def vals(n, kind, b):
        v = 2 * kind + lax.rem(n, 2)

        @pl.when(n >= 2)
        def _():
            vals_copy(v, b).wait()

        cur[pl.ds(0, users_dev), :] = grads[b, 0]
        cur[pl.ds(users_dev, users_dev), :] = grads[b, 1]
        base = b * capacity

        def some(s, _):
            start = base + s * unroll
            for k in range(unroll):
                c = codes_ref.at[pl.ds(k, codes_ref.shape[0] - unroll + 1)][start]
                vbuf[v, pl.ds(s * unroll + k, 1), :] = cur[pl.ds(c, 1), :]
            return 0

        lax.fori_loop(0, capacity // unroll, some, 0)
        vals_copy(v, b).start()

    digits = ((2, 0, 1), (2, 1, 0))
    delays = (-nx * ny, 1, 3)
    vals_delay = delays[2] + 1

    def spread(n, _):
        for h in range(2):
            a1, a2, a3 = ways[h]
            for level in (1, 2, 3):
                q = n - delays[level - 1]
                o = ranked(q, digits[h])
                if level == 1:
                    here = jnp.logical_and(o[a1] != 0, jnp.logical_and(o[a2] == 0, o[a3] == 0))
                elif level == 2:
                    here = jnp.logical_and(o[a2] != 0, o[a3] == 0)
                else:
                    here = o[a3] != 0

                @pl.when(jnp.logical_and(jnp.logical_and(q >= 0, q < plane), here))
                def _():
                    b = block(behind(o), core)
                    parcel(h, slot(o), b, partner).wait_recv()
                    for a in ways[h][level:]:
                        forward(h, o, b, a)

        def one(kind, _):
            j = n - vals_delay - TWIN_LAG * kind

            @pl.when(jnp.logical_and(j >= 0, j < plane))
            def _():
                o = ranked(j, digits[0])
                at = slot(o)
                b = block(behind(o), core + kind * (1 - 2 * core))

                @pl.when(jnp.logical_and(kind == 0, j > 0))
                def _():
                    twin(at, b).start()

                @pl.when(kind == 1)
                def _():
                    twin(at, b).wait_recv()

                vals(j, kind, b)

            return 0

        lax.fori_loop(0, 2, one, 0)

        for stage in range(5):
            @pl.when(n == 4 * stage + 3)
            def _():
                gram_step(1, upart, stage)

        return 0

    lax.fori_loop(0, plane + vals_delay + TWIN_LAG, spread, 0)
    ugram_ref[...] = gfull[1]

    def drain(n):
        pair_copy(n).wait_send()
        twin(n, me).wait_send()

    each(0, plane, drain)

    def drain_mail(n):
        for h in range(2):
            letter(h, n, partner).wait_send()
            parcel(h, n, me, partner).wait_send()

    each(1, plane, drain_mail)
    gram_drain(0, gram_ref)
    gram_drain(1, upart)
    each(0, VSLOTS, lambda v: vals_copy(v, me).wait())


def scatter_kernel(
    coef, chunk, unroll, tile,
    rows_hbm, vals_ref, ugram_ref, table_ref, state_ref, new_table_ref, new_state_ref,
    rows_ref, vbuf, table, state, vsem, in_sem, out_sem, *accs,
):
    entries = rows_ref.shape[0]
    chunks = entries // chunk
    part = chunk // len(accs)
    rows_dev, width = table.shape
    tiles = rows_dev // tile

    def vals_copy(n):
        s = lax.rem(n, 2)
        return pltpu.make_async_copy(
            vals_ref.at[pl.ds(pl.multiple_of(n * chunk, 8), chunk)], vbuf.at[s], vsem.at[s]
        )

    table_copy = pltpu.make_async_copy(table_ref, table, in_sem.at[0])
    state_copy = pltpu.make_async_copy(state_ref, state, in_sem.at[1])
    rows_copy = pltpu.make_async_copy(rows_hbm, rows_ref, in_sem.at[2])
    rows_copy.start()
    vals_copy(0).start()
    vals_copy(1).start()
    table_copy.start()
    state_copy.start()
    for acc in accs:
        acc[...] = jnp.zeros_like(acc)

    def one(n, _):
        v = lax.rem(n, 2)
        vals_copy(n).wait()

        def scatter(s, _):
            start = n * chunk + s * unroll
            for q in range(unroll):
                rows = [
                    rows_ref.at[pl.ds(k * part + q, entries - chunk + part - unroll + 1)][start] for k in range(len(accs))
                ]
                news = [
                    acc[pl.ds(r, 1), :] + vbuf[v, pl.ds(s * unroll + (k * part + q), 1), :]
                    for k, (acc, r) in enumerate(zip(accs, rows))
                ]
                for acc, r, new in zip(accs, rows, news):
                    acc[pl.ds(r, 1), :] = new
            return 0

        lax.fori_loop(0, part // unroll, scatter, 0)

        @pl.when(n + 2 < chunks)
        def _():
            vals_copy(n + 2).start()

        return 0

    rows_copy.wait()
    lax.fori_loop(0, chunks, one, 0)
    table_copy.wait()
    state_copy.wait()
    u0, u1 = split2(ugram_ref[...])
    u00 = jnp.concatenate([u0, u0], axis=0)

    def out_copy(t, which):
        at = pl.ds(pl.multiple_of(t * tile, 8), tile)
        src, dst = ((table, new_table_ref), (state, new_state_ref))[which]
        return pltpu.make_async_copy(src.at[at], dst.at[at], out_sem.at[which, t])

    def finish(t, _):
        at = pl.ds(pl.multiple_of(t * tile, 8), tile)
        item = table[at, :]
        t0, t1 = split2(item)
        g = jnp.dot(jnp.concatenate([t0, t1], axis=1), u00, preferred_element_type=f32)
        g = 2.0 * coef * (g + jnp.dot(t0, u1, preferred_element_type=f32))
        add = accs[0][at, :]
        for acc in accs[1:]:
            add = add + acc[at, :]
        g = g + add
        new = state[at, :] + g * g
        state[at, :] = new
        table[at, :] = item - step_size * g * lax.rsqrt(new)
        out_copy(t, 0).start()
        out_copy(t, 1).start()
        return 0

    lax.fori_loop(0, tiles, finish, 0)

    def drain(t, _):
        out_copy(t, 0).wait()
        out_copy(t, 1).wait()
        return 0

    lax.fori_loop(0, tiles, drain, 0)


VM = pl.BlockSpec(memory_space=pltpu.VMEM)
HB = pl.BlockSpec(memory_space=pl.ANY)
SM = pl.BlockSpec(memory_space=pltpu.SMEM)
PARAMS = pltpu.CompilerParams(vmem_limit_bytes=60 * 1024 * 1024)


def shards(item_table, adagrad_state, history_ids, positive_ids):
    rows_dev, width = item_table.shape
    users_dev, hist_len = history_ids.shape
    devices = lax.axis_size("dp") * lax.axis_size("rows")
    groups = 2 * users_dev
    count = users_dev * (hist_len + 1)
    capacity = max(8, (count * 5 // (2 * devices) + 7) // 8 * 8)
    entries = devices * capacity
    asks = round_up(hist_len + 1, ROWS_AT_ONCE)
    data, shard = lax.axis_size("dp"), lax.axis_size("rows")
    sizes = line_sizes(data, shard)
    plane = devices // 2
    lines = sum(sizes) - 1
    unroll = max(n for n in (8, 16, 32, 64, 128) if capacity % n == 0)
    coef = penalty_weight / (rows_dev * devices)
    dma = pltpu.SemaphoreType.DMA
    list_shape = jax.ShapeDtypeStruct((devices, 1, capacity), i32)
    rows, codes, item_gram = pl.pallas_call(
        functools.partial(ask_kernel, data, shard, capacity),
        out_shape=(list_shape, list_shape, jax.ShapeDtypeStruct((width, width), f32)),
        in_specs=[VM, VM, HB],
        out_specs=(HB, HB, VM),
        scratch_shapes=[
            pltpu.VMEM((asks, users_dev), i32),
            pltpu.VMEM((4 * devices, capacity), f32),
            pltpu.VMEM((devices, 1, capacity), i32),
            pltpu.VMEM((devices, 1, capacity), i32),
            pltpu.VMEM((rows_dev, width), f32),
        ]
        + [dma((devices,))] * 4
        + [dma((3,))],
        compiler_params=pltpu.CompilerParams(
            vmem_limit_bytes=60 * 1024 * 1024, collective_id=1, has_side_effects=True
        ),
        name="ask",
    )(history_ids.T, positive_ids[None], item_table)
    flat = rows.reshape(-1)
    vals, user_gram = pl.pallas_call(
        functools.partial(exchange_kernel, sizes, capacity, users_dev, hist_len, coef, unroll),
        out_shape=(
            jax.ShapeDtypeStruct((devices, capacity, width), f32),
            jax.ShapeDtypeStruct((width, width), f32),
        ),
        in_specs=[HB, HB, VM, VM, HB],
        out_specs=(HB, VM),
        scratch_shapes=[
            pltpu.SMEM((entries,), i32),
            pltpu.SMEM((entries,), i32),
            pltpu.VMEM((rows_dev, width), f32),
            dma((3,)),
            pltpu.VMEM((capacity, width), f32),
            pltpu.VMEM((2, plane, 2, users_dev, width), f32),
            pltpu.VMEM((plane, 2, users_dev, width), f32),
            pltpu.VMEM((2, plane, users_dev, width), f32),
            pltpu.VMEM((devices, 2, users_dev, width), f32),
            pltpu.VMEM((groups + 8, width), f32),
            pltpu.VMEM((VSLOTS, capacity, width), f32),
            pltpu.VMEM((width, width), f32),
            pltpu.VMEM((2, 4, width // 2, width), f32),
            pltpu.VMEM((2, lines, width // 2, width), f32),
            pltpu.VMEM((2, width, width), f32),
            dma((plane,)),
            dma((plane,)),
            dma((2, plane)),
            dma((2, plane)),
            dma((2, plane)),
            dma((2, plane)),
            dma((plane,)),
            dma((plane,)),
            dma((2, lines)),
            dma((2, lines)),
            dma((VSLOTS,)),
        ],
        compiler_params=pltpu.CompilerParams(
            vmem_limit_bytes=60 * 1024 * 1024, collective_id=0, has_side_effects=True
        ),
        name="exchange",
    )(flat, codes.reshape(-1), codes, item_gram, item_table)
    chunk, tile = min(4096, entries), 512
    return pl.pallas_call(
        functools.partial(scatter_kernel, coef, chunk, 8, tile),
        out_shape=(
            jax.ShapeDtypeStruct(item_table.shape, f32),
            jax.ShapeDtypeStruct(item_table.shape, f32),
        ),
        in_specs=[HB, HB, VM, HB, HB],
        out_specs=(HB, HB),
        scratch_shapes=[
            pltpu.SMEM((entries,), i32),
            pltpu.VMEM((2, chunk, width), f32),
            pltpu.VMEM((rows_dev, width), f32),
            pltpu.VMEM((rows_dev, width), f32),
            dma((2,)),
            dma((3,)),
            dma((2, rows_dev // tile)),
        ]
        + [pltpu.VMEM((rows_dev, width), f32)] * STREAMS,
        compiler_params=PARAMS,
        name="scatter",
    )(flat, vals.reshape(entries, width), user_gram, item_table, adagrad_state)


def solution(mesh):
    return jax.shard_map(
        shards,
        mesh=mesh,
        in_specs=(
            P(("dp", "rows"), None),
            P(("dp", "rows"), None),
            P(("dp", "rows"), None),
            P(("dp", "rows")),
        ),
        out_specs=(P(("dp", "rows"), None), P(("dp", "rows"), None)),
        check_vma=False,
    )
```

```python
import functools

import jax
import jax.numpy as jnp
from jax import lax
from jax.experimental import pallas as pl
from jax.experimental.pallas import tpu as pltpu
from jax.sharding import PartitionSpec as P

penalty_weight = 10.0
step_size = 0.05
LOW = 128
STREAMS = 16
HIGHEST = lax.Precision.HIGHEST
f32, bf16, i32 = jnp.float32, jnp.bfloat16, jnp.int32


def round_up(value, unit):
    return (value + unit - 1) // unit * unit


def split2(x):
    hi = x.astype(bf16)
    return hi, (x - hi.astype(f32)).astype(bf16)


def ask_kernel(
    data, shard, capacity, hist_ref, pos_ref, item_ref, rows_ref, codes_ref, gram_ref,
    ids, acc, rows, codes, table_ref, row_send, row_recv, code_send, code_recv, own_sem,
):
    devices = data * shard
    hist_len, users_dev = hist_ref.shape
    width = item_ref.shape[1]
    dp, rw = lax.axis_index("dp"), lax.axis_index("rows")

    def each(first, count, act):
        def step(k, _):
            act(k)
            return 0

        lax.fori_loop(first, count, step, 0)

    me = dp * shard + rw
    rows_dev = item_ref.shape[0]
    item_copy = pltpu.make_async_copy(item_ref, table_ref, own_sem.at[2])
    item_copy.start()
    barrier = pltpu.get_barrier_semaphore()

    def place(n):
        return n // shard, lax.rem(n, shard)

    def greet(k):
        pl.semaphore_signal(
            barrier, inc=1, device_id=place(lax.rem(me + k, devices)), device_id_type=pl.DeviceIdType.MESH
        )

    each(1, devices, greet)
    asks = ids.shape[0]
    ids[0:hist_len, :] = hist_ref[...]
    ids[hist_len : hist_len + 1, :] = pos_ref[...]
    if asks > hist_len + 1:
        ids[hist_len + 1 :, :] = jnp.full((asks - hist_len - 1, users_dev), devices * rows_dev, i32)
    wide = ROWS_AT_ONCE * users_dev
    upper = (
        lax.broadcasted_iota(i32, (wide, wide), 0) <= lax.broadcasted_iota(i32, (wide, wide), 1)
    ).astype(bf16)
    owners = lax.broadcasted_iota(i32, (devices, wide), 0)
    ranks_to = lax.broadcasted_iota(i32, (capacity, wide), 0)
    lane = lax.broadcasted_iota(i32, (1, users_dev), 1)
    acc[...] = jnp.zeros_like(acc)

    def route(j, carry):
        parts = [ids[pl.ds(j * ROWS_AT_ONCE + q, 1), :] for q in range(ROWS_AT_ONCE)]
        codes = [
            (lane + jnp.where(j * ROWS_AT_ONCE + q >= hist_len, users_dev, 0)).astype(f32)
            for q in range(ROWS_AT_ONCE)
        ]
        want = jnp.concatenate(parts, axis=1)
        code = jnp.concatenate(codes, axis=1)
        owner = want // rows_dev
        local = want - owner * rows_dev
        high = (local // LOW).astype(f32)
        low = (local % LOW).astype(f32)
        member = (owner == owners).astype(f32)
        prefix = jnp.dot(member.astype(bf16), upper, preferred_element_type=f32)
        rank = jnp.sum(member * (prefix + carry), axis=0, keepdims=True) - 1.0
        left = jnp.concatenate([member * high, member * low, member * code, member], axis=0).astype(bf16)
        right = (rank.astype(i32) == ranks_to).astype(f32).astype(bf16)
        acc[...] += lax.dot_general(left, right, (((1,), (1,)), ((), ())), preferred_element_type=f32)
        return carry + jnp.sum(member, axis=1, keepdims=True)

    carry = jnp.zeros((devices, 1), f32)
    for j in range(asks // ROWS_AT_ONCE):
        carry = route(j, carry)

    def write(d):
        row = acc[pl.ds(d, 1), :] * LOW + acc[pl.ds(devices + d, 1), :]
        code = acc[pl.ds(2 * devices + d, 1), :]
        present = acc[pl.ds(3 * devices + d, 1), :]
        rows[d] = row.astype(i32)
        codes[d] = jnp.where(present > 0.5, code, 2.0 * users_dev).astype(i32)

    for d in range(devices):
        write(d)
    pl.semaphore_wait(barrier, devices - 1)

    def list_copies(k, to, at):
        return tuple(
            pltpu.make_async_remote_copy(
                src_ref=src.at[to], dst_ref=dst.at[at], send_sem=send.at[k], recv_sem=recv.at[k],
                device_id=place(to), device_id_type=pl.DeviceIdType.MESH,
            )
            for src, dst, send, recv in (
                (rows, rows_ref, row_send, row_recv),
                (codes, codes_ref, code_send, code_recv),
            )
        )

    def send_list(k):
        for copy in list_copies(k, lax.rem(me + k, devices), me):
            copy.start()

    each(1, devices, send_list)
    own = (
        pltpu.make_async_copy(rows.at[me], rows_ref.at[me], own_sem.at[0]),
        pltpu.make_async_copy(codes.at[me], codes_ref.at[me], own_sem.at[1]),
    )
    for copy in own:
        copy.start()
    item_copy.wait()
    tall = 512
    gram_ref[...] = jnp.zeros_like(gram_ref)

    def square(n):
        hi, lo = split2(table_ref[pl.ds(pl.multiple_of(n * tall, 8), tall), :])
        both = lax.dot_general(
            hi, jnp.concatenate([hi, lo], axis=1), (((0,), (0,)), ((), ())), preferred_element_type=f32
        )
        gram_ref[...] += both[:, :width] + (both[:, width:] + both[:, width:].T)

    each(0, rows_dev // tall, square)

    def finish(k):
        n = lax.rem(me - k + devices, devices)
        for copy in list_copies(k, n, n):
            copy.wait_recv()
            copy.wait_send()

    each(1, devices, finish)
    for copy in own:
        copy.wait()


def line_sizes(data, shard):
    cols = max(n for n in range(1, shard + 1) if shard % n == 0 and n * n <= shard)
    return data // 2, cols, shard // cols


ORDERS = ((0, 1, 2), (1, 0, 2))
LAGS = (2, 4, 6, 8)
VSLOTS = 4
ROWS_AT_ONCE = 8
TWIN_LAG = 2


def exchange_kernel(
    sizes, capacity, users_dev, hist_len, coef, unroll,
    rows_hbm, codes_hbm, hot_ref, gram_ref, item_ref, vals_ref, ugram_ref,
    rows_ref, codes_ref, table_ref, fetch_sem, picked, part, pair, mail, grads, cur, vbuf, upart, gsum, gmail, gfull,
    pair_send, pair_recv, mail_send, mail_recv, ag_send, ag_recv, twin_send, twin_recv, gram_send, gram_recv, vsem,
):
    nx, ny, nz = sizes
    plane = nx * ny * nz
    shard = ny * nz
    width = item_ref.shape[1]
    half = width // 2
    dp, rw = lax.axis_index("dp"), lax.axis_index("rows")
    core = lax.rem(dp, 2)
    pos = (dp // 2, lax.rem(rw, ny), rw // ny)
    origin = (0, 0, 0)
    axes = (0, 1, 2)

    def device(chip, c):
        return chip[0] * 2 + c, chip[2] * ny + chip[1]

    def block(chip, c):
        d, r = device(chip, c)
        return d * shard + r

    def ahead(r):
        return tuple(lax.rem(p + k, n) for p, k, n in zip(pos, r, sizes))

    def behind(o):
        return tuple(lax.rem(p - k + n, n) for p, k, n in zip(pos, o, sizes))

    def only(a, k):
        return tuple(k if b == a else 0 for b in axes)

    def add(r, a, k):
        return tuple(v + k if b == a else v for b, v in enumerate(r))

    def slot(r):
        return (r[0] * ny + r[1]) * nz + r[2]

    def ranked(n, digits):
        out = [0, 0, 0]
        for a in reversed(digits):
            out[a] = lax.rem(n, sizes[a])
            n = n // sizes[a]
        return tuple(out)

    partner = device(pos, 1 - core)

    def remote(src, dst, send, recv, dev):
        return pltpu.make_async_remote_copy(
            src_ref=src, dst_ref=dst, send_sem=send, recv_sem=recv,
            device_id=dev, device_id_type=pl.DeviceIdType.MESH,
        )

    def each(first, count, act):
        def step(k, _):
            act(k)
            return 0

        lax.fori_loop(first, count, step, 0)

    me = block(pos, core)
    devices = 2 * plane
    fetches = (
        pltpu.make_async_copy(rows_hbm, rows_ref, fetch_sem.at[0]),
        pltpu.make_async_copy(codes_hbm, codes_ref, fetch_sem.at[1]),
        pltpu.make_async_copy(item_ref, table_ref, fetch_sem.at[2]),
    )
    for fetch in fetches:
        fetch.start()
    barrier = pltpu.get_barrier_semaphore()
    greeted = 1
    pl.semaphore_signal(barrier, inc=1, device_id=partner, device_id_type=pl.DeviceIdType.MESH)
    for a in axes:
        for k in range(1, sizes[a]):
            greeted += 1
            pl.semaphore_signal(
                barrier, inc=1, device_id=device(ahead(only(a, k)), core), device_id_type=pl.DeviceIdType.MESH
            )
    pl.semaphore_wait(barrier, greeted)
    for fetch in fetches:
        fetch.wait()

    def pair_copy(at):
        return remote(part.at[0, at], pair.at[at], pair_send.at[at], pair_recv.at[at], partner)

    def letter(h, at, dev):
        return remote(part.at[1, at, h], mail.at[h, at], mail_send.at[h, at], mail_recv.at[h, at], dev)

    def parcel(h, at, b, dev):
        return remote(grads.at[b, h], grads.at[b, h], ag_send.at[h, at], ag_recv.at[h, at], dev)

    def twin(at, b):
        return remote(grads.at[b], grads.at[b], twin_send.at[at], twin_recv.at[at], partner)

    first = [1]
    for a in axes:
        first.append(first[-1] + sizes[a] - 1)
    last = first[3]
    mine = pl.ds(pl.multiple_of(core * half, 8), half)
    theirs = pl.ds(pl.multiple_of((1 - core) * half, 8), half)

    def gram_pair(t, src):
        return remote(src.at[theirs], gmail.at[t, 0], gram_send.at[t, 0], gram_recv.at[t, 0], partner)

    def gram_line(t, a, k):
        at = first[a] + k - 1
        return remote(
            gsum.at[t, a], gmail.at[t, at], gram_send.at[t, at], gram_recv.at[t, at], device(ahead(only(a, k)), core)
        )

    def gram_final(t):
        return remote(gsum.at[t, 3], gfull.at[t, mine], gram_send.at[t, last], gram_recv.at[t, last], partner)

    def gram_open(t, src):
        gram_pair(t, src).start()

    def gram_send_line(t, a):
        for k in range(1, sizes[a]):
            gram_line(t, a, k).start()

    def gram_step(t, src, stage):
        if stage == 0:
            gram_pair(t, src).wait_recv()
            gsum[t, 0] = src[mine, :] + gmail[t, 0]
        elif stage <= 3:
            a = stage - 1
            total = gsum[t, a]
            for k in range(1, sizes[a]):
                gram_line(t, a, k).wait_recv()
                total = total + gmail[t, first[a] + k - 1]
            gsum[t, a + 1] = total
        else:
            gram_final(t).wait_recv()
        if stage < 3:
            gram_send_line(t, stage)
        elif stage == 3:
            gram_final(t).start()
            gfull[t, mine] = gsum[t, 3]

    def gram_drain(t, src):
        gram_pair(t, src).wait_send()
        for a in axes:
            for k in range(1, sizes[a]):
                gram_line(t, a, k).wait_send()
        gram_final(t).wait_send()

    codes_to = lax.broadcasted_iota(i32, (2 * users_dev, capacity), 0)

    def gather(b, j, at):
        base = b * capacity

        def some(s, _):
            start = base + s * unroll
            for k in range(unroll):
                r = rows_ref.at[pl.ds(k, rows_ref.shape[0] - unroll + 1)][start]
                picked[pl.ds(s * unroll + k, 1), :] = table_ref[pl.ds(r, 1), :]
            return 0

        lax.fori_loop(0, capacity // unroll, some, 0)
        x = picked[...]
        hi, lo = split2(x)
        hot = (hot_ref[b] == codes_to).astype(f32).astype(bf16)
        both = jnp.dot(hot, jnp.concatenate([hi, lo], axis=1), preferred_element_type=f32)
        out = both[:, :width] + both[:, width:]
        part[j, at, 0] = out[:users_dev]
        part[j, at, 1] = out[users_dev:]

    def arrive(h, r, a):
        at = slot(r)
        for k in range(1, sizes[a]):
            m = slot(add(r, a, k))
            letter(h, m, partner).wait_recv()
            part[1, at, h] = part[1, at, h] + mail[h, m]

    def leave(h, r, a):
        @pl.when(r[a] != 0)
        def _():
            chip = tuple(lax.rem(p + r[a], n) if b == a else p for b, (p, n) in enumerate(zip(pos, sizes)))
            letter(h, slot(r), device(chip, core)).start()

    gram_open(0, gram_ref)

    def reduce_step(i, _):
        for stage in range(4):
            j = i - LAGS[stage]

            @pl.when(jnp.logical_and(j >= 0, j < plane))
            def _():
                r = ranked(plane - 1 - j, (2, 0, 1))
                at = slot(r)
                if stage == 0:
                    pair_copy(at).wait_recv()
                    for h in range(2):
                        part[1, at, h] = part[1, at, h] + pair[at, h]
                        leave(h, r, ORDERS[h][0])
                else:
                    for h in range(2):
                        order = ORDERS[h]
                        clear = r[order[0]] == 0
                        for a in order[1:stage]:
                            clear = jnp.logical_and(clear, r[a] == 0)

                        @pl.when(clear)
                        def _():
                            arrive(h, r, order[stage - 1])
                            if stage < 3:
                                leave(h, r, order[stage])

        for stage in range(5):
            @pl.when(i == 3 * stage + 3)
            def _():
                gram_step(0, gram_ref, stage)

        @pl.when(i < plane)
        def _():
            r = ranked(plane - 1 - i, (2, 0, 1))
            at = slot(r)
            chip = ahead(r)

            def one(j, _):
                c = (1 - core) * (1 - j) + core * j
                gather(block(chip, c), j, at)

                @pl.when(j == 0)
                def _():
                    pair_copy(at).start()

                return 0

            lax.fori_loop(0, 2, one, 0)

        return 0

    lax.fori_loop(0, plane + LAGS[3], reduce_step, 0)

    uv = part[1, 0, 0] / hist_len
    pv = part[1, 0, 1]
    gap = jnp.sum(uv * pv, axis=1, keepdims=True) - 1.0
    ug = 2.0 * gap * pv + 2.0 * coef * jnp.dot(uv, gfull[0], precision=HIGHEST, preferred_element_type=f32)
    grads[me, 0] = ug / hist_len
    grads[me, 1] = 2.0 * gap * uv

    def forward(h, o, b, a):
        for k in range(1, sizes[a]):
            chip = tuple(lax.rem(p + k, n) if c == a else p for c, (p, n) in enumerate(zip(pos, sizes)))
            parcel(h, slot(add(o, a, k)), b, device(chip, core)).start()

    ways = tuple(order[::-1] for order in ORDERS)
    line = ways[0][0]
    for k in range(1, sizes[line]):
        for h in range(2):
            parcel(h, slot(only(line, k)), me, device(ahead(only(line, k)), core)).start()
    for a in (1, 2):
        for h in range(2):
            forward(h, origin, me, ways[h][a])
    twin(0, me).start()
    upart[...] = lax.dot_general(
        uv, uv, (((0,), (0,)), ((), ())), precision=HIGHEST, preferred_element_type=f32
    )
    gram_open(1, upart)
    cur[pl.ds(2 * users_dev, 8), :] = jnp.zeros((8, width), f32)

    def vals_copy(v, b):
        return pltpu.make_async_copy(vbuf.at[v], vals_ref.at[b], vsem.at[v])

    def vals(n, kind, b):
        v = 2 * kind + lax.rem(n, 2)

        @pl.when(n >= 2)
        def _():
            vals_copy(v, b).wait()

        cur[pl.ds(0, users_dev), :] = grads[b, 0]
        cur[pl.ds(users_dev, users_dev), :] = grads[b, 1]
        base = b * capacity

        def some(s, _):
            start = base + s * unroll
            for k in range(unroll):
                c = codes_ref.at[pl.ds(k, codes_ref.shape[0] - unroll + 1)][start]
                vbuf[v, pl.ds(s * unroll + k, 1), :] = cur[pl.ds(c, 1), :]
            return 0

        lax.fori_loop(0, capacity // unroll, some, 0)
        vals_copy(v, b).start()

    digits = ((2, 0, 1), (2, 1, 0))
    delays = (-nx * ny, 1, 3)
    vals_delay = delays[2] + 1

    def spread(n, _):
        for h in range(2):
            a1, a2, a3 = ways[h]
            for level in (1, 2, 3):
                q = n - delays[level - 1]
                o = ranked(q, digits[h])
                if level == 1:
                    here = jnp.logical_and(o[a1] != 0, jnp.logical_and(o[a2] == 0, o[a3] == 0))
                elif level == 2:
                    here = jnp.logical_and(o[a2] != 0, o[a3] == 0)
                else:
                    here = o[a3] != 0

                @pl.when(jnp.logical_and(jnp.logical_and(q >= 0, q < plane), here))
                def _():
                    b = block(behind(o), core)
                    parcel(h, slot(o), b, partner).wait_recv()
                    for a in ways[h][level:]:
                        forward(h, o, b, a)

        def one(kind, _):
            j = n - vals_delay - TWIN_LAG * kind

            @pl.when(jnp.logical_and(j >= 0, j < plane))
            def _():
                o = ranked(j, digits[0])
                at = slot(o)
                b = block(behind(o), core + kind * (1 - 2 * core))

                @pl.when(jnp.logical_and(kind == 0, j > 0))
                def _():
                    twin(at, b).start()

                @pl.when(kind == 1)
                def _():
                    twin(at, b).wait_recv()

                vals(j, kind, b)

            return 0

        lax.fori_loop(0, 2, one, 0)

        for stage in range(5):
            @pl.when(n == 4 * stage + 3)
            def _():
                gram_step(1, upart, stage)

        return 0

    lax.fori_loop(0, plane + vals_delay + TWIN_LAG, spread, 0)
    ugram_ref[...] = gfull[1]

    def drain(n):
        pair_copy(n).wait_send()
        twin(n, me).wait_send()

    each(0, plane, drain)

    def drain_mail(n):
        for h in range(2):
            letter(h, n, partner).wait_send()
            parcel(h, n, me, partner).wait_send()

    each(1, plane, drain_mail)
    gram_drain(0, gram_ref)
    gram_drain(1, upart)
    each(0, VSLOTS, lambda v: vals_copy(v, me).wait())


def scatter_kernel(
    coef, chunk, unroll, tile,
    rows_hbm, vals_ref, ugram_ref, table_ref, state_ref, new_table_ref, new_state_ref,
    rows_ref, vbuf, table, state, vsem, in_sem, out_sem, *accs,
):
    entries = rows_ref.shape[0]
    chunks = entries // chunk
    part = chunk // len(accs)
    rows_dev, width = table.shape
    tiles = rows_dev // tile

    def vals_copy(n):
        s = lax.rem(n, 2)
        return pltpu.make_async_copy(
            vals_ref.at[pl.ds(pl.multiple_of(n * chunk, 8), chunk)], vbuf.at[s], vsem.at[s]
        )

    table_copy = pltpu.make_async_copy(table_ref, table, in_sem.at[0])
    state_copy = pltpu.make_async_copy(state_ref, state, in_sem.at[1])
    rows_copy = pltpu.make_async_copy(rows_hbm, rows_ref, in_sem.at[2])
    rows_copy.start()
    vals_copy(0).start()
    vals_copy(1).start()
    table_copy.start()
    state_copy.start()
    for acc in accs:
        acc[...] = jnp.zeros_like(acc)

    def one(n, _):
        v = lax.rem(n, 2)
        vals_copy(n).wait()

        def scatter(s, _):
            start = n * chunk + s * unroll
            for q in range(unroll):
                rows = [
                    rows_ref.at[pl.ds(k * part + q, entries - chunk + part - unroll + 1)][start] for k in range(len(accs))
                ]
                news = [
                    acc[pl.ds(r, 1), :] + vbuf[v, pl.ds(s * unroll + (k * part + q), 1), :]
                    for k, (acc, r) in enumerate(zip(accs, rows))
                ]
                for acc, r, new in zip(accs, rows, news):
                    acc[pl.ds(r, 1), :] = new
            return 0

        lax.fori_loop(0, part // unroll, scatter, 0)

        @pl.when(n + 2 < chunks)
        def _():
            vals_copy(n + 2).start()

        return 0

    rows_copy.wait()
    lax.fori_loop(0, chunks, one, 0)
    table_copy.wait()
    state_copy.wait()
    u0, u1 = split2(ugram_ref[...])
    u00 = jnp.concatenate([u0, u0], axis=0)

    def out_copy(t, which):
        at = pl.ds(pl.multiple_of(t * tile, 8), tile)
        src, dst = ((table, new_table_ref), (state, new_state_ref))[which]
        return pltpu.make_async_copy(src.at[at], dst.at[at], out_sem.at[which, t])

    def finish(t, _):
        at = pl.ds(pl.multiple_of(t * tile, 8), tile)
        item = table[at, :]
        t0, t1 = split2(item)
        g = jnp.dot(jnp.concatenate([t0, t1], axis=1), u00, preferred_element_type=f32)
        g = 2.0 * coef * (g + jnp.dot(t0, u1, preferred_element_type=f32))
        add = accs[0][at, :]
        for acc in accs[1:]:
            add = add + acc[at, :]
        g = g + add
        new = state[at, :] + g * g
        state[at, :] = new
        table[at, :] = item - step_size * g * lax.rsqrt(new)
        out_copy(t, 0).start()
        out_copy(t, 1).start()
        return 0

    lax.fori_loop(0, tiles, finish, 0)

    def drain(t, _):
        out_copy(t, 0).wait()
        out_copy(t, 1).wait()
        return 0

    lax.fori_loop(0, tiles, drain, 0)


VM = pl.BlockSpec(memory_space=pltpu.VMEM)
HB = pl.BlockSpec(memory_space=pl.ANY)
SM = pl.BlockSpec(memory_space=pltpu.SMEM)
PARAMS = pltpu.CompilerParams(vmem_limit_bytes=60 * 1024 * 1024)


def shards(item_table, adagrad_state, history_ids, positive_ids):
    rows_dev, width = item_table.shape
    users_dev, hist_len = history_ids.shape
    devices = lax.axis_size("dp") * lax.axis_size("rows")
    groups = 2 * users_dev
    count = users_dev * (hist_len + 1)
    capacity = max(8, (count * 5 // (2 * devices) + 7) // 8 * 8)
    entries = devices * capacity
    asks = round_up(hist_len + 1, ROWS_AT_ONCE)
    data, shard = lax.axis_size("dp"), lax.axis_size("rows")
    sizes = line_sizes(data, shard)
    plane = devices // 2
    lines = sum(sizes) - 1
    unroll = max(n for n in (8, 16, 32, 64, 128) if capacity % n == 0)
    coef = penalty_weight / (rows_dev * devices)
    dma = pltpu.SemaphoreType.DMA
    list_shape = jax.ShapeDtypeStruct((devices, 1, capacity), i32)
    rows, codes, item_gram = pl.pallas_call(
        functools.partial(ask_kernel, data, shard, capacity),
        out_shape=(list_shape, list_shape, jax.ShapeDtypeStruct((width, width), f32)),
        in_specs=[VM, VM, HB],
        out_specs=(HB, HB, VM),
        scratch_shapes=[
            pltpu.VMEM((asks, users_dev), i32),
            pltpu.VMEM((4 * devices, capacity), f32),
            pltpu.VMEM((devices, 1, capacity), i32),
            pltpu.VMEM((devices, 1, capacity), i32),
            pltpu.VMEM((rows_dev, width), f32),
        ]
        + [dma((devices,))] * 4
        + [dma((3,))],
        compiler_params=pltpu.CompilerParams(
            vmem_limit_bytes=60 * 1024 * 1024, collective_id=1, has_side_effects=True
        ),
        name="ask",
    )(history_ids.T, positive_ids[None], item_table)
    flat = rows.reshape(-1)
    vals, user_gram = pl.pallas_call(
        functools.partial(exchange_kernel, sizes, capacity, users_dev, hist_len, coef, unroll),
        out_shape=(
            jax.ShapeDtypeStruct((devices, capacity, width), f32),
            jax.ShapeDtypeStruct((width, width), f32),
        ),
        in_specs=[HB, HB, VM, VM, HB],
        out_specs=(HB, VM),
        scratch_shapes=[
            pltpu.SMEM((entries,), i32),
            pltpu.SMEM((entries,), i32),
            pltpu.VMEM((rows_dev, width), f32),
            dma((3,)),
            pltpu.VMEM((capacity, width), f32),
            pltpu.VMEM((2, plane, 2, users_dev, width), f32),
            pltpu.VMEM((plane, 2, users_dev, width), f32),
            pltpu.VMEM((2, plane, users_dev, width), f32),
            pltpu.VMEM((devices, 2, users_dev, width), f32),
            pltpu.VMEM((groups + 8, width), f32),
            pltpu.VMEM((VSLOTS, capacity, width), f32),
            pltpu.VMEM((width, width), f32),
            pltpu.VMEM((2, 4, width // 2, width), f32),
            pltpu.VMEM((2, lines, width // 2, width), f32),
            pltpu.VMEM((2, width, width), f32),
            dma((plane,)),
            dma((plane,)),
            dma((2, plane)),
            dma((2, plane)),
            dma((2, plane)),
            dma((2, plane)),
            dma((plane,)),
            dma((plane,)),
            dma((2, lines)),
            dma((2, lines)),
            dma((VSLOTS,)),
        ],
        compiler_params=pltpu.CompilerParams(
            vmem_limit_bytes=60 * 1024 * 1024, collective_id=0, has_side_effects=True
        ),
        name="exchange",
    )(flat, codes.reshape(-1), codes, item_gram, item_table)
    chunk, tile = min(4096, entries), 512
    return pl.pallas_call(
        functools.partial(scatter_kernel, coef, chunk, 8, tile),
        out_shape=(
            jax.ShapeDtypeStruct(item_table.shape, f32),
            jax.ShapeDtypeStruct(item_table.shape, f32),
        ),
        in_specs=[HB, HB, VM, HB, HB],
        out_specs=(HB, HB),
        scratch_shapes=[
            pltpu.SMEM((entries,), i32),
            pltpu.VMEM((2, chunk, width), f32),
            pltpu.VMEM((rows_dev, width), f32),
            pltpu.VMEM((rows_dev, width), f32),
            dma((2,)),
            dma((3,)),
            dma((2, rows_dev // tile)),
        ]
        + [pltpu.VMEM((rows_dev, width), f32)] * STREAMS,
        compiler_params=PARAMS,
        name="scatter",
    )(flat, vals.reshape(entries, width), user_gram, item_table, adagrad_state)


def solution(mesh):
    return jax.shard_map(
        shards,
        mesh=mesh,
        in_specs=(
            P(("dp", "rows"), None),
            P(("dp", "rows"), None),
            P(("dp", "rows"), None),
            P(("dp", "rows")),
        ),
        out_specs=(P(("dp", "rows"), None), P(("dp", "rows"), None)),
        check_vma=False,
    )
```

```python
import functools

import jax
import jax.numpy as jnp
from jax import lax
from jax.experimental import pallas as pl
from jax.experimental.pallas import tpu as pltpu
from jax.sharding import PartitionSpec as P

penalty_weight = 10.0
step_size = 0.05
LOW = 128
STREAMS = 16
HIGHEST = lax.Precision.HIGHEST
f32, bf16, i32 = jnp.float32, jnp.bfloat16, jnp.int32


def round_up(value, unit):
    return (value + unit - 1) // unit * unit


def split2(x):
    hi = x.astype(bf16)
    return hi, (x - hi.astype(f32)).astype(bf16)


def ask_kernel(
    data, shard, capacity, hist_ref, pos_ref, item_ref, rows_ref, codes_ref, gram_hbm,
    gram_ref, ids, acc, rows, codes, table_ref, row_send, row_recv, code_send, code_recv, own_sem,
):
    devices = data * shard
    hist_len, users_dev = hist_ref.shape
    width = item_ref.shape[1]
    dp, rw = lax.axis_index("dp"), lax.axis_index("rows")

    def each(first, count, act):
        def step(k, _):
            act(k)
            return 0

        lax.fori_loop(first, count, step, 0)

    me = dp * shard + rw
    rows_dev = item_ref.shape[0]
    item_copy = pltpu.make_async_copy(item_ref, table_ref, own_sem.at[2])
    item_copy.start()
    barrier = pltpu.get_barrier_semaphore()

    def place(n):
        return n // shard, lax.rem(n, shard)

    def greet(k):
        pl.semaphore_signal(
            barrier, inc=1, device_id=place(lax.rem(me + k, devices)), device_id_type=pl.DeviceIdType.MESH
        )

    each(1, devices, greet)
    asks = ids.shape[0]
    ids[0:hist_len, :] = hist_ref[...]
    ids[hist_len : hist_len + 1, :] = pos_ref[...]
    if asks > hist_len + 1:
        ids[hist_len + 1 :, :] = jnp.full((asks - hist_len - 1, users_dev), devices * rows_dev, i32)
    wide = ROWS_AT_ONCE * users_dev
    upper = (
        lax.broadcasted_iota(i32, (wide, wide), 0) <= lax.broadcasted_iota(i32, (wide, wide), 1)
    ).astype(bf16)
    owners = lax.broadcasted_iota(i32, (devices, wide), 0)
    ranks_to = lax.broadcasted_iota(i32, (capacity, wide), 0)
    lane = lax.broadcasted_iota(i32, (1, users_dev), 1)
    acc[...] = jnp.zeros_like(acc)

    def route(j, carry):
        parts = [ids[pl.ds(j * ROWS_AT_ONCE + q, 1), :] for q in range(ROWS_AT_ONCE)]
        codes = [
            (lane + jnp.where(j * ROWS_AT_ONCE + q >= hist_len, users_dev, 0)).astype(f32)
            for q in range(ROWS_AT_ONCE)
        ]
        want = jnp.concatenate(parts, axis=1)
        code = jnp.concatenate(codes, axis=1)
        owner = want // rows_dev
        local = want - owner * rows_dev
        high = (local // LOW).astype(f32)
        low = (local % LOW).astype(f32)
        member = (owner == owners).astype(f32)
        prefix = jnp.dot(member.astype(bf16), upper, preferred_element_type=f32)
        rank = jnp.sum(member * (prefix + carry), axis=0, keepdims=True) - 1.0
        left = jnp.concatenate([member * high, member * low, member * code, member], axis=0).astype(bf16)
        right = (rank.astype(i32) == ranks_to).astype(f32).astype(bf16)
        acc[...] += lax.dot_general(left, right, (((1,), (1,)), ((), ())), preferred_element_type=f32)
        return carry + jnp.sum(member, axis=1, keepdims=True)

    carry = jnp.zeros((devices, 1), f32)
    for j in range(asks // ROWS_AT_ONCE):
        carry = route(j, carry)

    def write(d):
        row = acc[pl.ds(d, 1), :] * LOW + acc[pl.ds(devices + d, 1), :]
        code = acc[pl.ds(2 * devices + d, 1), :]
        present = acc[pl.ds(3 * devices + d, 1), :]
        rows[d] = row.astype(i32)
        codes[d] = jnp.where(present > 0.5, code, 2.0 * users_dev).astype(i32)

    for d in range(devices):
        write(d)
    pl.semaphore_wait(barrier, devices - 1)

    def list_copies(k, to, at):
        return tuple(
            pltpu.make_async_remote_copy(
                src_ref=src.at[to], dst_ref=dst.at[at], send_sem=send.at[k], recv_sem=recv.at[k],
                device_id=place(to), device_id_type=pl.DeviceIdType.MESH,
            )
            for src, dst, send, recv in (
                (rows, rows_ref, row_send, row_recv),
                (codes, codes_ref, code_send, code_recv),
            )
        )

    def send_list(k):
        for copy in list_copies(k, lax.rem(me + k, devices), me):
            copy.start()

    each(1, devices, send_list)
    own = (
        pltpu.make_async_copy(rows.at[me], rows_ref.at[me], own_sem.at[0]),
        pltpu.make_async_copy(codes.at[me], codes_ref.at[me], own_sem.at[1]),
    )
    for copy in own:
        copy.start()
    item_copy.wait()
    tall = 512
    gram_ref[...] = jnp.zeros_like(gram_ref)

    def square(n):
        hi, lo = split2(table_ref[pl.ds(pl.multiple_of(n * tall, 8), tall), :])
        both = lax.dot_general(
            hi, jnp.concatenate([hi, lo], axis=1), (((0,), (0,)), ((), ())), preferred_element_type=f32
        )
        gram_ref[...] += both[:, :width] + (both[:, width:] + both[:, width:].T)

    each(0, rows_dev // tall, square)
    gram_copy = pltpu.make_async_copy(gram_ref, gram_hbm, own_sem.at[3])
    gram_copy.start()

    def finish(k):
        n = lax.rem(me - k + devices, devices)
        for copy in list_copies(k, n, n):
            copy.wait_recv()
            copy.wait_send()

    each(1, devices, finish)
    for copy in own:
        copy.wait()
    gram_copy.wait()


def line_sizes(data, shard):
    cols = max(n for n in range(1, shard + 1) if shard % n == 0 and n * n <= shard)
    return data // 2, cols, shard // cols


ORDERS = ((0, 1, 2), (1, 0, 2))
LAGS = (2, 4, 6, 8)
VSLOTS = 4
ROWS_AT_ONCE = 8
TWIN_LAG = 2


def exchange_kernel(
    sizes, capacity, users_dev, hist_len, coef, unroll,
    rows_hbm, codes_hbm, hot_hbm, gram_hbm, item_ref, vals_ref, ugram_hbm,
    rows_ref, codes_ref, hot_ref, gram_ref, table_ref, fetch_sem, picked, part, pair, mail, grads, cur, vbuf, upart, gsum, gmail, gfull,
    pair_send, pair_recv, mail_send, mail_recv, ag_send, ag_recv, twin_send, twin_recv, gram_send, gram_recv, vsem,
):
    nx, ny, nz = sizes
    plane = nx * ny * nz
    shard = ny * nz
    width = item_ref.shape[1]
    half = width // 2
    dp, rw = lax.axis_index("dp"), lax.axis_index("rows")
    core = lax.rem(dp, 2)
    pos = (dp // 2, lax.rem(rw, ny), rw // ny)
    origin = (0, 0, 0)
    axes = (0, 1, 2)

    def device(chip, c):
        return chip[0] * 2 + c, chip[2] * ny + chip[1]

    def block(chip, c):
        d, r = device(chip, c)
        return d * shard + r

    def ahead(r):
        return tuple(lax.rem(p + k, n) for p, k, n in zip(pos, r, sizes))

    def behind(o):
        return tuple(lax.rem(p - k + n, n) for p, k, n in zip(pos, o, sizes))

    def only(a, k):
        return tuple(k if b == a else 0 for b in axes)

    def add(r, a, k):
        return tuple(v + k if b == a else v for b, v in enumerate(r))

    def slot(r):
        return (r[0] * ny + r[1]) * nz + r[2]

    def ranked(n, digits):
        out = [0, 0, 0]
        for a in reversed(digits):
            out[a] = lax.rem(n, sizes[a])
            n = lax.div(n, sizes[a])
        return tuple(out)

    partner = device(pos, 1 - core)

    def remote(src, dst, send, recv, dev):
        return pltpu.make_async_remote_copy(
            src_ref=src, dst_ref=dst, send_sem=send, recv_sem=recv,
            device_id=dev, device_id_type=pl.DeviceIdType.MESH,
        )

    def each(first, count, act):
        def step(k, _):
            act(k)
            return 0

        lax.fori_loop(first, count, step, 0)

    me = block(pos, core)
    devices = 2 * plane
    fetches = (
        pltpu.make_async_copy(rows_hbm, rows_ref, fetch_sem.at[0]),
        pltpu.make_async_copy(codes_hbm, codes_ref, fetch_sem.at[1]),
        pltpu.make_async_copy(item_ref, table_ref, fetch_sem.at[2]),
        pltpu.make_async_copy(hot_hbm, hot_ref, fetch_sem.at[3]),
        pltpu.make_async_copy(gram_hbm, gram_ref, fetch_sem.at[4]),
    )
    for fetch in fetches:
        fetch.start()
    barrier = pltpu.get_barrier_semaphore()
    greeted = 1
    pl.semaphore_signal(barrier, inc=1, device_id=partner, device_id_type=pl.DeviceIdType.MESH)
    for a in axes:
        for k in range(1, sizes[a]):
            greeted += 1
            pl.semaphore_signal(
                barrier, inc=1, device_id=device(ahead(only(a, k)), core), device_id_type=pl.DeviceIdType.MESH
            )
    pl.semaphore_wait(barrier, greeted)
    for fetch in fetches:
        fetch.wait()

    def pair_copy(at):
        return remote(part.at[0, at], pair.at[at], pair_send.at[at], pair_recv.at[at], partner)

    def letter(h, at, dev):
        return remote(part.at[1, at, h], mail.at[h, at], mail_send.at[h, at], mail_recv.at[h, at], dev)

    def parcel(h, at, b, dev):
        return remote(grads.at[b, h], grads.at[b, h], ag_send.at[h, at], ag_recv.at[h, at], dev)

    def twin(at, b):
        return remote(grads.at[b], grads.at[b], twin_send.at[at], twin_recv.at[at], partner)

    first = [1]
    for a in axes:
        first.append(first[-1] + sizes[a] - 1)
    last = first[3]
    mine = pl.ds(pl.multiple_of(core * half, 8), half)
    theirs = pl.ds(pl.multiple_of((1 - core) * half, 8), half)

    def gram_pair(t, src):
        return remote(src.at[theirs], gmail.at[t, 0], gram_send.at[t, 0], gram_recv.at[t, 0], partner)

    def gram_line(t, a, k):
        at = first[a] + k - 1
        return remote(
            gsum.at[t, a], gmail.at[t, at], gram_send.at[t, at], gram_recv.at[t, at], device(ahead(only(a, k)), core)
        )

    def gram_final(t):
        return remote(gsum.at[t, 3], gfull.at[t, mine], gram_send.at[t, last], gram_recv.at[t, last], partner)

    def gram_open(t, src):
        gram_pair(t, src).start()

    def gram_send_line(t, a):
        for k in range(1, sizes[a]):
            gram_line(t, a, k).start()

    def gram_step(t, src, stage):
        if stage == 0:
            gram_pair(t, src).wait_recv()
            gsum[t, 0] = src[mine, :] + gmail[t, 0]
        elif stage <= 3:
            a = stage - 1
            total = gsum[t, a]
            for k in range(1, sizes[a]):
                gram_line(t, a, k).wait_recv()
                total = total + gmail[t, first[a] + k - 1]
            gsum[t, a + 1] = total
        else:
            gram_final(t).wait_recv()
        if stage < 3:
            gram_send_line(t, stage)
        elif stage == 3:
            gram_final(t).start()
            gfull[t, mine] = gsum[t, 3]

    def gram_drain(t, src):
        gram_pair(t, src).wait_send()
        for a in axes:
            for k in range(1, sizes[a]):
                gram_line(t, a, k).wait_send()
        gram_final(t).wait_send()

    codes_to = lax.broadcasted_iota(i32, (2 * users_dev, capacity), 0)

    def gather(b, j, at):
        base = b * capacity

        def some(s, _):
            start = base + s * unroll
            for k in range(unroll):
                r = rows_ref.at[pl.ds(k, rows_ref.shape[0] - unroll + 1)][start]
                picked[pl.ds(s * unroll + k, 1), :] = table_ref[pl.ds(r, 1), :]
            return 0

        lax.fori_loop(0, capacity // unroll, some, 0)
        x = picked[...]
        hi, lo = split2(x)
        hot = (hot_ref[b] == codes_to).astype(f32).astype(bf16)
        both = jnp.dot(hot, jnp.concatenate([hi, lo], axis=1), preferred_element_type=f32)
        out = both[:, :width] + both[:, width:]
        part[j, at, 0] = out[:users_dev]
        part[j, at, 1] = out[users_dev:]

    def arrive(h, r, a):
        at = slot(r)
        for k in range(1, sizes[a]):
            m = slot(add(r, a, k))
            letter(h, m, partner).wait_recv()
            part[1, at, h] = part[1, at, h] + mail[h, m]

    def leave(h, r, a):
        @pl.when(r[a] != 0)
        def _():
            chip = tuple(lax.rem(p + r[a], n) if b == a else p for b, (p, n) in enumerate(zip(pos, sizes)))
            letter(h, slot(r), device(chip, core)).start()

    gram_open(0, gram_ref)

    def reduce_step(i, _):
        for stage in range(4):
            j = i - LAGS[stage]

            @pl.when(jnp.logical_and(j >= 0, j < plane))
            def _():
                r = ranked(plane - 1 - j, (2, 0, 1))
                at = slot(r)
                if stage == 0:
                    pair_copy(at).wait_recv()
                    for h in range(2):
                        part[1, at, h] = part[1, at, h] + pair[at, h]
                        leave(h, r, ORDERS[h][0])
                else:
                    for h in range(2):
                        order = ORDERS[h]
                        clear = r[order[0]] == 0
                        for a in order[1:stage]:
                            clear = jnp.logical_and(clear, r[a] == 0)

                        @pl.when(clear)
                        def _():
                            arrive(h, r, order[stage - 1])
                            if stage < 3:
                                leave(h, r, order[stage])

        for stage in range(5):
            @pl.when(i == 3 * stage + 3)
            def _():
                gram_step(0, gram_ref, stage)

        @pl.when(i < plane)
        def _():
            r = ranked(plane - 1 - i, (2, 0, 1))
            at = slot(r)
            chip = ahead(r)

            def one(j, _):
                c = (1 - core) * (1 - j) + core * j
                gather(block(chip, c), j, at)

                @pl.when(j == 0)
                def _():
                    pair_copy(at).start()

                return 0

            lax.fori_loop(0, 2, one, 0)

        return 0

    lax.fori_loop(0, plane + LAGS[3], reduce_step, 0)

    uv = part[1, 0, 0] / hist_len
    pv = part[1, 0, 1]
    gap = jnp.sum(uv * pv, axis=1, keepdims=True) - 1.0
    ug = 2.0 * gap * pv + 2.0 * coef * jnp.dot(uv, gfull[0], precision=HIGHEST, preferred_element_type=f32)
    grads[me, 0] = ug / hist_len
    grads[me, 1] = 2.0 * gap * uv

    def forward(h, o, b, a):
        for k in range(1, sizes[a]):
            chip = tuple(lax.rem(p + k, n) if c == a else p for c, (p, n) in enumerate(zip(pos, sizes)))
            parcel(h, slot(add(o, a, k)), b, device(chip, core)).start()

    ways = tuple(order[::-1] for order in ORDERS)
    line = ways[0][0]
    for k in range(1, sizes[line]):
        for h in range(2):
            parcel(h, slot(only(line, k)), me, device(ahead(only(line, k)), core)).start()
    for a in (1, 2):
        for h in range(2):
            forward(h, origin, me, ways[h][a])
    twin(0, me).start()
    upart[...] = lax.dot_general(
        uv, uv, (((0,), (0,)), ((), ())), precision=HIGHEST, preferred_element_type=f32
    )
    gram_open(1, upart)
    cur[pl.ds(2 * users_dev, 8), :] = jnp.zeros((8, width), f32)

    def vals_copy(v, b):
        return pltpu.make_async_copy(vbuf.at[v], vals_ref.at[b], vsem.at[v])

    def vals(n, kind, b):
        v = 2 * kind + lax.rem(n, 2)

        @pl.when(n >= 2)
        def _():
            vals_copy(v, b).wait()

        cur[pl.ds(0, users_dev), :] = grads[b, 0]
        cur[pl.ds(users_dev, users_dev), :] = grads[b, 1]
        base = b * capacity

        def some(s, _):
            start = base + s * unroll
            for k in range(unroll):
                c = codes_ref.at[pl.ds(k, codes_ref.shape[0] - unroll + 1)][start]
                vbuf[v, pl.ds(s * unroll + k, 1), :] = cur[pl.ds(c, 1), :]
            return 0

        lax.fori_loop(0, capacity // unroll, some, 0)
        vals_copy(v, b).start()

    digits = ((2, 0, 1), (2, 1, 0))
    delays = (-nx * ny, 1, 3)
    vals_delay = delays[2] + 1

    def spread(n, _):
        for h in range(2):
            a1, a2, a3 = ways[h]
            for level in (1, 2, 3):
                q = n - delays[level - 1]
                o = ranked(q, digits[h])
                if level == 1:
                    here = jnp.logical_and(o[a1] != 0, jnp.logical_and(o[a2] == 0, o[a3] == 0))
                elif level == 2:
                    here = jnp.logical_and(o[a2] != 0, o[a3] == 0)
                else:
                    here = o[a3] != 0

                @pl.when(jnp.logical_and(jnp.logical_and(q >= 0, q < plane), here))
                def _():
                    b = block(behind(o), core)
                    parcel(h, slot(o), b, partner).wait_recv()
                    for a in ways[h][level:]:
                        forward(h, o, b, a)

        def one(kind, _):
            j = n - vals_delay - TWIN_LAG * kind

            @pl.when(jnp.logical_and(j >= 0, j < plane))
            def _():
                o = ranked(j, digits[0])
                at = slot(o)
                b = block(behind(o), core + kind * (1 - 2 * core))

                @pl.when(jnp.logical_and(kind == 0, j > 0))
                def _():
                    twin(at, b).start()

                @pl.when(kind == 1)
                def _():
                    twin(at, b).wait_recv()

                vals(j, kind, b)

            return 0

        lax.fori_loop(0, 2, one, 0)

        for stage in range(5):
            @pl.when(n == 4 * stage + 3)
            def _():
                gram_step(1, upart, stage)

        return 0

    lax.fori_loop(0, plane + vals_delay + TWIN_LAG, spread, 0)
    ugram_copy = pltpu.make_async_copy(gfull.at[1], ugram_hbm, fetch_sem.at[5])
    ugram_copy.start()

    def drain(n):
        pair_copy(n).wait_send()
        twin(n, me).wait_send()

    each(0, plane, drain)

    def drain_mail(n):
        for h in range(2):
            letter(h, n, partner).wait_send()
            parcel(h, n, me, partner).wait_send()

    each(1, plane, drain_mail)
    gram_drain(0, gram_ref)
    gram_drain(1, upart)
    each(0, VSLOTS, lambda v: vals_copy(v, me).wait())
    ugram_copy.wait()


def scatter_kernel(
    coef, chunk, unroll, tile,
    rows_hbm, vals_ref, ugram_hbm, table_ref, state_ref, new_table_ref, new_state_ref,
    rows_ref, ugram_ref, vbuf, table, state, vsem, in_sem, out_sem, *accs,
):
    entries = rows_ref.shape[0]
    chunks = entries // chunk
    part = chunk // len(accs)
    rows_dev, width = table.shape
    tiles = rows_dev // tile

    def vals_copy(n):
        s = lax.rem(n, 2)
        return pltpu.make_async_copy(
            vals_ref.at[pl.ds(pl.multiple_of(n * chunk, 8), chunk)], vbuf.at[s], vsem.at[s]
        )

    table_copy = pltpu.make_async_copy(table_ref, table, in_sem.at[0])
    state_copy = pltpu.make_async_copy(state_ref, state, in_sem.at[1])
    rows_copy = pltpu.make_async_copy(rows_hbm, rows_ref, in_sem.at[2])
    ugram_copy = pltpu.make_async_copy(ugram_hbm, ugram_ref, in_sem.at[3])
    rows_copy.start()
    vals_copy(0).start()
    vals_copy(1).start()
    table_copy.start()
    state_copy.start()
    ugram_copy.start()
    for acc in accs:
        acc[...] = jnp.zeros_like(acc)

    def one(n, _):
        v = lax.rem(n, 2)
        vals_copy(n).wait()

        def scatter(s, _):
            start = n * chunk + s * unroll
            for q in range(unroll):
                rows = [
                    rows_ref.at[pl.ds(k * part + q, entries - chunk + part - unroll + 1)][start] for k in range(len(accs))
                ]
                news = [
                    acc[pl.ds(r, 1), :] + vbuf[v, pl.ds(s * unroll + (k * part + q), 1), :]
                    for k, (acc, r) in enumerate(zip(accs, rows))
                ]
                for acc, r, new in zip(accs, rows, news):
                    acc[pl.ds(r, 1), :] = new
            return 0

        lax.fori_loop(0, part // unroll, scatter, 0)

        @pl.when(n + 2 < chunks)
        def _():
            vals_copy(n + 2).start()

        return 0

    rows_copy.wait()
    lax.fori_loop(0, chunks, one, 0)
    table_copy.wait()
    state_copy.wait()
    ugram_copy.wait()
    u0, u1 = split2(ugram_ref[...])
    u00 = jnp.concatenate([u0, u0], axis=0)

    def out_copy(t, which):
        at = pl.ds(pl.multiple_of(t * tile, 8), tile)
        src, dst = ((table, new_table_ref), (state, new_state_ref))[which]
        return pltpu.make_async_copy(src.at[at], dst.at[at], out_sem.at[which, t])

    def finish(t, _):
        at = pl.ds(pl.multiple_of(t * tile, 8), tile)
        item = table[at, :]
        t0, t1 = split2(item)
        g = jnp.dot(jnp.concatenate([t0, t1], axis=1), u00, preferred_element_type=f32)
        g = 2.0 * coef * (g + jnp.dot(t0, u1, preferred_element_type=f32))
        add = accs[0][at, :]
        for acc in accs[1:]:
            add = add + acc[at, :]
        g = g + add
        new = state[at, :] + g * g
        state[at, :] = new
        table[at, :] = item - step_size * g * lax.rsqrt(new)
        out_copy(t, 0).start()
        out_copy(t, 1).start()
        return 0

    lax.fori_loop(0, tiles, finish, 0)

    def drain(t, _):
        out_copy(t, 0).wait()
        out_copy(t, 1).wait()
        return 0

    lax.fori_loop(0, tiles, drain, 0)


VM = pl.BlockSpec(memory_space=pltpu.VMEM)
HB = pl.BlockSpec(memory_space=pl.ANY)
SM = pl.BlockSpec(memory_space=pltpu.SMEM)
PARAMS = pltpu.CompilerParams(vmem_limit_bytes=60 * 1024 * 1024)


def shards(item_table, adagrad_state, history_ids, positive_ids):
    rows_dev, width = item_table.shape
    users_dev, hist_len = history_ids.shape
    devices = lax.axis_size("dp") * lax.axis_size("rows")
    groups = 2 * users_dev
    count = users_dev * (hist_len + 1)
    capacity = max(8, (count * 5 // (2 * devices) + 7) // 8 * 8)
    entries = devices * capacity
    asks = round_up(hist_len + 1, ROWS_AT_ONCE)
    data, shard = lax.axis_size("dp"), lax.axis_size("rows")
    sizes = line_sizes(data, shard)
    plane = devices // 2
    lines = sum(sizes) - 1
    unroll = max(n for n in (8, 16, 32, 64, 128) if capacity % n == 0)
    coef = penalty_weight / (rows_dev * devices)
    dma = pltpu.SemaphoreType.DMA
    list_shape = jax.ShapeDtypeStruct((devices, 1, capacity), i32)
    rows, codes, item_gram = pl.pallas_call(
        functools.partial(ask_kernel, data, shard, capacity),
        out_shape=(list_shape, list_shape, jax.ShapeDtypeStruct((width, width), f32)),
        in_specs=[VM, VM, HB],
        out_specs=(HB, HB, HB),
        scratch_shapes=[
            pltpu.VMEM((width, width), f32),
            pltpu.VMEM((asks, users_dev), i32),
            pltpu.VMEM((4 * devices, capacity), f32),
            pltpu.VMEM((devices, 1, capacity), i32),
            pltpu.VMEM((devices, 1, capacity), i32),
            pltpu.VMEM((rows_dev, width), f32),
        ]
        + [dma((devices,))] * 4
        + [dma((4,))],
        compiler_params=pltpu.CompilerParams(
            vmem_limit_bytes=60 * 1024 * 1024, collective_id=1, has_side_effects=True
        ),
        name="ask",
    )(history_ids.T, positive_ids[None], item_table)
    flat = rows.reshape(-1)
    vals, user_gram = pl.pallas_call(
        functools.partial(exchange_kernel, sizes, capacity, users_dev, hist_len, coef, unroll),
        out_shape=(
            jax.ShapeDtypeStruct((devices, capacity, width), f32),
            jax.ShapeDtypeStruct((width, width), f32),
        ),
        in_specs=[HB, HB, HB, HB, HB],
        out_specs=(HB, HB),
        scratch_shapes=[
            pltpu.SMEM((entries,), i32),
            pltpu.SMEM((entries,), i32),
            pltpu.VMEM((devices, 1, capacity), i32),
            pltpu.VMEM((width, width), f32),
            pltpu.VMEM((rows_dev, width), f32),
            dma((6,)),
            pltpu.VMEM((capacity, width), f32),
            pltpu.VMEM((2, plane, 2, users_dev, width), f32),
            pltpu.VMEM((plane, 2, users_dev, width), f32),
            pltpu.VMEM((2, plane, users_dev, width), f32),
            pltpu.VMEM((devices, 2, users_dev, width), f32),
            pltpu.VMEM((groups + 8, width), f32),
            pltpu.VMEM((VSLOTS, capacity, width), f32),
            pltpu.VMEM((width, width), f32),
            pltpu.VMEM((2, 4, width // 2, width), f32),
            pltpu.VMEM((2, lines, width // 2, width), f32),
            pltpu.VMEM((2, width, width), f32),
            dma((plane,)),
            dma((plane,)),
            dma((2, plane)),
            dma((2, plane)),
            dma((2, plane)),
            dma((2, plane)),
            dma((plane,)),
            dma((plane,)),
            dma((2, lines)),
            dma((2, lines)),
            dma((VSLOTS,)),
        ],
        compiler_params=pltpu.CompilerParams(
            vmem_limit_bytes=60 * 1024 * 1024, collective_id=0, has_side_effects=True
        ),
        name="exchange",
    )(flat, codes.reshape(-1), codes, item_gram, item_table)
    chunk, tile = min(4096, entries), 512
    return pl.pallas_call(
        functools.partial(scatter_kernel, coef, chunk, 8, tile),
        out_shape=(
            jax.ShapeDtypeStruct(item_table.shape, f32),
            jax.ShapeDtypeStruct(item_table.shape, f32),
        ),
        in_specs=[HB, HB, HB, HB, HB],
        out_specs=(HB, HB),
        scratch_shapes=[
            pltpu.SMEM((entries,), i32),
            pltpu.VMEM((width, width), f32),
            pltpu.VMEM((2, chunk, width), f32),
            pltpu.VMEM((rows_dev, width), f32),
            pltpu.VMEM((rows_dev, width), f32),
            dma((2,)),
            dma((4,)),
            dma((2, rows_dev // tile)),
        ]
        + [pltpu.VMEM((rows_dev, width), f32)] * STREAMS,
        compiler_params=PARAMS,
        name="scatter",
    )(flat, vals.reshape(entries, width), user_gram, item_table, adagrad_state)


def solution(mesh):
    return jax.shard_map(
        shards,
        mesh=mesh,
        in_specs=(
            P(("dp", "rows"), None),
            P(("dp", "rows"), None),
            P(("dp", "rows"), None),
            P(("dp", "rows")),
        ),
        out_specs=(P(("dp", "rows"), None), P(("dp", "rows"), None)),
        check_vma=False,
    )
```

```python
import functools

import jax
import jax.numpy as jnp
from jax import lax
from jax.experimental import pallas as pl
from jax.experimental.pallas import tpu as pltpu
from jax.sharding import PartitionSpec as P

penalty_weight = 10.0
step_size = 0.05
LOW = 128
STREAMS = 16
HIGHEST = lax.Precision.HIGHEST
f32, bf16, i32 = jnp.float32, jnp.bfloat16, jnp.int32


def round_up(value, unit):
    return (value + unit - 1) // unit * unit


def split2(x):
    hi = x.astype(bf16)
    return hi, (x - hi.astype(f32)).astype(bf16)


def ask_kernel(
    data, shard, capacity, hist_hbm, pos_hbm, item_ref, rows_ref, codes_ref, gram_hbm,
    gram_ref, ids, acc, rows, codes, table_ref, row_send, row_recv, code_send, code_recv, own_sem,
):
    devices = data * shard
    hist_len, users_dev = hist_hbm.shape
    width = item_ref.shape[1]
    dp, rw = lax.axis_index("dp"), lax.axis_index("rows")

    def each(first, count, act):
        def step(k, _):
            act(k)
            return 0

        lax.fori_loop(first, count, step, 0)

    me = dp * shard + rw
    rows_dev = item_ref.shape[0]
    item_copy = pltpu.make_async_copy(item_ref, table_ref, own_sem.at[2])
    ids_copies = (
        pltpu.make_async_copy(hist_hbm, ids.at[pl.ds(0, hist_len)], own_sem.at[4]),
        pltpu.make_async_copy(pos_hbm, ids.at[pl.ds(hist_len, 1)], own_sem.at[5]),
    )
    for copy in ids_copies:
        copy.start()
    item_copy.start()
    barrier = pltpu.get_barrier_semaphore()

    def place(n):
        return n // shard, lax.rem(n, shard)

    def greet(k):
        pl.semaphore_signal(
            barrier, inc=1, device_id=place(lax.rem(me + k, devices)), device_id_type=pl.DeviceIdType.MESH
        )

    each(1, devices, greet)
    asks = ids.shape[0]
    if asks > hist_len + 1:
        ids[hist_len + 1 :, :] = jnp.full((asks - hist_len - 1, users_dev), devices * rows_dev, i32)
    wide = ROWS_AT_ONCE * users_dev
    upper = (
        lax.broadcasted_iota(i32, (wide, wide), 0) <= lax.broadcasted_iota(i32, (wide, wide), 1)
    ).astype(bf16)
    owners = lax.broadcasted_iota(i32, (devices, wide), 0)
    ranks_to = lax.broadcasted_iota(i32, (capacity, wide), 0)
    lane = lax.broadcasted_iota(i32, (1, users_dev), 1)
    acc[...] = jnp.zeros_like(acc)

    def route(j, carry):
        parts = [ids[pl.ds(j * ROWS_AT_ONCE + q, 1), :] for q in range(ROWS_AT_ONCE)]
        codes = [
            (lane + jnp.where(j * ROWS_AT_ONCE + q >= hist_len, users_dev, 0)).astype(f32)
            for q in range(ROWS_AT_ONCE)
        ]
        want = jnp.concatenate(parts, axis=1)
        code = jnp.concatenate(codes, axis=1)
        owner = want // rows_dev
        local = want - owner * rows_dev
        high = (local // LOW).astype(f32)
        low = (local % LOW).astype(f32)
        member = (owner == owners).astype(f32)
        prefix = jnp.dot(member.astype(bf16), upper, preferred_element_type=f32)
        rank = jnp.sum(member * (prefix + carry), axis=0, keepdims=True) - 1.0
        left = jnp.concatenate([member * high, member * low, member * code, member], axis=0).astype(bf16)
        right = (rank.astype(i32) == ranks_to).astype(f32).astype(bf16)
        acc[...] += lax.dot_general(left, right, (((1,), (1,)), ((), ())), preferred_element_type=f32)
        return carry + jnp.sum(member, axis=1, keepdims=True)

    for copy in ids_copies:
        copy.wait()
    carry = jnp.zeros((devices, 1), f32)
    for j in range(asks // ROWS_AT_ONCE):
        carry = route(j, carry)

    def write(d):
        row = acc[pl.ds(d, 1), :] * LOW + acc[pl.ds(devices + d, 1), :]
        code = acc[pl.ds(2 * devices + d, 1), :]
        present = acc[pl.ds(3 * devices + d, 1), :]
        rows[d] = row.astype(i32)
        codes[d] = jnp.where(present > 0.5, code, 2.0 * users_dev).astype(i32)

    for d in range(devices):
        write(d)
    pl.semaphore_wait(barrier, devices - 1)

    def list_copies(k, to, at):
        return tuple(
            pltpu.make_async_remote_copy(
                src_ref=src.at[to], dst_ref=dst.at[at], send_sem=send.at[k], recv_sem=recv.at[k],
                device_id=place(to), device_id_type=pl.DeviceIdType.MESH,
            )
            for src, dst, send, recv in (
                (rows, rows_ref, row_send, row_recv),
                (codes, codes_ref, code_send, code_recv),
            )
        )

    def send_list(k):
        for copy in list_copies(k, lax.rem(me + k, devices), me):
            copy.start()

    each(1, devices, send_list)
    own = (
        pltpu.make_async_copy(rows.at[me], rows_ref.at[me], own_sem.at[0]),
        pltpu.make_async_copy(codes.at[me], codes_ref.at[me], own_sem.at[1]),
    )
    for copy in own:
        copy.start()
    item_copy.wait()
    tall = 512
    gram_ref[...] = jnp.zeros_like(gram_ref)

    def square(n):
        hi, lo = split2(table_ref[pl.ds(pl.multiple_of(n * tall, 8), tall), :])
        both = lax.dot_general(
            hi, jnp.concatenate([hi, lo], axis=1), (((0,), (0,)), ((), ())), preferred_element_type=f32
        )
        gram_ref[...] += both[:, :width] + (both[:, width:] + both[:, width:].T)

    each(0, rows_dev // tall, square)
    gram_copy = pltpu.make_async_copy(gram_ref, gram_hbm, own_sem.at[3])
    gram_copy.start()

    def finish(k):
        n = lax.rem(me - k + devices, devices)
        for copy in list_copies(k, n, n):
            copy.wait_recv()
            copy.wait_send()

    each(1, devices, finish)
    for copy in own:
        copy.wait()
    gram_copy.wait()


def line_sizes(data, shard):
    cols = max(n for n in range(1, shard + 1) if shard % n == 0 and n * n <= shard)
    return data // 2, cols, shard // cols


ORDERS = ((0, 1, 2), (1, 0, 2))
LAGS = (2, 4, 6, 8)
VSLOTS = 4
GRAM_ORDERS = ((2, 0, 1), (0, 1, 2))
ROWS_AT_ONCE = 8
TWIN_LAG = 2


def exchange_kernel(
    sizes, capacity, users_dev, hist_len, coef, unroll,
    rows_hbm, codes_hbm, hot_hbm, gram_hbm, item_ref, vals_ref, ugram_hbm,
    rows_ref, codes_ref, hot_ref, gram_ref, table_ref, fetch_sem, picked, part, pair, mail, grads, cur, vbuf, upart, gsum, gmail, gfull,
    pair_send, pair_recv, mail_send, mail_recv, ag_send, ag_recv, twin_send, twin_recv, gram_send, gram_recv, vsem,
):
    nx, ny, nz = sizes
    plane = nx * ny * nz
    shard = ny * nz
    width = item_ref.shape[1]
    half = width // 2
    dp, rw = lax.axis_index("dp"), lax.axis_index("rows")
    core = lax.rem(dp, 2)
    pos = (dp // 2, lax.rem(rw, ny), rw // ny)
    origin = (0, 0, 0)
    axes = (0, 1, 2)

    def device(chip, c):
        return chip[0] * 2 + c, chip[2] * ny + chip[1]

    def block(chip, c):
        d, r = device(chip, c)
        return d * shard + r

    def ahead(r):
        return tuple(lax.rem(p + k, n) for p, k, n in zip(pos, r, sizes))

    def behind(o):
        return tuple(lax.rem(p - k + n, n) for p, k, n in zip(pos, o, sizes))

    def only(a, k):
        return tuple(k if b == a else 0 for b in axes)

    def add(r, a, k):
        return tuple(v + k if b == a else v for b, v in enumerate(r))

    def slot(r):
        return (r[0] * ny + r[1]) * nz + r[2]

    def ranked(n, digits):
        out = [0, 0, 0]
        for a in reversed(digits):
            out[a] = lax.rem(n, sizes[a])
            n = lax.div(n, sizes[a])
        return tuple(out)

    partner = device(pos, 1 - core)

    def remote(src, dst, send, recv, dev):
        return pltpu.make_async_remote_copy(
            src_ref=src, dst_ref=dst, send_sem=send, recv_sem=recv,
            device_id=dev, device_id_type=pl.DeviceIdType.MESH,
        )

    def each(first, count, act):
        def step(k, _):
            act(k)
            return 0

        lax.fori_loop(first, count, step, 0)

    me = block(pos, core)
    devices = 2 * plane
    fetches = (
        pltpu.make_async_copy(rows_hbm, rows_ref, fetch_sem.at[0]),
        pltpu.make_async_copy(codes_hbm, codes_ref, fetch_sem.at[1]),
        pltpu.make_async_copy(item_ref, table_ref, fetch_sem.at[2]),
        pltpu.make_async_copy(hot_hbm, hot_ref, fetch_sem.at[3]),
        pltpu.make_async_copy(gram_hbm, gram_ref, fetch_sem.at[4]),
    )
    for fetch in fetches:
        fetch.start()
    barrier = pltpu.get_barrier_semaphore()
    greeted = 1
    pl.semaphore_signal(barrier, inc=1, device_id=partner, device_id_type=pl.DeviceIdType.MESH)
    for a in axes:
        for k in range(1, sizes[a]):
            greeted += 1
            pl.semaphore_signal(
                barrier, inc=1, device_id=device(ahead(only(a, k)), core), device_id_type=pl.DeviceIdType.MESH
            )
    pl.semaphore_wait(barrier, greeted)
    for fetch in fetches:
        fetch.wait()

    def pair_copy(at):
        return remote(part.at[0, at], pair.at[at], pair_send.at[at], pair_recv.at[at], partner)

    def letter(h, at, dev):
        return remote(part.at[1, at, h], mail.at[h, at], mail_send.at[h, at], mail_recv.at[h, at], dev)

    def parcel(h, at, b, dev):
        return remote(grads.at[b, h], grads.at[b, h], ag_send.at[h, at], ag_recv.at[h, at], dev)

    def twin(at, b):
        return remote(grads.at[b], grads.at[b], twin_send.at[at], twin_recv.at[at], partner)

    first = [1]
    for a in axes:
        first.append(first[-1] + sizes[a] - 1)
    last = first[3]
    mine = pl.ds(pl.multiple_of(core * half, 8), half)
    theirs = pl.ds(pl.multiple_of((1 - core) * half, 8), half)

    def gram_pair(t, src):
        return remote(src.at[theirs], gmail.at[t, 0], gram_send.at[t, 0], gram_recv.at[t, 0], partner)

    def gram_line(t, s, k):
        a = GRAM_ORDERS[t][s]
        at = first[a] + k - 1
        return remote(
            gsum.at[t, s], gmail.at[t, at], gram_send.at[t, at], gram_recv.at[t, at], device(ahead(only(a, k)), core)
        )

    def gram_final(t):
        return remote(gsum.at[t, 3], gfull.at[t, mine], gram_send.at[t, last], gram_recv.at[t, last], partner)

    def gram_open(t, src):
        gram_pair(t, src).start()

    def gram_send_line(t, s):
        for k in range(1, sizes[GRAM_ORDERS[t][s]]):
            gram_line(t, s, k).start()

    def gram_step(t, src, stage):
        if stage == 0:
            gram_pair(t, src).wait_recv()
            gsum[t, 0] = src[mine, :] + gmail[t, 0]
        elif stage <= 3:
            s = stage - 1
            a = GRAM_ORDERS[t][s]
            total = gsum[t, s]
            for k in range(1, sizes[a]):
                gram_line(t, s, k).wait_recv()
                total = total + gmail[t, first[a] + k - 1]
            gsum[t, s + 1] = total
        else:
            gram_final(t).wait_recv()
        if stage < 3:
            gram_send_line(t, stage)
        elif stage == 3:
            gram_final(t).start()
            gfull[t, mine] = gsum[t, 3]

    def gram_drain(t, src):
        gram_pair(t, src).wait_send()
        for s in range(3):
            for k in range(1, sizes[GRAM_ORDERS[t][s]]):
                gram_line(t, s, k).wait_send()
        gram_final(t).wait_send()

    codes_to = lax.broadcasted_iota(i32, (2 * users_dev, capacity), 0)

    def gather(b, j, at):
        base = b * capacity

        def some(s, _):
            start = base + s * unroll
            for k in range(unroll):
                r = rows_ref.at[pl.ds(k, rows_ref.shape[0] - unroll + 1)][start]
                picked[pl.ds(s * unroll + k, 1), :] = table_ref[pl.ds(r, 1), :]
            return 0

        lax.fori_loop(0, capacity // unroll, some, 0)
        x = picked[...]
        hi, lo = split2(x)
        hot = (hot_ref[b] == codes_to).astype(f32).astype(bf16)
        both = jnp.dot(hot, jnp.concatenate([hi, lo], axis=1), preferred_element_type=f32)
        out = both[:, :width] + both[:, width:]
        part[j, at, 0] = out[:users_dev]
        part[j, at, 1] = out[users_dev:]

    def arrive(h, r, a):
        at = slot(r)
        for k in range(1, sizes[a]):
            m = slot(add(r, a, k))
            letter(h, m, partner).wait_recv()
            part[1, at, h] = part[1, at, h] + mail[h, m]

    def leave(h, r, a):
        @pl.when(r[a] != 0)
        def _():
            chip = tuple(lax.rem(p + r[a], n) if b == a else p for b, (p, n) in enumerate(zip(pos, sizes)))
            letter(h, slot(r), device(chip, core)).start()

    gram_open(0, gram_ref)

    def reduce_step(i, _):
        for stage in range(4):
            j = i - LAGS[stage]

            @pl.when(jnp.logical_and(j >= 0, j < plane))
            def _():
                r = ranked(plane - 1 - j, (2, 0, 1))
                at = slot(r)
                if stage == 0:
                    pair_copy(at).wait_recv()
                    for h in range(2):
                        part[1, at, h] = part[1, at, h] + pair[at, h]
                        leave(h, r, ORDERS[h][0])
                else:
                    for h in range(2):
                        order = ORDERS[h]
                        clear = r[order[0]] == 0
                        for a in order[1:stage]:
                            clear = jnp.logical_and(clear, r[a] == 0)

                        @pl.when(clear)
                        def _():
                            arrive(h, r, order[stage - 1])
                            if stage < 3:
                                leave(h, r, order[stage])

        for stage in range(5):
            @pl.when(i == 3 * stage + 1)
            def _():
                gram_step(0, gram_ref, stage)

        @pl.when(i < plane)
        def _():
            r = ranked(plane - 1 - i, (2, 0, 1))
            at = slot(r)
            chip = ahead(r)

            def one(j, _):
                c = (1 - core) * (1 - j) + core * j
                gather(block(chip, c), j, at)

                @pl.when(j == 0)
                def _():
                    pair_copy(at).start()

                return 0

            lax.fori_loop(0, 2, one, 0)

        return 0

    lax.fori_loop(0, plane + LAGS[3], reduce_step, 0)

    uv = part[1, 0, 0] / hist_len
    pv = part[1, 0, 1]
    gap = jnp.sum(uv * pv, axis=1, keepdims=True) - 1.0
    ug = 2.0 * gap * pv + 2.0 * coef * jnp.dot(uv, gfull[0], precision=HIGHEST, preferred_element_type=f32)
    grads[me, 0] = ug / hist_len
    grads[me, 1] = 2.0 * gap * uv

    def forward(h, o, b, a):
        for k in range(1, sizes[a]):
            chip = tuple(lax.rem(p + k, n) if c == a else p for c, (p, n) in enumerate(zip(pos, sizes)))
            parcel(h, slot(add(o, a, k)), b, device(chip, core)).start()

    ways = tuple(order[::-1] for order in ORDERS)
    line = ways[0][0]
    for k in range(1, sizes[line]):
        for h in range(2):
            parcel(h, slot(only(line, k)), me, device(ahead(only(line, k)), core)).start()
    for a in (1, 2):
        for h in range(2):
            forward(h, origin, me, ways[h][a])
    twin(0, me).start()
    upart[...] = lax.dot_general(
        uv, uv, (((0,), (0,)), ((), ())), precision=HIGHEST, preferred_element_type=f32
    )
    gram_open(1, upart)
    cur[pl.ds(2 * users_dev, 8), :] = jnp.zeros((8, width), f32)

    def vals_copy(v, b):
        return pltpu.make_async_copy(vbuf.at[v], vals_ref.at[b], vsem.at[v])

    def vals(n, kind, b):
        v = 2 * kind + lax.rem(n, 2)

        @pl.when(n >= 2)
        def _():
            vals_copy(v, b).wait()

        cur[pl.ds(0, users_dev), :] = grads[b, 0]
        cur[pl.ds(users_dev, users_dev), :] = grads[b, 1]
        base = b * capacity

        def some(s, _):
            start = base + s * unroll
            for k in range(unroll):
                c = codes_ref.at[pl.ds(k, codes_ref.shape[0] - unroll + 1)][start]
                vbuf[v, pl.ds(s * unroll + k, 1), :] = cur[pl.ds(c, 1), :]
            return 0

        lax.fori_loop(0, capacity // unroll, some, 0)
        vals_copy(v, b).start()

    digits = ((2, 0, 1), (2, 1, 0))
    delays = (-nx * ny, 1, 3)
    vals_delay = delays[2] + 1

    def spread(n, _):
        for h in range(2):
            a1, a2, a3 = ways[h]
            for level in (1, 2, 3):
                q = n - delays[level - 1]
                o = ranked(q, digits[h])
                if level == 1:
                    here = jnp.logical_and(o[a1] != 0, jnp.logical_and(o[a2] == 0, o[a3] == 0))
                elif level == 2:
                    here = jnp.logical_and(o[a2] != 0, o[a3] == 0)
                else:
                    here = o[a3] != 0

                @pl.when(jnp.logical_and(jnp.logical_and(q >= 0, q < plane), here))
                def _():
                    b = block(behind(o), core)
                    parcel(h, slot(o), b, partner).wait_recv()
                    for a in ways[h][level:]:
                        forward(h, o, b, a)

        def one(kind, _):
            j = n - vals_delay - TWIN_LAG * kind

            @pl.when(jnp.logical_and(j >= 0, j < plane))
            def _():
                o = ranked(j, digits[0])
                at = slot(o)
                b = block(behind(o), core + kind * (1 - 2 * core))

                @pl.when(jnp.logical_and(kind == 0, j > 0))
                def _():
                    twin(at, b).start()

                @pl.when(kind == 1)
                def _():
                    twin(at, b).wait_recv()

                vals(j, kind, b)

            return 0

        lax.fori_loop(0, 2, one, 0)

        for stage in range(5):
            @pl.when(n == 4 * stage + 3)
            def _():
                gram_step(1, upart, stage)

        return 0

    lax.fori_loop(0, plane + vals_delay + TWIN_LAG, spread, 0)
    ugram_copy = pltpu.make_async_copy(gfull.at[1], ugram_hbm, fetch_sem.at[5])
    ugram_copy.start()

    def drain(n):
        pair_copy(n).wait_send()
        twin(n, me).wait_send()

    each(0, plane, drain)

    def drain_mail(n):
        for h in range(2):
            letter(h, n, partner).wait_send()
            parcel(h, n, me, partner).wait_send()

    each(1, plane, drain_mail)
    gram_drain(0, gram_ref)
    gram_drain(1, upart)
    each(0, VSLOTS, lambda v: vals_copy(v, me).wait())
    ugram_copy.wait()


def scatter_kernel(
    coef, chunk, unroll, tile,
    rows_hbm, vals_ref, ugram_hbm, table_ref, state_ref, new_table_ref, new_state_ref,
    rows_ref, ugram_ref, vbuf, table, state, vsem, in_sem, out_sem, *accs,
):
    entries = rows_ref.shape[0]
    chunks = entries // chunk
    part = chunk // len(accs)
    rows_dev, width = table.shape
    tiles = rows_dev // tile

    def vals_copy(n):
        s = lax.rem(n, 2)
        return pltpu.make_async_copy(
            vals_ref.at[pl.ds(pl.multiple_of(n * chunk, 8), chunk)], vbuf.at[s], vsem.at[s]
        )

    table_copy = pltpu.make_async_copy(table_ref, table, in_sem.at[0])
    state_copy = pltpu.make_async_copy(state_ref, state, in_sem.at[1])
    rows_copy = pltpu.make_async_copy(rows_hbm, rows_ref, in_sem.at[2])
    ugram_copy = pltpu.make_async_copy(ugram_hbm, ugram_ref, in_sem.at[3])
    rows_copy.start()
    vals_copy(0).start()
    vals_copy(1).start()
    table_copy.start()
    state_copy.start()
    ugram_copy.start()
    for acc in accs:
        acc[...] = jnp.zeros_like(acc)

    def one(n, _):
        v = lax.rem(n, 2)
        vals_copy(n).wait()

        def scatter(s, _):
            start = n * chunk + s * unroll
            for q in range(unroll):
                rows = [
                    rows_ref.at[pl.ds(k * part + q, entries - chunk + part - unroll + 1)][start] for k in range(len(accs))
                ]
                news = [
                    acc[pl.ds(r, 1), :] + vbuf[v, pl.ds(s * unroll + (k * part + q), 1), :]
                    for k, (acc, r) in enumerate(zip(accs, rows))
                ]
                for acc, r, new in zip(accs, rows, news):
                    acc[pl.ds(r, 1), :] = new
            return 0

        lax.fori_loop(0, part // unroll, scatter, 0)

        @pl.when(n + 2 < chunks)
        def _():
            vals_copy(n + 2).start()

        return 0

    rows_copy.wait()
    lax.fori_loop(0, chunks, one, 0)
    table_copy.wait()
    state_copy.wait()
    ugram_copy.wait()
    u0, u1 = split2(ugram_ref[...])
    u00 = jnp.concatenate([u0, u0], axis=0)

    def out_copy(t, which):
        at = pl.ds(pl.multiple_of(t * tile, 8), tile)
        src, dst = ((table, new_table_ref), (state, new_state_ref))[which]
        return pltpu.make_async_copy(src.at[at], dst.at[at], out_sem.at[which, t])

    def finish(t, _):
        at = pl.ds(pl.multiple_of(t * tile, 8), tile)
        item = table[at, :]
        t0, t1 = split2(item)
        g = jnp.dot(jnp.concatenate([t0, t1], axis=1), u00, preferred_element_type=f32)
        g = 2.0 * coef * (g + jnp.dot(t0, u1, preferred_element_type=f32))
        add = accs[0][at, :]
        for acc in accs[1:]:
            add = add + acc[at, :]
        g = g + add
        new = state[at, :] + g * g
        state[at, :] = new
        table[at, :] = item - step_size * g * lax.rsqrt(new)
        out_copy(t, 0).start()
        out_copy(t, 1).start()
        return 0

    lax.fori_loop(0, tiles, finish, 0)

    def drain(t, _):
        out_copy(t, 0).wait()
        out_copy(t, 1).wait()
        return 0

    lax.fori_loop(0, tiles, drain, 0)


VM = pl.BlockSpec(memory_space=pltpu.VMEM)
HB = pl.BlockSpec(memory_space=pl.ANY)
SM = pl.BlockSpec(memory_space=pltpu.SMEM)
PARAMS = pltpu.CompilerParams(vmem_limit_bytes=60 * 1024 * 1024)


def shards(item_table, adagrad_state, history_ids, positive_ids):
    rows_dev, width = item_table.shape
    users_dev, hist_len = history_ids.shape
    devices = lax.axis_size("dp") * lax.axis_size("rows")
    groups = 2 * users_dev
    count = users_dev * (hist_len + 1)
    capacity = max(8, (count * 5 // (2 * devices) + 7) // 8 * 8)
    entries = devices * capacity
    asks = round_up(hist_len + 1, ROWS_AT_ONCE)
    data, shard = lax.axis_size("dp"), lax.axis_size("rows")
    sizes = line_sizes(data, shard)
    plane = devices // 2
    lines = sum(sizes) - 1
    unroll = max(n for n in (8, 16, 32, 64, 128) if capacity % n == 0)
    coef = penalty_weight / (rows_dev * devices)
    dma = pltpu.SemaphoreType.DMA
    list_shape = jax.ShapeDtypeStruct((devices, 1, capacity), i32)
    rows, codes, item_gram = pl.pallas_call(
        functools.partial(ask_kernel, data, shard, capacity),
        out_shape=(list_shape, list_shape, jax.ShapeDtypeStruct((width, width), f32)),
        in_specs=[HB, HB, HB],
        out_specs=(HB, HB, HB),
        scratch_shapes=[
            pltpu.VMEM((width, width), f32),
            pltpu.VMEM((asks, users_dev), i32),
            pltpu.VMEM((4 * devices, capacity), f32),
            pltpu.VMEM((devices, 1, capacity), i32),
            pltpu.VMEM((devices, 1, capacity), i32),
            pltpu.VMEM((rows_dev, width), f32),
        ]
        + [dma((devices,))] * 4
        + [dma((6,))],
        compiler_params=pltpu.CompilerParams(
            vmem_limit_bytes=60 * 1024 * 1024, collective_id=1, has_side_effects=True
        ),
        name="ask",
    )(history_ids.T, positive_ids[None], item_table)
    flat = rows.reshape(-1)
    vals, user_gram = pl.pallas_call(
        functools.partial(exchange_kernel, sizes, capacity, users_dev, hist_len, coef, unroll),
        out_shape=(
            jax.ShapeDtypeStruct((devices, capacity, width), f32),
            jax.ShapeDtypeStruct((width, width), f32),
        ),
        in_specs=[HB, HB, HB, HB, HB],
        out_specs=(HB, HB),
        scratch_shapes=[
            pltpu.SMEM((entries,), i32),
            pltpu.SMEM((entries,), i32),
            pltpu.VMEM((devices, 1, capacity), i32),
            pltpu.VMEM((width, width), f32),
            pltpu.VMEM((rows_dev, width), f32),
            dma((6,)),
            pltpu.VMEM((capacity, width), f32),
            pltpu.VMEM((2, plane, 2, users_dev, width), f32),
            pltpu.VMEM((plane, 2, users_dev, width), f32),
            pltpu.VMEM((2, plane, users_dev, width), f32),
            pltpu.VMEM((devices, 2, users_dev, width), f32),
            pltpu.VMEM((groups + 8, width), f32),
            pltpu.VMEM((VSLOTS, capacity, width), f32),
            pltpu.VMEM((width, width), f32),
            pltpu.VMEM((2, 4, width // 2, width), f32),
            pltpu.VMEM((2, lines, width // 2, width), f32),
            pltpu.VMEM((2, width, width), f32),
            dma((plane,)),
            dma((plane,)),
            dma((2, plane)),
            dma((2, plane)),
            dma((2, plane)),
            dma((2, plane)),
            dma((plane,)),
            dma((plane,)),
            dma((2, lines)),
            dma((2, lines)),
            dma((VSLOTS,)),
        ],
        compiler_params=pltpu.CompilerParams(
            vmem_limit_bytes=60 * 1024 * 1024, collective_id=0, has_side_effects=True
        ),
        name="exchange",
    )(flat, codes.reshape(-1), codes, item_gram, item_table)
    chunk, tile = min(4096, entries), 512
    return pl.pallas_call(
        functools.partial(scatter_kernel, coef, chunk, 8, tile),
        out_shape=(
            jax.ShapeDtypeStruct(item_table.shape, f32),
            jax.ShapeDtypeStruct(item_table.shape, f32),
        ),
        in_specs=[HB, HB, HB, HB, HB],
        out_specs=(HB, HB),
        scratch_shapes=[
            pltpu.SMEM((entries,), i32),
            pltpu.VMEM((width, width), f32),
            pltpu.VMEM((2, chunk, width), f32),
            pltpu.VMEM((rows_dev, width), f32),
            pltpu.VMEM((rows_dev, width), f32),
            dma((2,)),
            dma((4,)),
            dma((2, rows_dev // tile)),
        ]
        + [pltpu.VMEM((rows_dev, width), f32)] * STREAMS,
        compiler_params=PARAMS,
        name="scatter",
    )(flat, vals.reshape(entries, width), user_gram, item_table, adagrad_state)


def solution(mesh):
    return jax.shard_map(
        shards,
        mesh=mesh,
        in_specs=(
            P(("dp", "rows"), None),
            P(("dp", "rows"), None),
            P(("dp", "rows"), None),
            P(("dp", "rows")),
        ),
        out_specs=(P(("dp", "rows"), None), P(("dp", "rows"), None)),
        check_vma=False,
    )
```

```python
import functools

import jax
import jax.numpy as jnp
from jax import lax
from jax.experimental import pallas as pl
from jax.experimental.pallas import tpu as pltpu
from jax.sharding import PartitionSpec as P

penalty_weight = 10.0
step_size = 0.05
LOW = 128
STREAMS = 16
HIGHEST = lax.Precision.HIGHEST
f32, bf16, i32 = jnp.float32, jnp.bfloat16, jnp.int32


def round_up(value, unit):
    return (value + unit - 1) // unit * unit


def split2(x):
    hi = x.astype(bf16)
    return hi, (x - hi.astype(f32)).astype(bf16)


def ask_kernel(
    data, shard, capacity, hist_hbm, pos_hbm, item_ref, rows_ref, codes_ref, gram_hbm,
    gram_ref, ids, acc, rows, codes, table_ref, row_send, row_recv, code_send, code_recv, own_sem,
):
    devices = data * shard
    hist_len, users_dev = hist_hbm.shape
    width = item_ref.shape[1]
    dp, rw = lax.axis_index("dp"), lax.axis_index("rows")

    def each(first, count, act):
        def step(k, _):
            act(k)
            return 0

        lax.fori_loop(first, count, step, 0)

    me = dp * shard + rw
    rows_dev = item_ref.shape[0]
    item_copy = pltpu.make_async_copy(item_ref, table_ref, own_sem.at[2])
    ids_copies = (
        pltpu.make_async_copy(hist_hbm, ids.at[pl.ds(0, hist_len)], own_sem.at[4]),
        pltpu.make_async_copy(pos_hbm, ids.at[pl.ds(hist_len, 1)], own_sem.at[5]),
    )
    for copy in ids_copies:
        copy.start()
    item_copy.start()
    barrier = pltpu.get_barrier_semaphore()

    def place(n):
        return n // shard, lax.rem(n, shard)

    def greet(k):
        pl.semaphore_signal(
            barrier, inc=1, device_id=place(lax.rem(me + k, devices)), device_id_type=pl.DeviceIdType.MESH
        )

    each(1, devices, greet)
    asks = ids.shape[0]
    if asks > hist_len + 1:
        ids[hist_len + 1 :, :] = jnp.full((asks - hist_len - 1, users_dev), devices * rows_dev, i32)
    wide = ROWS_AT_ONCE * users_dev
    upper = (
        lax.broadcasted_iota(i32, (wide, wide), 0) <= lax.broadcasted_iota(i32, (wide, wide), 1)
    ).astype(bf16)
    owners = lax.broadcasted_iota(i32, (devices, wide), 0)
    ranks_to = lax.broadcasted_iota(i32, (capacity, wide), 0)
    lane = lax.broadcasted_iota(i32, (1, users_dev), 1)
    acc[...] = jnp.zeros_like(acc)

    def route(j, carry):
        parts = [ids[pl.ds(j * ROWS_AT_ONCE + q, 1), :] for q in range(ROWS_AT_ONCE)]
        codes = [
            (lane + jnp.where(j * ROWS_AT_ONCE + q >= hist_len, users_dev, 0)).astype(f32)
            for q in range(ROWS_AT_ONCE)
        ]
        want = jnp.concatenate(parts, axis=1)
        code = jnp.concatenate(codes, axis=1)
        owner = want // rows_dev
        local = want - owner * rows_dev
        high = (local // LOW).astype(f32)
        low = (local % LOW).astype(f32)
        member = (owner == owners).astype(f32)
        prefix = jnp.dot(member.astype(bf16), upper, preferred_element_type=f32)
        rank = jnp.sum(member * (prefix + carry), axis=0, keepdims=True) - 1.0
        left = jnp.concatenate([member * high, member * low, member * code, member], axis=0).astype(bf16)
        right = (rank.astype(i32) == ranks_to).astype(f32).astype(bf16)
        acc[...] += lax.dot_general(left, right, (((1,), (1,)), ((), ())), preferred_element_type=f32)
        return carry + jnp.sum(member, axis=1, keepdims=True)

    for copy in ids_copies:
        copy.wait()
    carry = jnp.zeros((devices, 1), f32)
    for j in range(asks // ROWS_AT_ONCE):
        carry = route(j, carry)

    def write(d):
        row = acc[pl.ds(d, 1), :] * LOW + acc[pl.ds(devices + d, 1), :]
        code = acc[pl.ds(2 * devices + d, 1), :]
        present = acc[pl.ds(3 * devices + d, 1), :]
        rows[d] = row.astype(i32)
        codes[d] = jnp.where(present > 0.5, code, 2.0 * users_dev).astype(i32)

    for d in range(devices):
        write(d)
    pl.semaphore_wait(barrier, devices - 1)

    def list_copies(k, to, at):
        return tuple(
            pltpu.make_async_remote_copy(
                src_ref=src.at[to], dst_ref=dst.at[at], send_sem=send.at[k], recv_sem=recv.at[k],
                device_id=place(to), device_id_type=pl.DeviceIdType.MESH,
            )
            for src, dst, send, recv in (
                (rows, rows_ref, row_send, row_recv),
                (codes, codes_ref, code_send, code_recv),
            )
        )

    def send_list(k):
        for copy in list_copies(k, lax.rem(me + k, devices), me):
            copy.start()

    each(1, devices, send_list)
    own = (
        pltpu.make_async_copy(rows.at[me], rows_ref.at[me], own_sem.at[0]),
        pltpu.make_async_copy(codes.at[me], codes_ref.at[me], own_sem.at[1]),
    )
    for copy in own:
        copy.start()
    item_copy.wait()
    tall = 512
    gram_ref[...] = jnp.zeros_like(gram_ref)

    def square(n):
        hi, lo = split2(table_ref[pl.ds(pl.multiple_of(n * tall, 8), tall), :])
        both = lax.dot_general(
            hi, jnp.concatenate([hi, lo], axis=1), (((0,), (0,)), ((), ())), preferred_element_type=f32
        )
        gram_ref[...] += both[:, :width] + (both[:, width:] + both[:, width:].T)

    each(0, rows_dev // tall, square)
    gram_copy = pltpu.make_async_copy(gram_ref, gram_hbm, own_sem.at[3])
    gram_copy.start()

    def finish(k):
        n = lax.rem(me - k + devices, devices)
        for copy in list_copies(k, n, n):
            copy.wait_recv()
            copy.wait_send()

    each(1, devices, finish)
    for copy in own:
        copy.wait()
    gram_copy.wait()


def line_sizes(data, shard):
    cols = max(n for n in range(1, shard + 1) if shard % n == 0 and n * n <= shard)
    return data // 2, cols, shard // cols


ORDERS = ((0, 1, 2), (1, 0, 2))
LAGS = (2, 4, 6, 8)
VSLOTS = 4
GRAM_ORDERS = ((2, 0, 1), (0, 1, 2))
ROWS_AT_ONCE = 8
TWIN_LAG = 2


def exchange_kernel(
    sizes, capacity, users_dev, hist_len, coef, unroll,
    rows_hbm, codes_hbm, hot_hbm, gram_hbm, item_ref, vals_ref, ugram_hbm,
    rows_ref, codes_ref, hot_ref, gram_ref, table_ref, fetch_sem, picked, part, pair, mail, grads, cur, vbuf, upart, gsum, gmail, gfull,
    pair_send, pair_recv, mail_send, mail_recv, ag_send, ag_recv, twin_send, twin_recv, gram_send, gram_recv, vsem,
):
    nx, ny, nz = sizes
    plane = nx * ny * nz
    shard = ny * nz
    width = item_ref.shape[1]
    half = width // 2
    dp, rw = lax.axis_index("dp"), lax.axis_index("rows")
    core = lax.rem(dp, 2)
    pos = (dp // 2, lax.rem(rw, ny), rw // ny)
    origin = (0, 0, 0)
    axes = (0, 1, 2)

    def device(chip, c):
        return chip[0] * 2 + c, chip[2] * ny + chip[1]

    def block(chip, c):
        d, r = device(chip, c)
        return d * shard + r

    def ahead(r):
        return tuple(lax.rem(p + k, n) for p, k, n in zip(pos, r, sizes))

    def behind(o):
        return tuple(lax.rem(p - k + n, n) for p, k, n in zip(pos, o, sizes))

    def only(a, k):
        return tuple(k if b == a else 0 for b in axes)

    def add(r, a, k):
        return tuple(v + k if b == a else v for b, v in enumerate(r))

    def slot(r):
        return (r[0] * ny + r[1]) * nz + r[2]

    def ranked(n, digits):
        out = [0, 0, 0]
        for a in reversed(digits):
            out[a] = lax.rem(n, sizes[a])
            n = lax.div(n, sizes[a])
        return tuple(out)

    partner = device(pos, 1 - core)

    def remote(src, dst, send, recv, dev):
        return pltpu.make_async_remote_copy(
            src_ref=src, dst_ref=dst, send_sem=send, recv_sem=recv,
            device_id=dev, device_id_type=pl.DeviceIdType.MESH,
        )

    def each(first, count, act):
        def step(k, _):
            act(k)
            return 0

        lax.fori_loop(first, count, step, 0)

    me = block(pos, core)
    devices = 2 * plane
    fetches = (
        pltpu.make_async_copy(rows_hbm, rows_ref, fetch_sem.at[0]),
        pltpu.make_async_copy(codes_hbm, codes_ref, fetch_sem.at[1]),
        pltpu.make_async_copy(item_ref, table_ref, fetch_sem.at[2]),
        pltpu.make_async_copy(hot_hbm, hot_ref, fetch_sem.at[3]),
        pltpu.make_async_copy(gram_hbm, gram_ref, fetch_sem.at[4]),
    )
    for fetch in fetches:
        fetch.start()
    barrier = pltpu.get_barrier_semaphore()
    greeted = 1
    pl.semaphore_signal(barrier, inc=1, device_id=partner, device_id_type=pl.DeviceIdType.MESH)
    for a in axes:
        for k in range(1, sizes[a]):
            greeted += 1
            pl.semaphore_signal(
                barrier, inc=1, device_id=device(ahead(only(a, k)), core), device_id_type=pl.DeviceIdType.MESH
            )
    pl.semaphore_wait(barrier, greeted)
    for fetch in fetches:
        fetch.wait()

    def pair_copy(at):
        return remote(part.at[0, at], pair.at[at], pair_send.at[at], pair_recv.at[at], partner)

    def letter(h, at, dev):
        return remote(part.at[1, at, h], mail.at[h, at], mail_send.at[h, at], mail_recv.at[h, at], dev)

    def parcel(h, at, b, dev):
        return remote(grads.at[b, h], grads.at[b, h], ag_send.at[h, at], ag_recv.at[h, at], dev)

    def twin(at, b):
        return remote(grads.at[b], grads.at[b], twin_send.at[at], twin_recv.at[at], partner)

    first = [1]
    for a in axes:
        first.append(first[-1] + sizes[a] - 1)
    last = first[3]
    mine = pl.ds(pl.multiple_of(core * half, 8), half)
    theirs = pl.ds(pl.multiple_of((1 - core) * half, 8), half)

    def gram_pair(t, src):
        return remote(src.at[theirs], gmail.at[t, 0], gram_send.at[t, 0], gram_recv.at[t, 0], partner)

    def gram_line(t, s, k):
        a = GRAM_ORDERS[t][s]
        at = first[a] + k - 1
        return remote(
            gsum.at[t, s], gmail.at[t, at], gram_send.at[t, at], gram_recv.at[t, at], device(ahead(only(a, k)), core)
        )

    def gram_final(t):
        return remote(gsum.at[t, 3], gfull.at[t, mine], gram_send.at[t, last], gram_recv.at[t, last], partner)

    def gram_open(t, src):
        gram_pair(t, src).start()

    def gram_send_line(t, s):
        for k in range(1, sizes[GRAM_ORDERS[t][s]]):
            gram_line(t, s, k).start()

    def gram_step(t, src, stage):
        if stage == 0:
            gram_pair(t, src).wait_recv()
            gsum[t, 0] = src[mine, :] + gmail[t, 0]
        elif stage <= 3:
            s = stage - 1
            a = GRAM_ORDERS[t][s]
            total = gsum[t, s]
            for k in range(1, sizes[a]):
                gram_line(t, s, k).wait_recv()
                total = total + gmail[t, first[a] + k - 1]
            gsum[t, s + 1] = total
        else:
            gram_final(t).wait_recv()
        if stage < 3:
            gram_send_line(t, stage)
        elif stage == 3:
            gram_final(t).start()
            gfull[t, mine] = gsum[t, 3]

    def gram_drain(t, src):
        gram_pair(t, src).wait_send()
        for s in range(3):
            for k in range(1, sizes[GRAM_ORDERS[t][s]]):
                gram_line(t, s, k).wait_send()
        gram_final(t).wait_send()

    codes_to = lax.broadcasted_iota(i32, (2 * users_dev, capacity), 0)

    def gather(b, j, at):
        base = b * capacity

        def some(s, _):
            start = base + s * unroll
            for k in range(unroll):
                r = rows_ref.at[pl.ds(k, rows_ref.shape[0] - unroll + 1)][start]
                picked[pl.ds(s * unroll + k, 1), :] = table_ref[pl.ds(r, 1), :]
            return 0

        lax.fori_loop(0, capacity // unroll, some, 0)
        x = picked[...]
        hi, lo = split2(x)
        hot = (hot_ref[b] == codes_to).astype(f32).astype(bf16)
        both = jnp.dot(hot, jnp.concatenate([hi, lo], axis=1), preferred_element_type=f32)
        out = both[:, :width] + both[:, width:]
        part[j, at, 0] = out[:users_dev]
        part[j, at, 1] = out[users_dev:]

    def arrive(h, r, a):
        at = slot(r)
        for k in range(1, sizes[a]):
            m = slot(add(r, a, k))
            letter(h, m, partner).wait_recv()
            part[1, at, h] = part[1, at, h] + mail[h, m]

    def leave(h, r, a):
        @pl.when(r[a] != 0)
        def _():
            chip = tuple(lax.rem(p + r[a], n) if b == a else p for b, (p, n) in enumerate(zip(pos, sizes)))
            letter(h, slot(r), device(chip, core)).start()

    gram_open(0, gram_ref)

    def reduce_step(i, _):
        for stage in range(4):
            j = i - LAGS[stage]

            @pl.when(jnp.logical_and(j >= 0, j < plane))
            def _():
                r = ranked(plane - 1 - j, (2, 0, 1))
                at = slot(r)
                if stage == 0:
                    pair_copy(at).wait_recv()
                    for h in range(2):
                        part[1, at, h] = part[1, at, h] + pair[at, h]
                        leave(h, r, ORDERS[h][0])
                else:
                    for h in range(2):
                        order = ORDERS[h]
                        clear = r[order[0]] == 0
                        for a in order[1:stage]:
                            clear = jnp.logical_and(clear, r[a] == 0)

                        @pl.when(clear)
                        def _():
                            arrive(h, r, order[stage - 1])
                            if stage < 3:
                                leave(h, r, order[stage])

        for stage in range(5):
            @pl.when(i == 3 * stage + 1)
            def _():
                gram_step(0, gram_ref, stage)

        @pl.when(i < plane)
        def _():
            r = ranked(plane - 1 - i, (2, 0, 1))
            at = slot(r)
            chip = ahead(r)

            def one(j, _):
                c = (1 - core) * (1 - j) + core * j
                gather(block(chip, c), j, at)

                @pl.when(j == 0)
                def _():
                    pair_copy(at).start()

                return 0

            lax.fori_loop(0, 2, one, 0)

        return 0

    lax.fori_loop(0, plane + LAGS[3], reduce_step, 0)

    uv = part[1, 0, 0] / hist_len
    pv = part[1, 0, 1]
    gap = jnp.sum(uv * pv, axis=1, keepdims=True) - 1.0
    ug = 2.0 * gap * pv + 2.0 * coef * jnp.dot(uv, gfull[0], precision=HIGHEST, preferred_element_type=f32)
    grads[me, 0] = ug / hist_len
    grads[me, 1] = 2.0 * gap * uv

    def forward(h, o, b, a):
        for k in range(1, sizes[a]):
            chip = tuple(lax.rem(p + k, n) if c == a else p for c, (p, n) in enumerate(zip(pos, sizes)))
            parcel(h, slot(add(o, a, k)), b, device(chip, core)).start()

    ways = tuple(order[::-1] for order in ORDERS)
    line = ways[0][0]
    for k in range(1, sizes[line]):
        for h in range(2):
            parcel(h, slot(only(line, k)), me, device(ahead(only(line, k)), core)).start()
    for a in (1, 2):
        for h in range(2):
            forward(h, origin, me, ways[h][a])
    twin(0, me).start()
    upart[...] = lax.dot_general(
        uv, uv, (((0,), (0,)), ((), ())), precision=HIGHEST, preferred_element_type=f32
    )
    gram_open(1, upart)
    cur[pl.ds(2 * users_dev, 8), :] = jnp.zeros((8, width), f32)

    def vals_copy(v, b):
        return pltpu.make_async_copy(vbuf.at[v], vals_ref.at[b], vsem.at[v])

    def vals(n, kind, b):
        v = 2 * kind + lax.rem(n, 2)

        @pl.when(n >= 2)
        def _():
            vals_copy(v, b).wait()

        cur[pl.ds(0, users_dev), :] = grads[b, 0]
        cur[pl.ds(users_dev, users_dev), :] = grads[b, 1]
        base = b * capacity

        def some(s, _):
            start = base + s * unroll
            for k in range(unroll):
                c = codes_ref.at[pl.ds(k, codes_ref.shape[0] - unroll + 1)][start]
                vbuf[v, pl.ds(s * unroll + k, 1), :] = cur[pl.ds(c, 1), :]
            return 0

        lax.fori_loop(0, capacity // unroll, some, 0)
        vals_copy(v, b).start()

    digits = ((2, 0, 1), (2, 1, 0))
    delays = (-nx * ny, 1, 3)
    vals_delay = delays[2] + 1

    def spread(n, _):
        for h in range(2):
            a1, a2, a3 = ways[h]
            for level in (1, 2, 3):
                q = n - delays[level - 1]
                o = ranked(q, digits[h])
                if level == 1:
                    here = jnp.logical_and(o[a1] != 0, jnp.logical_and(o[a2] == 0, o[a3] == 0))
                elif level == 2:
                    here = jnp.logical_and(o[a2] != 0, o[a3] == 0)
                else:
                    here = o[a3] != 0

                @pl.when(jnp.logical_and(jnp.logical_and(q >= 0, q < plane), here))
                def _():
                    b = block(behind(o), core)
                    parcel(h, slot(o), b, partner).wait_recv()
                    for a in ways[h][level:]:
                        forward(h, o, b, a)

        def one(kind, _):
            j = n - vals_delay - TWIN_LAG * kind

            @pl.when(jnp.logical_and(j >= 0, j < plane))
            def _():
                o = ranked(j, digits[0])
                at = slot(o)
                b = block(behind(o), core + kind * (1 - 2 * core))

                @pl.when(jnp.logical_and(kind == 0, j > 0))
                def _():
                    twin(at, b).start()

                @pl.when(kind == 1)
                def _():
                    twin(at, b).wait_recv()

                vals(j, kind, b)

            return 0

        lax.fori_loop(0, 2, one, 0)

        for stage in range(5):
            @pl.when(n == 4 * stage + 3)
            def _():
                gram_step(1, upart, stage)

        return 0

    lax.fori_loop(0, plane + vals_delay + TWIN_LAG, spread, 0)
    ugram_copy = pltpu.make_async_copy(gfull.at[1], ugram_hbm, fetch_sem.at[5])
    ugram_copy.start()

    def drain(n):
        pair_copy(n).wait_send()
        twin(n, me).wait_send()

    each(0, plane, drain)

    def drain_mail(n):
        for h in range(2):
            letter(h, n, partner).wait_send()
            parcel(h, n, me, partner).wait_send()

    each(1, plane, drain_mail)
    gram_drain(0, gram_ref)
    gram_drain(1, upart)
    each(0, VSLOTS, lambda v: vals_copy(v, me).wait())
    ugram_copy.wait()


def scatter_kernel(
    coef, chunk, unroll, tile,
    rows_hbm, vals_ref, ugram_hbm, table_ref, state_ref, new_table_ref, new_state_ref,
    rows_ref, ugram_ref, vbuf, table, state, vsem, in_sem, out_sem, *accs,
):
    entries = rows_ref.shape[0]
    chunks = entries // chunk
    part = chunk // len(accs)
    rows_dev, width = table.shape
    tiles = rows_dev // tile

    def vals_copy(n):
        s = lax.rem(n, 2)
        return pltpu.make_async_copy(
            vals_ref.at[pl.ds(pl.multiple_of(n * chunk, 8), chunk)], vbuf.at[s], vsem.at[s]
        )

    table_copy = pltpu.make_async_copy(table_ref, table, in_sem.at[0])
    state_copy = pltpu.make_async_copy(state_ref, state, in_sem.at[1])
    rows_copy = pltpu.make_async_copy(rows_hbm, rows_ref, in_sem.at[2])
    ugram_copy = pltpu.make_async_copy(ugram_hbm, ugram_ref, in_sem.at[3])
    rows_copy.start()
    vals_copy(0).start()
    vals_copy(1).start()
    table_copy.start()
    state_copy.start()
    ugram_copy.start()
    for acc in accs:
        acc[...] = jnp.zeros_like(acc)

    def one(n, _):
        v = lax.rem(n, 2)
        vals_copy(n).wait()

        def scatter(s, _):
            start = n * chunk + s * unroll
            for q in range(unroll):
                rows = [
                    rows_ref.at[pl.ds(k * part + q, entries - chunk + part - unroll + 1)][start] for k in range(len(accs))
                ]
                news = [
                    acc[pl.ds(r, 1), :] + vbuf[v, pl.ds(s * unroll + (k * part + q), 1), :]
                    for k, (acc, r) in enumerate(zip(accs, rows))
                ]
                for acc, r, new in zip(accs, rows, news):
                    acc[pl.ds(r, 1), :] = new
            return 0

        lax.fori_loop(0, part // unroll, scatter, 0)

        @pl.when(n + 2 < chunks)
        def _():
            vals_copy(n + 2).start()

        return 0

    rows_copy.wait()
    lax.fori_loop(0, chunks, one, 0)
    table_copy.wait()
    state_copy.wait()
    ugram_copy.wait()
    u0, u1 = split2(ugram_ref[...])
    u00 = jnp.concatenate([u0, u0], axis=0)

    def out_copy(t, which):
        at = pl.ds(pl.multiple_of(t * tile, 8), tile)
        src, dst = ((table, new_table_ref), (state, new_state_ref))[which]
        return pltpu.make_async_copy(src.at[at], dst.at[at], out_sem.at[which, t])

    def finish(t, _):
        at = pl.ds(pl.multiple_of(t * tile, 8), tile)
        item = table[at, :]
        t0, t1 = split2(item)
        g = jnp.dot(jnp.concatenate([t0, t1], axis=1), u00, preferred_element_type=f32)
        g = 2.0 * coef * (g + jnp.dot(t0, u1, preferred_element_type=f32))
        add = accs[0][at, :]
        for acc in accs[1:]:
            add = add + acc[at, :]
        g = g + add
        new = state[at, :] + g * g
        state[at, :] = new
        table[at, :] = item - step_size * g * lax.rsqrt(new)
        out_copy(t, 0).start()
        out_copy(t, 1).start()
        return 0

    lax.fori_loop(0, tiles, finish, 0)

    def drain(t, _):
        out_copy(t, 0).wait()
        out_copy(t, 1).wait()
        return 0

    lax.fori_loop(0, tiles, drain, 0)


VM = pl.BlockSpec(memory_space=pltpu.VMEM)
HB = pl.BlockSpec(memory_space=pl.ANY)
SM = pl.BlockSpec(memory_space=pltpu.SMEM)
PARAMS = pltpu.CompilerParams(vmem_limit_bytes=60 * 1024 * 1024)


def shards(item_table, adagrad_state, history_ids, positive_ids):
    rows_dev, width = item_table.shape
    users_dev, hist_len = history_ids.shape
    devices = lax.axis_size("dp") * lax.axis_size("rows")
    groups = 2 * users_dev
    count = users_dev * (hist_len + 1)
    capacity = max(8, (count * 5 // (2 * devices) + 7) // 8 * 8)
    entries = devices * capacity
    asks = round_up(hist_len + 1, ROWS_AT_ONCE)
    data, shard = lax.axis_size("dp"), lax.axis_size("rows")
    sizes = line_sizes(data, shard)
    plane = devices // 2
    lines = sum(sizes) - 1
    unroll = max(n for n in (8, 16, 32, 64, 128) if capacity % n == 0)
    coef = penalty_weight / (rows_dev * devices)
    dma = pltpu.SemaphoreType.DMA
    list_shape = jax.ShapeDtypeStruct((devices, 1, capacity), i32)
    rows, codes, item_gram = pl.pallas_call(
        functools.partial(ask_kernel, data, shard, capacity),
        out_shape=(list_shape, list_shape, jax.ShapeDtypeStruct((width, width), f32)),
        in_specs=[HB, HB, HB],
        out_specs=(HB, HB, HB),
        scratch_shapes=[
            pltpu.VMEM((width, width), f32),
            pltpu.VMEM((asks, users_dev), i32),
            pltpu.VMEM((4 * devices, capacity), f32),
            pltpu.VMEM((devices, 1, capacity), i32),
            pltpu.VMEM((devices, 1, capacity), i32),
            pltpu.VMEM((rows_dev, width), f32),
        ]
        + [dma((devices,))] * 4
        + [dma((6,))],
        compiler_params=pltpu.CompilerParams(
            vmem_limit_bytes=60 * 1024 * 1024, collective_id=1, has_side_effects=True
        ),
        name="ask",
    )(history_ids.T, positive_ids[None], item_table)
    flat = rows.reshape(-1)
    vals, user_gram = pl.pallas_call(
        functools.partial(exchange_kernel, sizes, capacity, users_dev, hist_len, coef, unroll),
        out_shape=(
            jax.ShapeDtypeStruct((devices, capacity, width), f32),
            jax.ShapeDtypeStruct((width, width), f32),
        ),
        in_specs=[HB, HB, HB, HB, HB],
        out_specs=(HB, HB),
        scratch_shapes=[
            pltpu.SMEM((entries,), i32),
            pltpu.SMEM((entries,), i32),
            pltpu.VMEM((devices, 1, capacity), i32),
            pltpu.VMEM((width, width), f32),
            pltpu.VMEM((rows_dev, width), f32),
            dma((6,)),
            pltpu.VMEM((capacity, width), f32),
            pltpu.VMEM((2, plane, 2, users_dev, width), f32),
            pltpu.VMEM((plane, 2, users_dev, width), f32),
            pltpu.VMEM((2, plane, users_dev, width), f32),
            pltpu.VMEM((devices, 2, users_dev, width), f32),
            pltpu.VMEM((groups + 8, width), f32),
            pltpu.VMEM((VSLOTS, capacity, width), f32),
            pltpu.VMEM((width, width), f32),
            pltpu.VMEM((2, 4, width // 2, width), f32),
            pltpu.VMEM((2, lines, width // 2, width), f32),
            pltpu.VMEM((2, width, width), f32),
            dma((plane,)),
            dma((plane,)),
            dma((2, plane)),
            dma((2, plane)),
            dma((2, plane)),
            dma((2, plane)),
            dma((plane,)),
            dma((plane,)),
            dma((2, lines)),
            dma((2, lines)),
            dma((VSLOTS,)),
        ],
        compiler_params=pltpu.CompilerParams(
            vmem_limit_bytes=60 * 1024 * 1024, collective_id=0, has_side_effects=True
        ),
        name="exchange",
    )(flat, codes.reshape(-1), codes, item_gram, item_table)
    chunk, tile = min(4096, entries), 1024
    return pl.pallas_call(
        functools.partial(scatter_kernel, coef, chunk, 16, tile),
        out_shape=(
            jax.ShapeDtypeStruct(item_table.shape, f32),
            jax.ShapeDtypeStruct(item_table.shape, f32),
        ),
        in_specs=[HB, HB, HB, HB, HB],
        out_specs=(HB, HB),
        scratch_shapes=[
            pltpu.SMEM((entries,), i32),
            pltpu.VMEM((width, width), f32),
            pltpu.VMEM((2, chunk, width), f32),
            pltpu.VMEM((rows_dev, width), f32),
            pltpu.VMEM((rows_dev, width), f32),
            dma((2,)),
            dma((4,)),
            dma((2, rows_dev // tile)),
        ]
        + [pltpu.VMEM((rows_dev, width), f32)] * STREAMS,
        compiler_params=PARAMS,
        name="scatter",
    )(flat, vals.reshape(entries, width), user_gram, item_table, adagrad_state)


def solution(mesh):
    return jax.shard_map(
        shards,
        mesh=mesh,
        in_specs=(
            P(("dp", "rows"), None),
            P(("dp", "rows"), None),
            P(("dp", "rows"), None),
            P(("dp", "rows")),
        ),
        out_specs=(P(("dp", "rows"), None), P(("dp", "rows"), None)),
        check_vma=False,
    )
```
